32 devices in a mesh: dp: 8 (over z, y), head: 4 (over x, core).
Axes of the slice: x: 2, y: 2, z: 4, core: 2. Of those that a mesh axis runs over, the one named last changes fastest.
Arguments:
- hidden_in: bfloat16 [64, 512, 768], P(('dp', 'head')), may hold values from -6 to 6
- lengths: int32 [64], P(('dp', 'head')), may hold values from 1 to 512, 13107 in all
- labels: int32 [64], P(('dp', 'head')), may hold values from 0 to 2
- query_key_value_weight: bfloat16 [3, 768, 768], P(None, None, 'head'), may hold values from -0.21875 to 0.21875
- query_value_bias: float32 [2, 768], P(None, 'head'), may hold values from -3 to 3
- attention_output_weight: bfloat16 [768, 768], replicated, may hold values from -0.875 to 0.875
- attention_output_bias: float32 [768], replicated, may hold values from -3 to 3
- gain_att: float32 [768], replicated, may hold values from 0.5 to 1.5
- shift_att: float32 [768], replicated, may hold values from -3 to 3
- up_weight: bfloat16 [768, 3072], replicated, may hold values from -0.21875 to 0.21875
- up_bias: float32 [3072], replicated, may hold values from -3 to 3
- down_weight: bfloat16 [3072, 768], replicated, may hold values from -0.109375 to 0.109375
- down_bias: float32 [768], replicated, may hold values from -3 to 3
- gain_ffn: float32 [768], replicated, may hold values from 0.5 to 1.5
- shift_ffn: float32 [768], replicated, may hold values from -3 to 3
- w_pool: bfloat16 [768, 768], replicated, may hold values from -0.21875 to 0.21875
- b_pool: float32 [768], replicated, may hold values from -3 to 3
- w_class: bfloat16 [768, 3], replicated, may hold values from -0.625 to 0.625
- b_class: float32 [3], replicated, may hold values from -3 to 3
- cotangent: bfloat16 [64, 512, 768], P(('dp', 'head')), may hold values from -6 to 6
Outputs:
- hidden_out: bfloat16 [64, 512, 768], P(('dp', 'head'))
- ramp_loss: float32 [64], P(('dp', 'head'))
- grad_in: float32 [64, 512, 768], P(('dp', 'head'))
- grad_w_qkv: float32 [3, 768, 768], P(None, None, 'head')
- grad_b_qv: float32 [2, 768], P(None, 'head')
- grad_w_out: float32 [768, 768], replicated
- grad_b_out: float32 [768], replicated
- grad_gain_att: float32 [768], replicated
- grad_shift_att: float32 [768], replicated
- grad_w_up: float32 [768, 3072], P(None, ('dp', 'head'))
- grad_b_up: float32 [3072], replicated
- grad_w_down: float32 [3072, 768], P(('dp', 'head'))
- grad_b_down: float32 [768], replicated
- grad_gain_ffn: float32 [768], replicated
- grad_shift_ffn: float32 [768], replicated
- grad_w_pool: float32 [768, 768], replicated
- grad_b_pool: float32 [768], replicated
- grad_w_class: float32 [768, 3], replicated
- grad_b_class: float32 [3], replicated
The draws below stay inside these ranges and needn't reach their ends.
Inputs may be any that keep to these rules, and one draw needn't show every extreme that they name: A sequence's tokens are its first lengths entries, the rest is padding; some sequence has all 512.
All inputs are finite; a program needn't handle non-finite values. No bound on the sum of `lengths` on one device may be relied on, other than what follows from the above.
Results may differ from the reference program's by a relative error of at most 0.018.
Values may be sent and summed in bfloat16 or wider, within the bound.
A program may use at most 192 MiB of HBM per device.

```python
import math
import jax
import jax.numpy as jnp
import numpy as np
from jax import lax

D = 768
HEAD_DIM = 64
FF = 3072
CLASSES = 3
LEN = 512
SEQ_GRP = 8
SEQS = 64


def plant(values, own_key, smallest, top_value):
    longest = values.shape.index(max(values.shape))
    spots = []
    for shift in (0, 1):
        where = [jax.random.randint(jax.random.fold_in(own_key, axis), (), 0, length) for axis, length in enumerate(values.shape)]
        where[longest] = (where[longest] + shift) % values.shape[longest]
        spots.append(tuple(where))
    return values.at[spots[0]].set(smallest).at[spots[1]].set(top_value)


def block_levels(own_key, shape, pieces, low, high):
    level, own = 1.0, jax.random.fold_in(own_key, 6)
    for dim, shards_of in pieces:
        heights = jnp.exp(jax.random.uniform(jax.random.fold_in(own, dim), (shards_of,), jnp.float32, low / len(pieces), high / len(pieces)))
        level = level * jnp.repeat(heights, shape[dim] // shards_of).reshape([-1 if axis == dim else 1 for axis in range(len(shape))])
    return level


def length_profile(amount, total, most, lean):
    portions = [(1 << 20) // math.isqrt(grade ** lean) + 1 for grade in range(2, amount + 1)]
    spare, holding = total - most - (amount - 1), [1] * (amount - 1)
    while spare > 0:
        movable = [i for i in range(amount - 1) if holding[i] < most]
        whole, budget = sum([portions[i] for i in movable]), spare
        for i in movable:
            extra = min(most - holding[i], max(1, budget * portions[i] // whole), spare)
            holding[i] = holding[i] + extra
            spare = spare - extra
    return np.array([most] + holding)


def uneven(stream_key, count, total, bound, skew):
    if count == 2:
        one = jax.random.randint(stream_key, (), max(1, total - bound), min(bound, total - 1) + 1)
        return jnp.stack([one, total - one])
    sizes = jnp.asarray(length_profile(count, total, bound, skew), jnp.int32)
    couples = (count - 1) // 2
    donor, receiver = sizes[1:1 + 2 * couples:2], sizes[2:2 + 2 * couples:2]
    room = jnp.minimum(donor - 1, bound - receiver)
    passed = jax.random.randint(jax.random.fold_in(stream_key, 1), (couples,), 0, 1 << 20) % (room + 1)
    sizes = sizes.at[1:1 + 2 * couples:2].set(donor - passed).at[2:2 + 2 * couples:2].set(receiver + passed)
    return sizes[jax.random.permutation(jax.random.fold_in(stream_key, 2), count)]


def bell_draw(key, shape, width, reach, shards=(), kind=jnp.bfloat16):
    drawn = jax.random.normal(key, shape, jnp.float32) * width
    if len(shards) > 0:
        drawn = block_levels(key, shape, shards, -0.22, 0.18) * drawn
    return jnp.clip(drawn, min=-reach, max=reach).astype(kind)


def setup_inputs(seed: int = 0) -> dict:
    arg_keys = jax.random.split(jax.random.key(seed), 21)
    hidden_in = bell_draw(arg_keys[0], (SEQS, LEN, D), 1.0, 6.0, ((0, 32),))
    lengths = uneven(arg_keys[1], SEQS, 2 * SEQS * LEN // 5, LEN, 2).astype(jnp.int32)
    labels = plant(jax.random.randint(arg_keys[2], (SEQS,), 0, CLASSES), jax.random.fold_in(arg_keys[2], 1), 0, CLASSES - 1).astype(jnp.int32)
    query_key_value_weight = bell_draw(arg_keys[3], (3, D, D), D ** -0.5, 0.21875, ((2, 4),))
    query_value_bias = bell_draw(arg_keys[4], (2, D), 0.5, 3.0, ((1, 4),), jnp.float32)
    attention_output_weight = bell_draw(arg_keys[5], (D, D), (D // 16) ** -0.5, 0.875)
    attention_output_bias = bell_draw(arg_keys[6], (D,), 0.5, 3.0, (), jnp.float32)
    gain_att = jnp.clip(1.0 + 0.1 * jax.random.normal(arg_keys[7], (D,), jnp.float32), 0.5, 1.5)
    shift_att = bell_draw(arg_keys[8], (D,), 0.5, 3.0, (), jnp.float32)
    up_weight = bell_draw(arg_keys[9], (D, FF), D ** -0.5, 0.21875)
    up_bias = bell_draw(arg_keys[10], (FF,), 0.5, 3.0, (), jnp.float32)
    down_weight = bell_draw(arg_keys[11], (FF, D), FF ** -0.5, 0.109375)
    down_bias = bell_draw(arg_keys[12], (D,), 0.5, 3.0, (), jnp.float32)
    gain_ffn = jnp.clip(1.0 + 0.1 * jax.random.normal(arg_keys[13], (D,), jnp.float32), 0.5, 1.5)
    shift_ffn = bell_draw(arg_keys[14], (D,), 0.5, 3.0, (), jnp.float32)
    w_pool = bell_draw(arg_keys[15], (D, D), D ** -0.5, 0.21875)
    b_pool = bell_draw(arg_keys[16], (D,), 0.5, 3.0, (), jnp.float32)
    w_class = bell_draw(arg_keys[17], (D, CLASSES), (D // 9) ** -0.5, 0.625)
    b_class = bell_draw(arg_keys[18], (CLASSES,), 0.5, 3.0, (), jnp.float32)
    cotangent = bell_draw(arg_keys[19], (SEQS, LEN, D), 1.0, 6.0, ((0, 32),))
    return dict(hidden_in=hidden_in, lengths=lengths, labels=labels, query_key_value_weight=query_key_value_weight, query_value_bias=query_value_bias, attention_output_weight=attention_output_weight, attention_output_bias=attention_output_bias, gain_att=gain_att, shift_att=shift_att, up_weight=up_weight, up_bias=up_bias, down_weight=down_weight, down_bias=down_bias, gain_ffn=gain_ffn, shift_ffn=shift_ffn, w_pool=w_pool, b_pool=b_pool, w_class=w_class, b_class=b_class, cotangent=cotangent)


EXACT_MATMUL = lax.Precision.HIGHEST

@jax.custom_vjp
def reduced_input(v):
    return lax.optimization_barrier(v.astype(jnp.bfloat16)).astype(jnp.float32)

@jax.custom_vjp
def reduced_backward(v):
    return v

def low_keep(v):
    return (reduced_input(v), None)

def low_pass(kept, grad):
    return (grad,)

def back_keep(v):
    return (v, None)

def back_low(kept, grad):
    return (reduced_input(grad),)
reduced_input.defvjp(low_keep, low_pass)
reduced_backward.defvjp(back_keep, back_low)

def layer_norm(row_block, gain_row, shift_row):
    center = lax.optimization_barrier(jnp.mean(row_block, axis=-1, keepdims=True))
    centered = row_block - center
    spread = lax.optimization_barrier(jnp.mean(centered * centered, axis=-1, keepdims=True))
    return centered * lax.rsqrt(spread + 1e-06) * gain_row + shift_row

def attend(packed):
    query_rows, key_rows, value_rows, length = packed
    row_count = query_rows.shape[0]
    head_count = query_rows.shape[1] // HEAD_DIM
    query_heads = query_rows.reshape(row_count, head_count, HEAD_DIM)
    key_heads = key_rows.reshape(row_count, head_count, HEAD_DIM)
    value_heads = value_rows.reshape(row_count, head_count, HEAD_DIM)
    scores = reduced_backward(jnp.einsum('qhd,khd->hqk', query_heads, key_heads, precision=EXACT_MATMUL) * HEAD_DIM ** (-0.5))
    valid_keys = jnp.arange(row_count) < length
    scores = jnp.where(valid_keys[None, None, :], scores, -1000000000.0)
    attention = reduced_input(jax.nn.softmax(scores, axis=-1))
    context_rows = jnp.einsum('hqk,khd->qhd', attention, value_heads, precision=EXACT_MATMUL)
    return context_rows.reshape(row_count, head_count * HEAD_DIM)

def block_forward(params, hidden_state, lengths, labels, cotangent):
    query_key_value_weight, query_value_bias, attention_output_weight, attention_output_bias, gain_att, shift_att, up_weight, up_bias, down_weight, down_bias, gain_ffn, shift_ffn, w_pool, b_pool, w_class, b_class = params
    query_matrix = reduced_input(reduced_backward(jnp.einsum('qxg,gy->qxy', hidden_state, query_key_value_weight[0], precision=EXACT_MATMUL) + query_value_bias[0]))
    key_matrix = reduced_input(reduced_backward(jnp.einsum('qxg,gy->qxy', hidden_state, query_key_value_weight[1], precision=EXACT_MATMUL)))
    value_matrix = reduced_input(reduced_backward(jnp.einsum('qxg,gy->qxy', hidden_state, query_key_value_weight[2], precision=EXACT_MATMUL) + query_value_bias[1]))
    context_rows = lax.map(jax.checkpoint(attend), (query_matrix, key_matrix, value_matrix, lengths))
    context_rows = reduced_input(reduced_backward(context_rows))
    attention_result = reduced_backward(jnp.einsum('qxg,gy->qxy', context_rows, attention_output_weight, precision=EXACT_MATMUL) + attention_output_bias)
    normalized_first = layer_norm(hidden_state + attention_result, gain_att, shift_att)
    before_gelu = reduced_backward(jnp.einsum('kpi,im->kpm', reduced_input(normalized_first), up_weight, precision=EXACT_MATMUL) + up_bias)
    gelu_output = reduced_input(jax.nn.gelu(before_gelu, approximate=False))
    residual_branch = reduced_backward(jnp.einsum('wmi,iz->wmz', gelu_output, down_weight, precision=EXACT_MATMUL) + down_bias)
    output_rows = layer_norm(normalized_first + residual_branch, gain_ffn, shift_ffn)
    cls_rows = reduced_input(output_rows[:, 0, :])
    pooled = jnp.tanh(reduced_backward(jnp.dot(cls_rows, w_pool, precision=EXACT_MATMUL) + b_pool))
    logits = jnp.dot(pooled, w_class, precision=EXACT_MATMUL) + b_class
    onehot = jax.nn.one_hot(labels, CLASSES, dtype=jnp.float32)
    loss_rows = jax.nn.logsumexp(logits, axis=-1) - lax.optimization_barrier(jnp.sum(logits * onehot, axis=-1))
    objective = jnp.sum(output_rows * cotangent) + jnp.sum(loss_rows)
    return (objective, (output_rows, loss_rows))

def reference(hidden_in, lengths, labels, query_key_value_weight, query_value_bias, attention_output_weight, attention_output_bias, gain_att, shift_att, up_weight, up_bias, down_weight, down_bias, gain_ffn, shift_ffn, w_pool, b_pool, w_class, b_class, cotangent):
    params = tuple((weight.astype(jnp.float32) for weight in (query_key_value_weight, query_value_bias, attention_output_weight, attention_output_bias, gain_att, shift_att, up_weight, up_bias, down_weight, down_bias, gain_ffn, shift_ffn, w_pool, b_pool, w_class, b_class)))
    blocks = SEQS // SEQ_GRP

    def regroup(array):
        return array.reshape((blocks, SEQ_GRP) + array.shape[1:])
    inputs = (regroup(hidden_in.astype(jnp.float32)), regroup(lengths), regroup(labels), regroup(cotangent.astype(jnp.float32)))

    def step(totals, block_item):
        hidden_state, length_rows, label_rows, cot_block = block_item

        def objective(weights, hidden_rows):
            return block_forward(weights, hidden_rows, length_rows, label_rows, cot_block)
        unused, pullback, (output_rows, loss_rows) = jax.vjp(objective, params, hidden_state, has_aux=True)
        grad_params, grad_hidden = pullback(jnp.ones((), jnp.float32))
        totals = jax.tree.map(lambda earlier, latest: earlier + latest, totals, grad_params)
        return (totals, (output_rows.astype(jnp.bfloat16), loss_rows, grad_hidden))
    zero_grads = jax.tree.map(jnp.zeros_like, params)
    totals, (outputs, losses, grads_in) = lax.scan(step, zero_grads, inputs)
    return (outputs.reshape(SEQS, LEN, D), losses.reshape(SEQS), grads_in.reshape(SEQS, LEN, D), totals[0], totals[1], totals[2], totals[3], totals[4], totals[5], totals[6], totals[7], totals[8], totals[9], totals[10], totals[11], totals[12], totals[13], totals[14], totals[15])
```

```python
import jax
import jax.numpy as jnp
from jax import lax
from jax.sharding import PartitionSpec as P

HEAD_DIM = 64
EPSILON = 1e-06
MASKED = -1000000000.0
BF16, F32 = jnp.bfloat16, jnp.float32


def bit_count(n):
    assert n & (n - 1) == 0
    return n.bit_length() - 1


def exchange(value, axis, bit):
    size = lax.axis_size(axis)
    step = 1 << bit
    return lax.ppermute(value, axis, [(i, i ^ step) for i in range(size)])


def own_bit(axis, bit):
    return (lax.axis_index(axis) >> bit) & 1


def bits_of(axes):
    found = []
    for axis in axes:
        found += [(axis, b) for b in reversed(range(bit_count(lax.axis_size(axis))))]
    return found


def halve(value, position, axis, bit):
    mine = own_bit(axis, bit)
    send = lax.dynamic_index_in_dim(value, 1 - mine, position, keepdims=True)
    keep = lax.dynamic_index_in_dim(value, mine, position, keepdims=True)
    got = exchange(send, axis, bit)
    return keep.astype(F32) + got.astype(F32)


def scatter_sum(value, axes, order):
    joint = bits_of(axes)
    rows = value.shape[0] >> len(joint)
    value = value.reshape((2,) * len(joint) + (rows,) + value.shape[1:])
    for axis, bit in order:
        total = halve(value, joint.index((axis, bit)), axis, bit)
        value = total.astype(BF16)
    return total.reshape((rows,) + value.shape[len(joint) + 1 :])


def gather_blocks(value, axes, order):
    joint = bits_of(axes)
    value = value.reshape((1,) * len(joint) + value.shape)
    for axis, bit in order:
        mine = own_bit(axis, bit)
        place = joint.index((axis, bit))
        got = exchange(value, axis, bit)
        value = jnp.where(
            mine == 0,
            jnp.concatenate([value, got], axis=place),
            jnp.concatenate([got, value], axis=place),
        )
    return value.reshape((-1,) + value.shape[len(joint) + 1 :])


def all_sum(value, axes):
    for axis, bit in reversed(bits_of(axes)):
        value = value + exchange(value, axis, bit)
    return value


def normalize(row_block, gain_row, shift_row):
    center = jnp.mean(row_block, axis=-1, keepdims=True)
    centered = row_block - center
    spread = jnp.mean(centered * centered, axis=-1, keepdims=True)
    return centered * lax.rsqrt(spread + EPSILON) * gain_row + shift_row


def gelu_exact(values):
    return jax.nn.gelu(values, approximate=False)


def split_heads(row_block):
    return row_block.reshape(row_block.shape[0], row_block.shape[1] // HEAD_DIM, HEAD_DIM)


def head_scores(query_rows, key_rows, length):
    scores = jnp.einsum(
        "qhd,khd->hqk", split_heads(query_rows), split_heads(key_rows), preferred_element_type=F32
    ) * HEAD_DIM ** (-0.5)
    valid_keys = jnp.arange(key_rows.shape[0]) < length
    return jnp.where(valid_keys[None, None, :], scores, MASKED)


def attend_one(packed):
    query_rows, key_rows, value_rows, length = packed
    scores = head_scores(query_rows, key_rows, length)
    highest = jnp.max(scores, axis=-1, keepdims=True)
    shifted = jnp.exp(scores - highest)
    summed = jnp.sum(shifted, axis=-1, keepdims=True)
    attention = (shifted / summed).astype(BF16)
    log_total = highest + jnp.log(summed)
    context_rows = jnp.einsum(
        "hqk,khd->qhd", attention, split_heads(value_rows), preferred_element_type=F32
    )
    return (context_rows.reshape(query_rows.shape[0], -1).astype(BF16), log_total[..., 0])


def attend_back(packed):
    query_rows, key_rows, value_rows, length, log_total, grad_context = packed
    scores = head_scores(query_rows, key_rows, length)
    attention = jnp.exp(scores - log_total[..., None])
    grad_heads = split_heads(grad_context)
    grad_value = jnp.einsum(
        "hqk,qhd->khd", attention.astype(BF16), grad_heads, preferred_element_type=F32
    )
    grad_attention = jnp.einsum(
        "qhd,khd->hqk", grad_heads, split_heads(value_rows), preferred_element_type=F32
    )
    weighted = jnp.sum(attention * grad_attention, axis=-1, keepdims=True)
    grad_scores = (attention * (grad_attention - weighted)).astype(BF16)
    score_scale = HEAD_DIM ** (-0.5)
    grad_query = (
        jnp.einsum("hqk,khd->qhd", grad_scores, split_heads(key_rows), preferred_element_type=F32)
        * score_scale
    )
    grad_key = (
        jnp.einsum("hqk,qhd->khd", grad_scores, split_heads(query_rows), preferred_element_type=F32)
        * score_scale
    )
    row_count, width = query_rows.shape
    return jnp.stack(
        [
            grad_query.reshape(row_count, width),
            grad_key.reshape(row_count, width),
            grad_value.reshape(row_count, width),
        ]
    ).astype(BF16)


def classify(cls_rows, labels, w_pool, b_pool, w_class, b_class):
    pooled = jnp.tanh(jnp.dot(cls_rows, w_pool, preferred_element_type=F32) + b_pool)
    class_weight = w_class.astype(F32)
    logits = jnp.dot(pooled, class_weight, precision=lax.Precision.HIGHEST) + b_class
    onehot = (labels[:, None] == jnp.arange(logits.shape[1])[None, :]).astype(F32)
    ramp_loss = jax.nn.logsumexp(logits, axis=-1) - jnp.sum(logits * onehot, axis=-1)
    grad_logits = jax.nn.softmax(logits, axis=-1) - onehot
    grad_pool = (
        jnp.dot(grad_logits, class_weight.T, precision=lax.Precision.HIGHEST)
        * (1.0 - pooled * pooled)
    ).astype(BF16)
    return pooled, ramp_loss, grad_logits, grad_pool


def body(
    hidden_in,
    lengths,
    labels,
    query_key_value_weight,
    query_value_bias,
    attention_output_weight,
    attention_output_bias,
    gain_att,
    shift_att,
    up_weight,
    up_bias,
    down_weight,
    down_bias,
    gain_ffn,
    shift_ffn,
    w_pool,
    b_pool,
    w_class,
    b_class,
    cotangent,
):
    seq_here, seq_len, width = hidden_in.shape
    tokens = seq_here * seq_len
    everyone = ("dp", "head")
    head_bits = bits_of(("head",))
    dp_bits = bits_of(("dp",))
    rows_in = hidden_in.reshape(tokens, width)

    weight_rows = jnp.transpose(query_key_value_weight, (2, 0, 1))
    all_weights = gather_blocks(weight_rows, ("head",), list(reversed(head_bits)))
    all_bias = gather_blocks(query_value_bias.T, ("head",), list(reversed(head_bits))).T
    bias_rows = jnp.stack([all_bias[0], jnp.zeros_like(all_bias[0]), all_bias[1]])
    projected = jnp.einsum("nd,etd->tne", rows_in, all_weights, preferred_element_type=F32)
    projected = (
        (projected + bias_rows[:, None, :]).astype(BF16).reshape(3, seq_here, seq_len, width)
    )
    context_rows, log_totals = lax.map(
        attend_one, (projected[0], projected[1], projected[2], lengths)
    )
    combined = context_rows.reshape(tokens, width)
    attended = (
        jnp.dot(combined, attention_output_weight, preferred_element_type=F32)
        + attention_output_bias
    )
    first_in = rows_in.astype(F32) + attended
    normalized_first = normalize(first_in, gain_att, shift_att)
    normed_low = normalized_first.astype(BF16)
    before_gelu = jnp.dot(normed_low, up_weight, preferred_element_type=F32) + up_bias
    gelu_output = gelu_exact(before_gelu).astype(BF16)
    branch = jnp.dot(gelu_output, down_weight, preferred_element_type=F32) + down_bias
    second_in = normalized_first + branch
    output_rows = normalize(second_in, gain_ffn, shift_ffn)
    hidden_out = output_rows.astype(BF16).reshape(seq_here, seq_len, width)
    cls_rows = hidden_out[:, 0, :]
    _, ramp_loss, _, grad_pool_here = classify(cls_rows, labels, w_pool, b_pool, w_class, b_class)
    grad_cls = jnp.dot(grad_pool_here, w_pool.T, preferred_element_type=F32)

    gather_order = list(reversed(bits_of(everyone)))
    all_cls = gather_blocks(cls_rows, everyone, gather_order)
    all_labels = gather_blocks(labels, everyone, gather_order)
    pooled, _, grad_logits, grad_pool = classify(
        all_cls, all_labels, w_pool, b_pool, w_class, b_class
    )
    grad_b_class = jnp.sum(grad_logits, axis=0)
    grad_w_class = jnp.dot(pooled.T, grad_logits, precision=lax.Precision.HIGHEST)
    grad_b_pool = jnp.sum(grad_pool, axis=0, dtype=F32)
    grad_w_pool = jnp.dot(all_cls.T, grad_pool, preferred_element_type=F32)

    grad_output = cotangent.astype(F32).at[:, 0, :].add(grad_cls).reshape(tokens, width)
    _, second_back = jax.vjp(normalize, second_in, gain_ffn, shift_ffn)
    grad_second, grad_gain_ffn, grad_shift_ffn = second_back(grad_output)
    grad_branch = grad_second.astype(BF16)
    grad_b_down = jnp.sum(grad_branch, axis=0, dtype=F32)
    part_w_down = jnp.dot(gelu_output.T, grad_branch, preferred_element_type=F32).astype(BF16)
    grad_activated = jnp.dot(grad_branch, down_weight.T, preferred_element_type=F32)
    _, gelu_back = jax.vjp(gelu_exact, before_gelu)
    grad_pre = gelu_back(grad_activated)[0].astype(BF16)
    grad_b_up = jnp.sum(grad_pre, axis=0, dtype=F32)
    part_w_up = jnp.dot(grad_pre.T, normed_low, preferred_element_type=F32).astype(BF16)

    order_down = list(reversed(head_bits)) + list(reversed(dp_bits))
    order_up = [head_bits[-1], dp_bits[-1]] + list(reversed(head_bits[:-1])) + list(reversed(dp_bits[:-1]))
    grad_w_down = scatter_sum(part_w_down, everyone, order_down)
    grad_w_up = scatter_sum(part_w_up, everyone, order_up).T

    grad_first = grad_second + jnp.dot(grad_pre, up_weight.T, preferred_element_type=F32)
    _, first_back = jax.vjp(normalize, first_in, gain_att, shift_att)
    grad_first_in, grad_gain_att, grad_shift_att = first_back(grad_first)
    grad_attended = grad_first_in.astype(BF16)
    grad_b_out = jnp.sum(grad_attended, axis=0, dtype=F32)
    part_w_out = jnp.dot(combined.T, grad_attended, preferred_element_type=F32).astype(BF16)
    own_w_out = scatter_sum(part_w_out, everyone, order_down)
    grad_w_out = gather_blocks(
        own_w_out.astype(BF16), everyone, list(reversed(order_down))
    ).astype(F32)
    grad_context = (
        jnp.dot(grad_attended, attention_output_weight.T, preferred_element_type=F32)
        .astype(BF16)
        .reshape(seq_here, seq_len, width)
    )
    sums = all_sum(
        jnp.concatenate(
            [
                grad_b_out,
                grad_gain_att,
                grad_shift_att,
                grad_b_up,
                grad_b_down,
                grad_gain_ffn,
                grad_shift_ffn,
            ]
        ),
        everyone,
    )
    edges = [width, 2 * width, 3 * width, 3 * width + up_bias.shape[0]]
    edges += [edges[-1] + width, edges[-1] + 2 * width]
    (
        grad_b_out,
        grad_gain_att,
        grad_shift_att,
        grad_b_up,
        grad_b_down,
        grad_gain_ffn,
        grad_shift_ffn,
    ) = jnp.split(sums, edges)

    grads = lax.map(
        attend_back,
        (projected[0], projected[1], projected[2], lengths, log_totals, grad_context),
    )
    grads = jnp.moveaxis(grads, 1, 0).reshape(3, tokens, width)
    part_w_qkv = jnp.einsum("tne,nd->etd", grads, rows_in, preferred_element_type=F32).astype(BF16)
    own_w_qkv = scatter_sum(part_w_qkv, ("head",), list(reversed(head_bits)))
    local = own_w_qkv.shape[0]
    flat = own_w_qkv.astype(BF16).reshape(local * 3, width)
    dp_order = list(reversed(dp_bits))
    own_flat = scatter_sum(flat, ("dp",), dp_order)
    flat = gather_blocks(own_flat.astype(BF16), ("dp",), list(reversed(dp_order)))
    grad_w_qkv = jnp.transpose(flat.reshape(local, 3, width), (1, 2, 0)).astype(F32)
    bias_sums = jnp.sum(grads, axis=1, dtype=F32)
    bias_all = all_sum(jnp.stack([bias_sums[0], bias_sums[2]]), everyone)
    grad_b_qv = lax.dynamic_slice_in_dim(bias_all, lax.axis_index("head") * local, local, 1)
    grad_in = grad_first_in + jnp.einsum(
        "tne,etd->nd", grads, all_weights, preferred_element_type=F32
    )
    return (
        hidden_out,
        ramp_loss,
        grad_in.reshape(seq_here, seq_len, width),
        grad_w_qkv,
        grad_b_qv,
        grad_w_out,
        grad_b_out,
        grad_gain_att,
        grad_shift_att,
        grad_w_up,
        grad_b_up,
        grad_w_down,
        grad_b_down,
        grad_gain_ffn,
        grad_shift_ffn,
        grad_w_pool,
        grad_b_pool,
        grad_w_class,
        grad_b_class,
    )


def solution(mesh):
    rows = P(("dp", "head"))
    placed = (
        (P(("dp", "head"), None, None), rows, rows, P(None, None, "head"), P(None, "head"))
        + (P(),) * 14
        + (P(("dp", "head"), None, None),)
    )
    tokens = P(("dp", "head"), None, None)
    outs = (
        (tokens, rows, tokens, P(None, None, "head"), P(None, "head"))
        + (P(),) * 4
        + (P(None, ("dp", "head")), P(), P(("dp", "head"), None))
        + (P(),) * 7
    )
    return jax.shard_map(body, mesh=mesh, in_specs=placed, out_specs=outs, check_vma=False)
```

```python
import jax
import jax.numpy as jnp
from jax import lax
from jax.experimental import pallas as pl
from jax.experimental.pallas import tpu as pltpu
from jax.sharding import PartitionSpec as P

HEAD_DIM = 64
EPSILON = 1e-06
MASKED = -1000000000.0
BF16, F32 = jnp.bfloat16, jnp.float32


def bit_count(n):
    assert n & (n - 1) == 0
    return n.bit_length() - 1


def exchange(value, axis, bit):
    size = lax.axis_size(axis)
    step = 1 << bit
    return lax.ppermute(value, axis, [(i, i ^ step) for i in range(size)])


def own_bit(axis, bit):
    return (lax.axis_index(axis) >> bit) & 1


def bits_of(axes):
    found = []
    for axis in axes:
        found += [(axis, b) for b in reversed(range(bit_count(lax.axis_size(axis))))]
    return found


def halve(value, position, axis, bit):
    mine = own_bit(axis, bit)
    send = lax.dynamic_index_in_dim(value, 1 - mine, position, keepdims=True)
    keep = lax.dynamic_index_in_dim(value, mine, position, keepdims=True)
    got = exchange(send, axis, bit)
    return keep.astype(F32) + got.astype(F32)


def scatter_sum(value, axes, order):
    joint = bits_of(axes)
    rows = value.shape[0] >> len(joint)
    value = value.reshape((2,) * len(joint) + (rows,) + value.shape[1:])
    for axis, bit in order:
        total = halve(value, joint.index((axis, bit)), axis, bit)
        value = total.astype(BF16)
    return total.reshape((rows,) + value.shape[len(joint) + 1 :])


def gather_blocks(value, axes, order):
    joint = bits_of(axes)
    value = value.reshape((1,) * len(joint) + value.shape)
    for axis, bit in order:
        mine = own_bit(axis, bit)
        place = joint.index((axis, bit))
        got = exchange(value, axis, bit)
        value = jnp.where(
            mine == 0,
            jnp.concatenate([value, got], axis=place),
            jnp.concatenate([got, value], axis=place),
        )
    return value.reshape((-1,) + value.shape[len(joint) + 1 :])


def all_sum(value, axes):
    for axis, bit in reversed(bits_of(axes)):
        value = value + exchange(value, axis, bit)
    return value


def normalize(row_block, gain_row, shift_row):
    center = jnp.mean(row_block, axis=-1, keepdims=True)
    centered = row_block - center
    spread = jnp.mean(centered * centered, axis=-1, keepdims=True)
    return centered * lax.rsqrt(spread + EPSILON) * gain_row + shift_row


LANES = 128
PAIR = LANES // HEAD_DIM
SCALE = HEAD_DIM ** (-0.5)


def dot_nt(left, right):
    return lax.dot_general(left, right, (((1,), (1,)), ((), ())), preferred_element_type=F32)


def dot_nn(left, right):
    return jnp.dot(left, right, preferred_element_type=F32)


def head_lanes(block, head):
    lane = lax.broadcasted_iota(jnp.int32, block.shape, 1)
    inside = (lane >= head * HEAD_DIM) & (lane < (head + 1) * HEAD_DIM)
    return jnp.where(inside, block.astype(F32), 0.0)


def attend_kernel(length_ref, query_ref, key_ref, value_ref, context_ref, probs_ref):
    length = length_ref[pl.program_id(0)]
    query, key = query_ref[...], key_ref[...]
    value_t = value_ref[...].T
    rows = query.shape[0]
    key_at = lax.broadcasted_iota(jnp.int32, (rows, rows), 0)
    contexts = []
    for head in range(PAIR):
        own_query = (head_lanes(query, head) * SCALE).astype(BF16)
        scores = jnp.where(key_at < length, dot_nt(key, own_query), MASKED)
        shifted = jnp.exp(scores - jnp.max(scores, axis=0, keepdims=True))
        inverse = 1.0 / jnp.sum(shifted, axis=0, keepdims=True)
        probs = (shifted * inverse).astype(BF16)
        probs_ref[0, head] = probs
        contexts.append(dot_nn(value_t[head * HEAD_DIM : (head + 1) * HEAD_DIM], probs))
    context_ref[...] = jnp.concatenate(contexts, axis=0).T.astype(BF16)


def attend(lengths, query, key, value):
    seqs = lengths.shape[0]
    tokens, width = query.shape
    rows, pairs = tokens // seqs, width // LANES
    block = pl.BlockSpec((rows, LANES), lambda s, p: (s, p))
    return pl.pallas_call(
        attend_kernel,
        grid=(seqs, pairs),
        in_specs=[pl.BlockSpec(memory_space=pltpu.SMEM), block, block, block],
        out_specs=[block, pl.BlockSpec((1, PAIR, rows, rows), lambda s, p: (s, p, 0, 0))],
        out_shape=[
            jax.ShapeDtypeStruct((tokens, width), BF16),
            jax.ShapeDtypeStruct((seqs, pairs * PAIR, rows, rows), BF16),
        ],
        cost_estimate=pl.CostEstimate(
            flops=seqs * pairs * 12 * rows * rows * LANES,
            bytes_accessed=8 * tokens * width + 4 * tokens * rows * pairs,
            transcendentals=0,
        ),
    )(lengths, query, key, value)


def attend_back_kernel(
    query_ref, key_ref, value_ref, grad_ref, probs_ref, grad_q_ref, grad_k_ref, grad_v_ref
):
    query, value, grad = query_ref[...], value_ref[...], grad_ref[...]
    key_t = key_ref[...].T
    grad_key = grad_value = 0.0
    grad_query = []
    for head in range(PAIR):
        own_query = (head_lanes(query, head) * SCALE).astype(BF16)
        own_value = head_lanes(value, head).astype(BF16)
        own_grad = head_lanes(grad, head).astype(BF16)
        low = probs_ref[0, head]
        probs = low.astype(F32)
        grad_probs = dot_nt(own_value, grad)
        weighted = jnp.sum(probs * grad_probs, axis=0, keepdims=True)
        grad_scores = (probs * (grad_probs - weighted)).astype(BF16)
        grad_value += dot_nn(low, own_grad)
        grad_key += dot_nn(grad_scores, own_query)
        grad_query.append(dot_nn(key_t[head * HEAD_DIM : (head + 1) * HEAD_DIM], grad_scores))
    grad_q_ref[...] = (jnp.concatenate(grad_query, axis=0) * SCALE).T.astype(BF16)
    grad_k_ref[...] = grad_key.astype(BF16)
    grad_v_ref[...] = grad_value.astype(BF16)


def attend_back(query, key, value, grad_context, probs):
    seqs, _, rows, _ = probs.shape
    tokens, width = query.shape
    pairs = width // LANES
    block = pl.BlockSpec((rows, LANES), lambda s, p: (s, p))
    return pl.pallas_call(
        attend_back_kernel,
        grid=(seqs, pairs),
        in_specs=[block] * 4 + [pl.BlockSpec((1, PAIR, rows, rows), lambda s, p: (s, p, 0, 0))],
        out_specs=[block] * 3,
        out_shape=[jax.ShapeDtypeStruct((tokens, width), BF16)] * 3,
        cost_estimate=pl.CostEstimate(
            flops=seqs * pairs * 30 * rows * rows * LANES,
            bytes_accessed=14 * tokens * width + 4 * tokens * rows * pairs,
            transcendentals=0,
        ),
    )(query, key, value, grad_context, probs)


def gelu_parts(values):
    bell = jnp.exp(-0.5 * values * values)
    inner = 1.0 / (1.0 + (0.3275911 * 0.5**0.5) * jnp.abs(values))
    series = 0.5 * 1.061405429
    for term in (-1.453152027, 1.421413741, -0.284496736, 0.254829592):
        series = series * inner + 0.5 * term
    tail = series * inner * bell
    below = jnp.where(values < 0.0, tail, 1.0 - tail)
    return values * below, below + values * bell * 0.3989422804014327


FF_TILE = 512
ROW_TILE = 256


def feed_kernel(rows_ref, up_ref, up_bias_ref, down_ref, down_bias_ref, act_ref, slope_ref, out_ref):
    first = pl.program_id(0) == 0

    @pl.when(first)
    def _():
        out_ref[...] = jnp.broadcast_to(down_bias_ref[...], out_ref.shape)

    for start in range(0, rows_ref.shape[0], ROW_TILE):
        here = pl.ds(start, ROW_TILE)
        before = dot_nn(rows_ref[here, :], up_ref[...]) + up_bias_ref[...]
        active, slope = gelu_parts(before)
        active = active.astype(BF16)
        act_ref[here, :] = active
        slope_ref[here, :] = slope.astype(BF16)
        out_ref[here, :] += dot_nn(active, down_ref[...])


def feed_forward(rows, up_weight, up_bias, down_weight, down_bias):
    tokens, width = rows.shape
    units = up_weight.shape[1]
    whole = lambda shape: pl.BlockSpec(shape, lambda i: (0, 0))
    columns = lambda height: pl.BlockSpec((height, FF_TILE), lambda i: (0, i))
    return pl.pallas_call(
        feed_kernel,
        grid=(units // FF_TILE,),
        in_specs=[
            whole((tokens, width)),
            columns(width),
            columns(1),
            pl.BlockSpec((FF_TILE, width), lambda i: (i, 0)),
            whole((1, width)),
        ],
        out_specs=[columns(tokens), columns(tokens), whole((tokens, width))],
        out_shape=[
            jax.ShapeDtypeStruct((tokens, units), BF16),
            jax.ShapeDtypeStruct((tokens, units), BF16),
            jax.ShapeDtypeStruct((tokens, width), F32),
        ],
        cost_estimate=pl.CostEstimate(
            flops=8 * tokens * width * units,
            bytes_accessed=4 * tokens * units + 4 * width * units,
            transcendentals=0,
        ),
    )(rows, up_weight, up_bias[None], down_weight, down_bias[None])


def classify(cls_rows, labels, w_pool, b_pool, w_class, b_class):
    pooled = jnp.tanh(jnp.dot(cls_rows, w_pool, preferred_element_type=F32) + b_pool)
    class_weight = w_class.astype(F32)
    logits = jnp.dot(pooled, class_weight, precision=lax.Precision.HIGHEST) + b_class
    onehot = (labels[:, None] == jnp.arange(logits.shape[1])[None, :]).astype(F32)
    ramp_loss = jax.nn.logsumexp(logits, axis=-1) - jnp.sum(logits * onehot, axis=-1)
    grad_logits = jax.nn.softmax(logits, axis=-1) - onehot
    grad_pool = (
        jnp.dot(grad_logits, class_weight.T, precision=lax.Precision.HIGHEST)
        * (1.0 - pooled * pooled)
    ).astype(BF16)
    return pooled, ramp_loss, grad_logits, grad_pool


def body(
    hidden_in,
    lengths,
    labels,
    query_key_value_weight,
    query_value_bias,
    attention_output_weight,
    attention_output_bias,
    gain_att,
    shift_att,
    up_weight,
    up_bias,
    down_weight,
    down_bias,
    gain_ffn,
    shift_ffn,
    w_pool,
    b_pool,
    w_class,
    b_class,
    cotangent,
):
    seq_here, seq_len, width = hidden_in.shape
    tokens = seq_here * seq_len
    everyone = ("dp", "head")
    head_bits = bits_of(("head",))
    dp_bits = bits_of(("dp",))
    rows_in = hidden_in.reshape(tokens, width)

    half_bits, far_bit = head_bits[1:], head_bits[0]
    own_weight = jnp.transpose(query_key_value_weight, (2, 0, 1))
    own_weight = own_weight.transpose(1, 0, 2)
    far_weight = exchange(own_weight, *far_bit)
    far_bias = exchange(query_value_bias, *far_bit)
    low_order = list(reversed(half_bits))

    def join(blocks, order):
        for axis, bit in order:
            got = exchange(blocks, axis, bit)
            blocks = jnp.where(
                own_bit(axis, bit) == 0,
                jnp.concatenate([blocks, got], axis=1),
                jnp.concatenate([got, blocks], axis=1),
            )
        return blocks

    halves = []
    for weight, bias in ((own_weight, query_value_bias), (far_weight, far_bias)):
        weight, bias = join(weight, low_order), join(bias, low_order)
        query = (dot_nt(rows_in, weight[0]) + bias[0]).astype(BF16)
        key = dot_nt(rows_in, weight[1]).astype(BF16)
        value = (dot_nt(rows_in, weight[2]) + bias[1]).astype(BF16)
        context, probs = attend(lengths, query, key, value)
        halves.append((weight, query, key, value, context, probs))
    half_width = halves[0][1].shape[1]
    far_side = own_bit(*far_bit)

    def in_place(own, far, axis):
        return jnp.where(
            far_side == 0,
            jnp.concatenate([own, far], axis=axis),
            jnp.concatenate([far, own], axis=axis),
        )

    combined = in_place(halves[0][4], halves[1][4], 1)
    attended = (
        jnp.dot(combined, attention_output_weight, preferred_element_type=F32)
        + attention_output_bias
    )
    first_in = rows_in.astype(F32) + attended
    normalized_first = normalize(first_in, gain_att, shift_att)
    normed_low = normalized_first.astype(BF16)
    gelu_output, slope, branch = feed_forward(
        normed_low, up_weight, up_bias, down_weight, down_bias
    )
    second_in = normalized_first + branch
    output_rows = normalize(second_in, gain_ffn, shift_ffn)
    hidden_out = output_rows.astype(BF16).reshape(seq_here, seq_len, width)
    cls_rows = hidden_out[:, 0, :]
    _, ramp_loss, _, grad_pool_here = classify(cls_rows, labels, w_pool, b_pool, w_class, b_class)
    grad_cls = jnp.dot(grad_pool_here, w_pool.T, preferred_element_type=F32)

    gather_order = list(reversed(bits_of(everyone)))
    all_cls = gather_blocks(cls_rows, everyone, gather_order)
    all_labels = gather_blocks(labels, everyone, gather_order)
    pooled, _, grad_logits, grad_pool = classify(
        all_cls, all_labels, w_pool, b_pool, w_class, b_class
    )
    grad_b_class = jnp.sum(grad_logits, axis=0)
    grad_w_class = jnp.dot(pooled.T, grad_logits, precision=lax.Precision.HIGHEST)
    grad_b_pool = jnp.sum(grad_pool, axis=0, dtype=F32)
    grad_w_pool = jnp.dot(all_cls.T, grad_pool, preferred_element_type=F32)

    grad_output = cotangent.astype(F32).at[:, 0, :].add(grad_cls).reshape(tokens, width)
    _, second_back = jax.vjp(normalize, second_in, gain_ffn, shift_ffn)
    grad_second, grad_gain_ffn, grad_shift_ffn = second_back(grad_output)
    grad_branch = grad_second.astype(BF16)
    grad_b_down = jnp.sum(grad_branch, axis=0, dtype=F32)
    part_w_down = jnp.dot(gelu_output.T, grad_branch, preferred_element_type=F32).astype(BF16)
    grad_pre = (dot_nt(grad_branch, down_weight) * slope.astype(F32)).astype(BF16)
    grad_b_up = jnp.sum(grad_pre, axis=0, dtype=F32)
    part_w_up = jnp.dot(grad_pre.T, normed_low, preferred_element_type=F32).astype(BF16)

    order_down = list(reversed(head_bits)) + list(reversed(dp_bits))
    order_up = [head_bits[-1], dp_bits[-1]] + list(reversed(head_bits[:-1])) + list(reversed(dp_bits[:-1]))
    grad_w_down = scatter_sum(part_w_down, everyone, order_down)
    grad_w_up = scatter_sum(part_w_up, everyone, order_up).T

    grad_first = grad_second + jnp.dot(grad_pre, up_weight.T, preferred_element_type=F32)
    _, first_back = jax.vjp(normalize, first_in, gain_att, shift_att)
    grad_first_in, grad_gain_att, grad_shift_att = first_back(grad_first)
    grad_attended = grad_first_in.astype(BF16)
    grad_b_out = jnp.sum(grad_attended, axis=0, dtype=F32)
    part_w_out = jnp.dot(combined.T, grad_attended, preferred_element_type=F32).astype(BF16)
    own_w_out = scatter_sum(part_w_out, everyone, order_down)
    grad_w_out = gather_blocks(
        own_w_out.astype(BF16), everyone, list(reversed(order_down))
    ).astype(F32)
    grad_context = dot_nt(grad_attended, attention_output_weight).astype(BF16)
    far_context = lax.dynamic_slice_in_dim(
        grad_context, (1 - far_side) * half_width, half_width, 1
    )
    own_context = lax.dynamic_slice_in_dim(grad_context, far_side * half_width, half_width, 1)
    sums = all_sum(
        jnp.concatenate(
            [
                grad_b_out,
                grad_gain_att,
                grad_shift_att,
                grad_b_up,
                grad_b_down,
                grad_gain_ffn,
                grad_shift_ffn,
            ]
        ),
        everyone,
    )
    edges = [width, 2 * width, 3 * width, 3 * width + up_bias.shape[0]]
    edges += [edges[-1] + width, edges[-1] + 2 * width]
    (
        grad_b_out,
        grad_gain_att,
        grad_shift_att,
        grad_b_up,
        grad_b_down,
        grad_gain_ffn,
        grad_shift_ffn,
    ) = jnp.split(sums, edges)

    parts, shares, bias_parts = [], [], []
    for half, grad_half in ((halves[1], far_context), (halves[0], own_context)):
        weight, query, key, value, _, probs = half
        grads = attend_back(query, key, value, grad_half, probs)
        part = jnp.stack(
            [
                lax.dot_general(
                    grad, rows_in, (((0,), (0,)), ((), ())), preferred_element_type=F32
                ).astype(BF16)
                for grad in grads
            ]
        )
        own = part.shape[1] >> len(half_bits)
        part = part.reshape((3,) + (2,) * len(half_bits) + (own, width))
        for position, (axis, bit) in enumerate(half_bits):
            part = halve(part, 1 + position, axis, bit).astype(BF16)
        parts.append(part.reshape(3, own, width))
        bias_parts.append(jnp.stack([jnp.sum(grad, axis=0, dtype=F32) for grad in grads[::2]]))
        shares.append(sum(dot_nn(grad, w) for grad, w in zip(grads, weight)))
    crossed = exchange(parts[0], *far_bit)
    own_w_qkv = (parts[1].astype(F32) + crossed.astype(F32)).astype(BF16)
    local = own_w_qkv.shape[1]
    flat = own_w_qkv.reshape(3 * local, width)
    dp_order = list(reversed(dp_bits))
    own_flat = scatter_sum(flat, ("dp",), dp_order)
    flat = gather_blocks(own_flat.astype(BF16), ("dp",), list(reversed(dp_order)))
    grad_w_qkv = jnp.transpose(flat.reshape(3, local, width), (0, 2, 1)).astype(F32)
    bias_all = all_sum(in_place(bias_parts[1], bias_parts[0], 1), everyone)
    grad_b_qv = lax.dynamic_slice_in_dim(bias_all, lax.axis_index("head") * local, local, 1)
    grad_in = grad_first_in + shares[0] + shares[1]
    return (
        hidden_out,
        ramp_loss,
        grad_in.reshape(seq_here, seq_len, width),
        grad_w_qkv,
        grad_b_qv,
        grad_w_out,
        grad_b_out,
        grad_gain_att,
        grad_shift_att,
        grad_w_up,
        grad_b_up,
        grad_w_down,
        grad_b_down,
        grad_gain_ffn,
        grad_shift_ffn,
        grad_w_pool,
        grad_b_pool,
        grad_w_class,
        grad_b_class,
    )


def solution(mesh):
    rows = P(("dp", "head"))
    placed = (
        (P(("dp", "head"), None, None), rows, rows, P(None, None, "head"), P(None, "head"))
        + (P(),) * 14
        + (P(("dp", "head"), None, None),)
    )
    tokens = P(("dp", "head"), None, None)
    outs = (
        (tokens, rows, tokens, P(None, None, "head"), P(None, "head"))
        + (P(),) * 4
        + (P(None, ("dp", "head")), P(), P(("dp", "head"), None))
        + (P(),) * 7
    )
    return jax.shard_map(body, mesh=mesh, in_specs=placed, out_specs=outs, check_vma=False)
```

```python
import jax
import jax.numpy as jnp
from jax import lax
from jax.experimental import pallas as pl
from jax.experimental.pallas import tpu as pltpu
from jax.sharding import PartitionSpec as P

HEAD_DIM = 64
EPSILON = 1e-06
MASKED = -1000000000.0
BF16, F32 = jnp.bfloat16, jnp.float32


def bit_count(n):
    assert n & (n - 1) == 0
    return n.bit_length() - 1


def exchange(value, axis, bit):
    size = lax.axis_size(axis)
    step = 1 << bit
    return lax.ppermute(value, axis, [(i, i ^ step) for i in range(size)])


def own_bit(axis, bit):
    return (lax.axis_index(axis) >> bit) & 1


def bits_of(axes):
    found = []
    for axis in axes:
        found += [(axis, b) for b in reversed(range(bit_count(lax.axis_size(axis))))]
    return found


def normalize(row_block, gain_row, shift_row):
    center = jnp.mean(row_block, axis=-1, keepdims=True)
    centered = row_block - center
    spread = jnp.mean(centered * centered, axis=-1, keepdims=True)
    return centered * lax.rsqrt(spread + EPSILON) * gain_row + shift_row


LANES = 128
PAIR = LANES // HEAD_DIM
SCALE = HEAD_DIM ** (-0.5)


def dot_nt(left, right):
    return lax.dot_general(left, right, (((1,), (1,)), ((), ())), preferred_element_type=F32)


def dot_nn(left, right):
    return jnp.dot(left, right, preferred_element_type=F32)


def head_lanes(block, head):
    lane = lax.broadcasted_iota(jnp.int32, block.shape, 1)
    inside = (lane >= head * HEAD_DIM) & (lane < (head + 1) * HEAD_DIM)
    return jnp.where(inside, block.astype(F32), 0.0)


def attend_kernel(length_ref, query_ref, key_ref, value_ref, context_ref, probs_ref):
    length = length_ref[pl.program_id(0)]
    query, key = query_ref[...], key_ref[...]
    value_t = value_ref[...].T
    rows = query.shape[0]
    key_at = lax.broadcasted_iota(jnp.int32, (rows, rows), 0)
    contexts = []
    for head in range(PAIR):
        own_query = (head_lanes(query, head) * SCALE).astype(BF16)
        scores = jnp.where(key_at < length, dot_nt(key, own_query), MASKED)
        shifted = jnp.exp(scores - jnp.max(scores, axis=0, keepdims=True))
        inverse = 1.0 / jnp.sum(shifted, axis=0, keepdims=True)
        probs = (shifted * inverse).astype(BF16)
        probs_ref[0, head] = probs
        contexts.append(dot_nn(value_t[head * HEAD_DIM : (head + 1) * HEAD_DIM], probs))
    context_ref[...] = jnp.concatenate(contexts, axis=0).T.astype(BF16)


def attend(lengths, query, key, value):
    seqs = lengths.shape[0]
    tokens, width = query.shape
    rows, pairs = tokens // seqs, width // LANES
    block = pl.BlockSpec((rows, LANES), lambda s, p: (s, p))
    return pl.pallas_call(
        attend_kernel,
        grid=(seqs, pairs),
        in_specs=[pl.BlockSpec(memory_space=pltpu.SMEM), block, block, block],
        out_specs=[block, pl.BlockSpec((1, PAIR, rows, rows), lambda s, p: (s, p, 0, 0))],
        out_shape=[
            jax.ShapeDtypeStruct((tokens, width), BF16),
            jax.ShapeDtypeStruct((seqs, pairs * PAIR, rows, rows), BF16),
        ],
        cost_estimate=pl.CostEstimate(
            flops=seqs * pairs * 12 * rows * rows * LANES,
            bytes_accessed=8 * tokens * width + 4 * tokens * rows * pairs,
            transcendentals=0,
        ),
    )(lengths, query, key, value)


def attend_back_kernel(
    query_ref, key_ref, value_ref, grad_ref, probs_ref, grad_q_ref, grad_k_ref, grad_v_ref
):
    query, value, grad = query_ref[...], value_ref[...], grad_ref[...]
    key_t = key_ref[...].T
    grad_key = grad_value = 0.0
    grad_query = []
    for head in range(PAIR):
        own_query = (head_lanes(query, head) * SCALE).astype(BF16)
        own_value = head_lanes(value, head).astype(BF16)
        own_grad = head_lanes(grad, head).astype(BF16)
        low = probs_ref[0, head]
        probs = low.astype(F32)
        grad_probs = dot_nt(own_value, grad)
        weighted = jnp.sum(probs * grad_probs, axis=0, keepdims=True)
        grad_scores = (probs * (grad_probs - weighted)).astype(BF16)
        grad_value += dot_nn(low, own_grad)
        grad_key += dot_nn(grad_scores, own_query)
        grad_query.append(dot_nn(key_t[head * HEAD_DIM : (head + 1) * HEAD_DIM], grad_scores))
    grad_q_ref[...] = (jnp.concatenate(grad_query, axis=0) * SCALE).T.astype(BF16)
    grad_k_ref[...] = grad_key.astype(BF16)
    grad_v_ref[...] = grad_value.astype(BF16)


def attend_back(query, key, value, grad_context, probs):
    seqs, _, rows, _ = probs.shape
    tokens, width = query.shape
    pairs = width // LANES
    block = pl.BlockSpec((rows, LANES), lambda s, p: (s, p))
    return pl.pallas_call(
        attend_back_kernel,
        grid=(seqs, pairs),
        in_specs=[block] * 4 + [pl.BlockSpec((1, PAIR, rows, rows), lambda s, p: (s, p, 0, 0))],
        out_specs=[block] * 3,
        out_shape=[jax.ShapeDtypeStruct((tokens, width), BF16)] * 3,
        cost_estimate=pl.CostEstimate(
            flops=seqs * pairs * 30 * rows * rows * LANES,
            bytes_accessed=14 * tokens * width + 4 * tokens * rows * pairs,
            transcendentals=0,
        ),
    )(query, key, value, grad_context, probs)


def gelu_parts(values):
    bell = jnp.exp(-0.5 * values * values)
    inner = 1.0 / (1.0 + (0.3275911 * 0.5**0.5) * jnp.abs(values))
    series = 0.5 * 1.061405429
    for term in (-1.453152027, 1.421413741, -0.284496736, 0.254829592):
        series = series * inner + 0.5 * term
    tail = series * inner * bell
    below = jnp.where(values < 0.0, tail, 1.0 - tail)
    return values * below, below + values * bell * 0.3989422804014327


FF_TILE = 512
ROW_TILE = 256


def feed_kernel(rows_ref, up_ref, up_bias_ref, down_ref, down_bias_ref, act_ref, slope_ref, out_ref):
    first = pl.program_id(0) == 0

    @pl.when(first)
    def _():
        out_ref[...] = jnp.broadcast_to(down_bias_ref[...], out_ref.shape)

    for start in range(0, rows_ref.shape[0], ROW_TILE):
        here = pl.ds(start, ROW_TILE)
        before = dot_nn(rows_ref[here, :], up_ref[...]) + up_bias_ref[...]
        active, slope = gelu_parts(before)
        active = active.astype(BF16)
        act_ref[here, :] = active
        slope_ref[here, :] = slope.astype(BF16)
        out_ref[here, :] += dot_nn(active, down_ref[...])


def feed_forward(rows, up_weight, up_bias, down_weight, down_bias):
    tokens, width = rows.shape
    units = up_weight.shape[1]
    whole = lambda shape: pl.BlockSpec(shape, lambda i: (0, 0))
    columns = lambda height: pl.BlockSpec((height, FF_TILE), lambda i: (0, i))
    return pl.pallas_call(
        feed_kernel,
        grid=(units // FF_TILE,),
        in_specs=[
            whole((tokens, width)),
            columns(width),
            columns(1),
            pl.BlockSpec((FF_TILE, width), lambda i: (i, 0)),
            whole((1, width)),
        ],
        out_specs=[columns(tokens), columns(tokens), whole((tokens, width))],
        out_shape=[
            jax.ShapeDtypeStruct((tokens, units), BF16),
            jax.ShapeDtypeStruct((tokens, units), BF16),
            jax.ShapeDtypeStruct((tokens, width), F32),
        ],
        cost_estimate=pl.CostEstimate(
            flops=8 * tokens * width * units,
            bytes_accessed=4 * tokens * units + 4 * width * units,
            transcendentals=0,
        ),
    )(rows, up_weight, up_bias[None], down_weight, down_bias[None])


MESH = pl.DeviceIdType.MESH


def mine_of(axis, bit):
    return lax.rem(lax.div(lax.axis_index(axis), 1 << bit), 2)


def partner_of(axis, bit):
    return {axis: lax.axis_index(axis) + (1 << bit) * (1 - 2 * mine_of(axis, bit))}


def place_of(bits):
    place = 0
    for axis, bit in bits:
        place = 2 * place + mine_of(axis, bit)
    return place


def greet(bits):
    barrier = pltpu.get_barrier_semaphore()
    for axis, bit in bits:
        pl.semaphore_signal(
            barrier, inc=1, device_id=partner_of(axis, bit), device_id_type=MESH
        )
    pl.semaphore_wait(barrier, len(bits))


def copy_to(source, target, sems, bit):
    return pltpu.make_async_remote_copy(
        src_ref=source,
        dst_ref=target,
        send_sem=sems.at[0],
        recv_sem=sems.at[1],
        device_id=partner_of(*bit),
        device_id_type=MESH,
    )


class Scatter:
    def __init__(self, shape, lanes, joint, order, near=()):
        self.shape, self.lanes, self.joint, self.order, self.near = shape, lanes, joint, order, near

    def scratch(self):
        blocks, rows, _ = self.shape
        width = self.lanes[1]
        found = []
        for _ in self.order:
            blocks //= 2
            found.append(pltpu.VMEM((blocks, rows, width), BF16))
        return found + [pltpu.SemaphoreType.DMA((len(self.order), 2))]

    def bind(self, source, scratch, finish):
        self.source, self.slots, self.sems, self.last = source, scratch[:-1], scratch[-1], finish
        return self

    def split(self, stage):
        left = [bit for bit in self.joint if bit not in self.order[:stage]]
        place = left.index(self.order[stage])
        high, low = 1 << place, 1 << (len(left) - place - 1)
        side = 0 if self.order[stage] in self.near else mine_of(*self.order[stage])
        return high, low, side

    def view(self, stage, at):
        if stage == 0:
            return self.source.at[at, :, pl.ds(*self.lanes)]
        return self.slots[stage - 1].at[at]

    def steps(self):
        return len(self.order)

    def start(self, stage):
        high, low, side = self.split(stage)

        def send(run, carry):
            copy_to(
                self.view(stage, pl.ds((2 * run + 1 - side) * low, low)),
                self.slots[stage].at[pl.ds(run * low, low)],
                self.sems.at[stage],
                self.order[stage],
            ).start()
            return carry

        lax.fori_loop(0, high, send, 0)

    def whole(self, stage):
        slot = self.slots[stage]
        return copy_to(slot, slot, self.sems.at[stage], self.order[stage])

    def finish(self, stage):
        high, low, side = self.split(stage)
        slot = self.slots[stage]
        self.whole(stage).wait_recv()

        def total(index):
            kept = (2 * lax.div(index, low) + side) * low + lax.rem(index, low)
            return self.view(stage, kept)[...].astype(F32) + slot[index].astype(F32)

        if stage + 1 == len(self.order):
            self.last(total(0))
            return

        def add(index, carry):
            slot[index] = total(index).astype(BF16)
            return carry

        lax.fori_loop(0, high * low, add, 0)

    def drain(self):
        for stage in range(len(self.order)):
            self.whole(stage).wait_send()


class Gather:
    def __init__(self, shape, dtype, order):
        self.shape, self.dtype, self.order = shape, dtype, order

    def scratch(self):
        return [
            pltpu.VMEM((1 << len(self.order),) + self.shape, self.dtype),
            pltpu.SemaphoreType.DMA((len(self.order), 2)),
        ]

    def bind(self, scratch):
        self.buffer, self.sems = scratch
        self.place = place_of(list(reversed(self.order)))
        return self

    def steps(self):
        return len(self.order)

    def copy(self, stage, theirs):
        run = 1 << stage
        base = lax.div(self.place, run) * run
        if theirs:
            base = base + run * (1 - 2 * mine_of(*self.order[stage]))
        here = self.buffer.at[pl.ds(base, run)]
        return copy_to(here, here, self.sems.at[stage], self.order[stage])

    def start(self, stage):
        self.copy(stage, False).start()

    def finish(self, stage):
        self.copy(stage, True).wait_recv()

    def drain(self):
        for stage in range(len(self.order)):
            self.copy(stage, False).wait_send()

    def natural(self, position, bits):
        index = 0
        for bit in bits:
            index = 2 * index + lax.rem(lax.div(position, 1 << self.order.index(bit)), 2)
        return index


class Total:
    def __init__(self, shape, order):
        self.shape, self.order = shape, order

    def scratch(self):
        return [
            pltpu.VMEM((len(self.order) + 1,) + self.shape, F32),
            pltpu.VMEM((len(self.order),) + self.shape, F32),
            pltpu.SemaphoreType.DMA((len(self.order), 2)),
        ]

    def bind(self, scratch):
        self.held, self.slots, self.sems = scratch
        return self

    def steps(self):
        return len(self.order)

    def copy(self, stage):
        return copy_to(
            self.held.at[stage], self.slots.at[stage], self.sems.at[stage], self.order[stage]
        )

    def start(self, stage):
        self.copy(stage).start()

    def finish(self, stage):
        self.copy(stage).wait_recv()
        self.held[stage + 1] = self.held[stage] + self.slots[stage]

    def drain(self):
        for stage in range(len(self.order)):
            self.copy(stage).wait_send()


def take(scratch, chain):
    count = len(chain.scratch())
    return [scratch.pop(0) for _ in range(count)]


def run_chains(chains):
    for chain in chains:
        chain[0][0](chain[0][1])
    for turn in range(max(len(chain) for chain in chains)):
        for chain in chains:
            if turn < len(chain):
                chain[turn][2](chain[turn][1])
                if turn + 1 < len(chain):
                    chain[turn + 1][0](chain[turn + 1][1])


def stages(transfer):
    return [(transfer.start, stage, transfer.finish) for stage in range(transfer.steps())]


def reduce_all(head_bits, dp_bits, down, up, out, qkv, vector, cls):
    joint = dp_bits + head_bits
    low_head, low_dp = list(reversed(head_bits)), list(reversed(dp_bits))
    order = (
        low_head + low_dp,
        low_head[:-1] + low_dp[:1] + low_head[-1:] + low_dp[1:],
    )
    near = head_bits[:1]
    half = down.shape[2] // 2
    lanes = ((0, half), (half, half))
    large = [Scatter(a.shape, lanes[i], joint, order[i]) for a in (down, up) for i in range(2)]
    middle = [Scatter(out.shape, lanes[i], joint, order[i]) for i in range(2)]
    later = [Scatter(qkv.shape, lanes[i], head_bits + dp_bits, order[i], near) for i in range(2)]
    out_back = [Gather((out.shape[1], half), BF16, order[i][::-1]) for i in range(2)]
    qkv_back = [Gather((qkv.shape[1], half), BF16, dp_bits) for i in range(2)]
    small = Total(vector.shape, order[0])
    rows = Gather(cls.shape, F32, order[0][::-1])
    everything = large + middle + later + out_back + qkv_back + [small, rows]

    def kernel(down_ref, up_ref, out_ref, qkv_ref, vector_ref, cls_ref, *rest):
        results, scratch = rest[:6], list(rest[6:])
        bound = [take(scratch, t) for t in everything]
        down_sum, up_sum, out_sum, qkv_sum, vector_sum, cls_all = results
        greet(joint)

        def keep(target, lane):
            def store(total):
                target[:, pl.ds(*lane)] = total

            return store

        def hand_on(gather):
            def store(total):
                gather.buffer[gather.place] = total.astype(BF16)

            return store

        def spread(gather, target, bits, lane):
            def move(position, carry):
                target[gather.natural(position, bits), :, pl.ds(*lane)] = gather.buffer[
                    position
                ].astype(F32)
                return carry

            lax.fori_loop(0, gather.buffer.shape[0], move, 0)

        large_b, middle_b, later_b = bound[:4], bound[4:6], bound[6:8]
        out_b, qkv_b = bound[8:10], bound[10:12]
        for g, own in zip(out_back + qkv_back, out_b + qkv_b):
            g.bind(own)
        for i, t in enumerate(large):
            t.bind((down_ref, up_ref)[i // 2], large_b[i], keep((down_sum, up_sum)[i // 2], lanes[i % 2]))
        for i in range(2):
            middle[i].bind(out_ref, middle_b[i], hand_on(out_back[i]))
            later[i].bind(qkv_ref, later_b[i], hand_on(qkv_back[i]))
        small.bind(bound[12])
        rows.bind(bound[13])
        small.held[0] = vector_ref[...]
        rows.buffer[rows.place] = cls_ref[...]
        chains = [stages(later[i]) + stages(qkv_back[i]) for i in range(2)]
        chains += [stages(middle[i]) + stages(out_back[i]) for i in range(2)]
        chains += [stages(t) for t in large]
        chains += [stages(small), stages(rows)]
        run_chains(chains)
        for i in range(2):
            spread(out_back[i], out_sum, joint, lanes[i])
            spread(qkv_back[i], qkv_sum, dp_bits, lanes[i])
        vector_sum[...] = small.held[len(small.order)]

        def lift(position, carry):
            cls_all[rows.natural(position, joint)] = rows.buffer[position]
            return carry

        lax.fori_loop(0, rows.buffer.shape[0], lift, 0)
        for t in everything:
            t.drain()

    blocks = 1 << len(joint)
    dp_blocks = 1 << len(dp_bits)
    return pl.pallas_call(
        kernel,
        in_specs=[pl.BlockSpec(memory_space=pltpu.VMEM)] * 6,
        out_specs=[pl.BlockSpec(memory_space=pltpu.VMEM)] * 6,
        out_shape=[
            jax.ShapeDtypeStruct(down.shape[1:], F32),
            jax.ShapeDtypeStruct(up.shape[1:], F32),
            jax.ShapeDtypeStruct(out.shape, F32),
            jax.ShapeDtypeStruct((dp_blocks,) + qkv.shape[1:], F32),
            jax.ShapeDtypeStruct(vector.shape, F32),
            jax.ShapeDtypeStruct((blocks,) + cls.shape, F32),
        ],
        scratch_shapes=[x for t in everything for x in t.scratch()],
        compiler_params=pltpu.CompilerParams(
            collective_id=0, has_side_effects=True, vmem_limit_bytes=60 * 1024 * 1024
        ),
    )(down, up, out, qkv, vector, cls)


def classify(cls_rows, labels, w_pool, b_pool, w_class, b_class):
    pooled = jnp.tanh(jnp.dot(cls_rows, w_pool, preferred_element_type=F32) + b_pool)
    class_weight = w_class.astype(F32)
    logits = jnp.dot(pooled, class_weight, precision=lax.Precision.HIGHEST) + b_class
    onehot = (labels[:, None] == jnp.arange(logits.shape[1])[None, :]).astype(F32)
    ramp_loss = jax.nn.logsumexp(logits, axis=-1) - jnp.sum(logits * onehot, axis=-1)
    grad_logits = jax.nn.softmax(logits, axis=-1) - onehot
    grad_pool = (
        jnp.dot(grad_logits, class_weight.T, precision=lax.Precision.HIGHEST)
        * (1.0 - pooled * pooled)
    ).astype(BF16)
    return pooled, ramp_loss, grad_logits, grad_pool


def body(
    hidden_in,
    lengths,
    labels,
    query_key_value_weight,
    query_value_bias,
    attention_output_weight,
    attention_output_bias,
    gain_att,
    shift_att,
    up_weight,
    up_bias,
    down_weight,
    down_bias,
    gain_ffn,
    shift_ffn,
    w_pool,
    b_pool,
    w_class,
    b_class,
    cotangent,
):
    seq_here, seq_len, width = hidden_in.shape
    tokens = seq_here * seq_len
    everyone = ("dp", "head")
    head_bits = bits_of(("head",))
    dp_bits = bits_of(("dp",))
    rows_in = hidden_in.reshape(tokens, width)

    half_bits, far_bit = head_bits[1:], head_bits[0]
    own_weight = jnp.transpose(query_key_value_weight, (2, 0, 1))
    own_weight = own_weight.transpose(1, 0, 2)
    far_weight = exchange(own_weight, *far_bit)
    far_bias = exchange(query_value_bias, *far_bit)
    low_order = list(reversed(half_bits))

    def join(blocks, order):
        for axis, bit in order:
            got = exchange(blocks, axis, bit)
            blocks = jnp.where(
                own_bit(axis, bit) == 0,
                jnp.concatenate([blocks, got], axis=1),
                jnp.concatenate([got, blocks], axis=1),
            )
        return blocks

    halves = []
    for weight, bias in ((own_weight, query_value_bias), (far_weight, far_bias)):
        weight, bias = join(weight, low_order), join(bias, low_order)
        query = (dot_nt(rows_in, weight[0]) + bias[0]).astype(BF16)
        key = dot_nt(rows_in, weight[1]).astype(BF16)
        value = (dot_nt(rows_in, weight[2]) + bias[1]).astype(BF16)
        context, probs = attend(lengths, query, key, value)
        halves.append((weight, query, key, value, context, probs))
    half_width = halves[0][1].shape[1]
    far_side = own_bit(*far_bit)

    def in_place(own, far, axis):
        return jnp.where(
            far_side == 0,
            jnp.concatenate([own, far], axis=axis),
            jnp.concatenate([far, own], axis=axis),
        )

    combined = in_place(halves[0][4], halves[1][4], 1)
    attended = (
        jnp.dot(combined, attention_output_weight, preferred_element_type=F32)
        + attention_output_bias
    )
    first_in = rows_in.astype(F32) + attended
    normalized_first = normalize(first_in, gain_att, shift_att)
    normed_low = normalized_first.astype(BF16)
    gelu_output, slope, branch = feed_forward(
        normed_low, up_weight, up_bias, down_weight, down_bias
    )
    second_in = normalized_first + branch
    output_rows = normalize(second_in, gain_ffn, shift_ffn)
    hidden_out = output_rows.astype(BF16).reshape(seq_here, seq_len, width)
    cls_rows = hidden_out[:, 0, :]
    pooled, ramp_loss, grad_logits, grad_pool = classify(
        cls_rows, labels, w_pool, b_pool, w_class, b_class
    )
    grad_cls = jnp.dot(grad_pool, w_pool.T, preferred_element_type=F32)
    classes = grad_logits.shape[1]
    cls_pack = jnp.concatenate(
        [
            cls_rows.astype(F32),
            grad_pool.astype(F32),
            pooled,
            jnp.pad(grad_logits, ((0, 0), (0, LANES - classes))),
        ],
        axis=1,
    )
    pack_width = cls_pack.shape[1]
    cls_pack = cls_pack.reshape(-1, LANES)

    grad_output = cotangent.astype(F32).at[:, 0, :].add(grad_cls).reshape(tokens, width)
    _, second_back = jax.vjp(normalize, second_in, gain_ffn, shift_ffn)
    grad_second, grad_gain_ffn, grad_shift_ffn = second_back(grad_output)
    grad_branch = grad_second.astype(BF16)
    grad_b_down = jnp.sum(grad_branch, axis=0, dtype=F32)
    part_w_down = jnp.dot(gelu_output.T, grad_branch, preferred_element_type=F32).astype(BF16)
    grad_pre = (dot_nt(grad_branch, down_weight) * slope.astype(F32)).astype(BF16)
    grad_b_up = jnp.sum(grad_pre, axis=0, dtype=F32)
    part_w_up = jnp.dot(grad_pre.T, normed_low, preferred_element_type=F32).astype(BF16)

    grad_first = grad_second + jnp.dot(grad_pre, up_weight.T, preferred_element_type=F32)
    _, first_back = jax.vjp(normalize, first_in, gain_att, shift_att)
    grad_first_in, grad_gain_att, grad_shift_att = first_back(grad_first)
    grad_attended = grad_first_in.astype(BF16)
    grad_b_out = jnp.sum(grad_attended, axis=0, dtype=F32)
    part_w_out = jnp.dot(combined.T, grad_attended, preferred_element_type=F32).astype(BF16)
    grad_context = dot_nt(grad_attended, attention_output_weight).astype(BF16)
    far_context = lax.dynamic_slice_in_dim(
        grad_context, (1 - far_side) * half_width, half_width, 1
    )
    own_context = lax.dynamic_slice_in_dim(grad_context, far_side * half_width, half_width, 1)
    parts, shares, bias_parts = [], [], []
    for half, grad_half in ((halves[1], far_context), (halves[0], own_context)):
        weight, query, key, value, _, probs = half
        grads = attend_back(query, key, value, grad_half, probs)
        part = jnp.stack(
            [
                lax.dot_general(
                    grad, rows_in, (((0,), (0,)), ((), ())), preferred_element_type=F32
                ).astype(BF16)
                for grad in grads
            ]
        )
        own = part.shape[1] >> len(half_bits)
        part = part.reshape(3, -1, own, width).transpose(1, 0, 2, 3)
        parts.append(part)
        bias_parts.append(jnp.stack([jnp.sum(grad, axis=0, dtype=F32) for grad in grads[::2]]))
        shares.append(sum(dot_nn(grad, w) for grad, w in zip(grads, weight)))
    local = query_key_value_weight.shape[2]
    dp_size = lax.axis_size("dp")
    devices = dp_size * lax.axis_size("head")
    qkv = jnp.concatenate([parts[1], parts[0]]).reshape(
        devices, 3 * local // dp_size, width
    )
    bias_parts = in_place(bias_parts[1], bias_parts[0], 1)
    vectors = [
        grad_b_out,
        grad_gain_att,
        grad_shift_att,
        grad_b_up,
        grad_b_down,
        grad_gain_ffn,
        grad_shift_ffn,
        bias_parts.reshape(-1),
    ]
    grad_w_down, grad_w_up, grad_w_out, qkv, sums, cls_all = reduce_all(
        head_bits,
        dp_bits,
        part_w_down.reshape(devices, -1, width),
        part_w_up.reshape(devices, -1, width),
        part_w_out.reshape(devices, -1, width),
        qkv,
        jnp.concatenate(vectors).reshape(-1, LANES),
        cls_pack,
    )
    grad_w_up = grad_w_up.T
    grad_w_out = grad_w_out.reshape(width, width)
    grad_w_qkv = jnp.transpose(qkv.reshape(3, local, width), (0, 2, 1))
    edges, reached = [], 0
    for vector in vectors[:-1]:
        reached += vector.shape[0]
        edges.append(reached)
    (
        grad_b_out,
        grad_gain_att,
        grad_shift_att,
        grad_b_up,
        grad_b_down,
        grad_gain_ffn,
        grad_shift_ffn,
        bias_all,
    ) = jnp.split(sums.reshape(-1), edges)
    grad_b_qv = lax.dynamic_slice_in_dim(
        bias_all.reshape(2, width), lax.axis_index("head") * local, local, 1
    )
    cls_all = cls_all.reshape(-1, pack_width)
    all_cls, all_pool, pooled = jnp.split(cls_all[:, : 3 * width], 3, axis=1)
    grad_logits = cls_all[:, 3 * width : 3 * width + classes]
    grad_b_class = jnp.sum(grad_logits, axis=0)
    grad_w_class = jnp.dot(pooled.T, grad_logits, precision=lax.Precision.HIGHEST)
    grad_b_pool = jnp.sum(all_pool, axis=0)
    grad_w_pool = jnp.dot(
        all_cls.T.astype(BF16), all_pool.astype(BF16), preferred_element_type=F32
    )
    grad_in = grad_first_in + shares[0] + shares[1]
    return (
        hidden_out,
        ramp_loss,
        grad_in.reshape(seq_here, seq_len, width),
        grad_w_qkv,
        grad_b_qv,
        grad_w_out,
        grad_b_out,
        grad_gain_att,
        grad_shift_att,
        grad_w_up,
        grad_b_up,
        grad_w_down,
        grad_b_down,
        grad_gain_ffn,
        grad_shift_ffn,
        grad_w_pool,
        grad_b_pool,
        grad_w_class,
        grad_b_class,
    )


def solution(mesh):
    rows = P(("dp", "head"))
    placed = (
        (P(("dp", "head"), None, None), rows, rows, P(None, None, "head"), P(None, "head"))
        + (P(),) * 14
        + (P(("dp", "head"), None, None),)
    )
    tokens = P(("dp", "head"), None, None)
    outs = (
        (tokens, rows, tokens, P(None, None, "head"), P(None, "head"))
        + (P(),) * 4
        + (P(None, ("dp", "head")), P(), P(("dp", "head"), None))
        + (P(),) * 7
    )
    return jax.shard_map(body, mesh=mesh, in_specs=placed, out_specs=outs, check_vma=False)
```

```python
import jax
import jax.numpy as jnp
from jax import lax
from jax.experimental import pallas as pl
from jax.experimental.pallas import tpu as pltpu
from jax.sharding import PartitionSpec as P

HEAD_DIM = 64
EPSILON = 1e-06
MASKED = -1000000000.0
BF16, F32 = jnp.bfloat16, jnp.float32


def bit_count(n):
    assert n & (n - 1) == 0
    return n.bit_length() - 1


def exchange(value, axis, bit):
    size = lax.axis_size(axis)
    step = 1 << bit
    return lax.ppermute(value, axis, [(i, i ^ step) for i in range(size)])


def own_bit(axis, bit):
    return (lax.axis_index(axis) >> bit) & 1


def bits_of(axes):
    found = []
    for axis in axes:
        found += [(axis, b) for b in reversed(range(bit_count(lax.axis_size(axis))))]
    return found


def normalize(row_block, gain_row, shift_row):
    center = jnp.mean(row_block, axis=-1, keepdims=True)
    centered = row_block - center
    spread = jnp.mean(centered * centered, axis=-1, keepdims=True)
    return centered * lax.rsqrt(spread + EPSILON) * gain_row + shift_row


LANES = 128
PAIR = LANES // HEAD_DIM
SCALE = HEAD_DIM ** (-0.5)


def dot_nt(left, right):
    return lax.dot_general(left, right, (((1,), (1,)), ((), ())), preferred_element_type=F32)


def dot_nn(left, right):
    return jnp.dot(left, right, preferred_element_type=F32)


def head_lanes(block, head):
    lane = lax.broadcasted_iota(jnp.int32, block.shape, 1)
    inside = (lane >= head * HEAD_DIM) & (lane < (head + 1) * HEAD_DIM)
    return jnp.where(inside, block.astype(F32), 0.0)


def attend_kernel(length_ref, query_ref, key_ref, value_ref, context_ref, probs_ref):
    length = length_ref[pl.program_id(0)]
    query, key = query_ref[...], key_ref[...]
    value_t = value_ref[...].T
    rows = query.shape[0]
    key_at = lax.broadcasted_iota(jnp.int32, (rows, rows), 0)
    contexts = []
    for head in range(PAIR):
        own_query = (head_lanes(query, head) * SCALE).astype(BF16)
        scores = jnp.where(key_at < length, dot_nt(key, own_query), MASKED)
        shifted = jnp.exp(scores - jnp.max(scores, axis=0, keepdims=True))
        inverse = 1.0 / jnp.sum(shifted, axis=0, keepdims=True)
        probs = (shifted * inverse).astype(BF16)
        probs_ref[0, head] = probs
        contexts.append(dot_nn(value_t[head * HEAD_DIM : (head + 1) * HEAD_DIM], probs))
    context_ref[...] = jnp.concatenate(contexts, axis=0).T.astype(BF16)


def attend(lengths, query, key, value):
    seqs = lengths.shape[0]
    tokens, width = query.shape
    rows, pairs = tokens // seqs, width // LANES
    block = pl.BlockSpec((rows, LANES), lambda s, p: (s, p))
    return pl.pallas_call(
        attend_kernel,
        grid=(seqs, pairs),
        in_specs=[pl.BlockSpec(memory_space=pltpu.SMEM), block, block, block],
        out_specs=[block, pl.BlockSpec((1, PAIR, rows, rows), lambda s, p: (s, p, 0, 0))],
        out_shape=[
            jax.ShapeDtypeStruct((tokens, width), BF16),
            jax.ShapeDtypeStruct((seqs, pairs * PAIR, rows, rows), BF16),
        ],
        cost_estimate=pl.CostEstimate(
            flops=seqs * pairs * 12 * rows * rows * LANES,
            bytes_accessed=8 * tokens * width + 4 * tokens * rows * pairs,
            transcendentals=0,
        ),
    )(lengths, query, key, value)


def gelu_parts(values):
    bell = jnp.exp(-0.5 * values * values)
    inner = 1.0 / (1.0 + (0.3275911 * 0.5**0.5) * jnp.abs(values))
    series = 0.5 * 1.061405429
    for term in (-1.453152027, 1.421413741, -0.284496736, 0.254829592):
        series = series * inner + 0.5 * term
    tail = series * inner * bell
    below = jnp.where(values < 0.0, tail, 1.0 - tail)
    return values * below, below + values * bell * 0.3989422804014327


FF_TILE = 512
ROW_TILE = 256


def feed_kernel(rows_ref, up_ref, up_bias_ref, down_ref, down_bias_ref, act_ref, slope_ref, out_ref):
    first = pl.program_id(0) == 0

    @pl.when(first)
    def _():
        out_ref[...] = jnp.broadcast_to(down_bias_ref[...], out_ref.shape)

    for start in range(0, rows_ref.shape[0], ROW_TILE):
        here = pl.ds(start, ROW_TILE)
        before = dot_nn(rows_ref[here, :], up_ref[...]) + up_bias_ref[...]
        active, slope = gelu_parts(before)
        active = active.astype(BF16)
        act_ref[here, :] = active
        slope_ref[here, :] = slope.astype(BF16)
        out_ref[here, :] += dot_nn(active, down_ref[...])


def feed_forward(rows, up_weight, up_bias, down_weight, down_bias):
    tokens, width = rows.shape
    units = up_weight.shape[1]
    whole = lambda shape: pl.BlockSpec(shape, lambda i: (0, 0))
    columns = lambda height: pl.BlockSpec((height, FF_TILE), lambda i: (0, i))
    return pl.pallas_call(
        feed_kernel,
        grid=(units // FF_TILE,),
        in_specs=[
            whole((tokens, width)),
            columns(width),
            columns(1),
            pl.BlockSpec((FF_TILE, width), lambda i: (i, 0)),
            whole((1, width)),
        ],
        out_specs=[columns(tokens), columns(tokens), whole((tokens, width))],
        out_shape=[
            jax.ShapeDtypeStruct((tokens, units), BF16),
            jax.ShapeDtypeStruct((tokens, units), BF16),
            jax.ShapeDtypeStruct((tokens, width), F32),
        ],
        cost_estimate=pl.CostEstimate(
            flops=8 * tokens * width * units,
            bytes_accessed=4 * tokens * units + 4 * width * units,
            transcendentals=0,
        ),
    )(rows, up_weight, up_bias[None], down_weight, down_bias[None])


MESH = pl.DeviceIdType.MESH


def mine_of(axis, bit):
    return lax.rem(lax.div(lax.axis_index(axis), 1 << bit), 2)


def partner_of(axis, bit):
    return {axis: lax.axis_index(axis) + (1 << bit) * (1 - 2 * mine_of(axis, bit))}


def place_of(bits):
    place = 0
    for axis, bit in bits:
        place = 2 * place + mine_of(axis, bit)
    return place


def greet(bits):
    barrier = pltpu.get_barrier_semaphore()
    for axis, bit in bits:
        pl.semaphore_signal(
            barrier, inc=1, device_id=partner_of(axis, bit), device_id_type=MESH
        )
    pl.semaphore_wait(barrier, len(bits))


def copy_to(source, target, sems, bit):
    return pltpu.make_async_remote_copy(
        src_ref=source,
        dst_ref=target,
        send_sem=sems.at[0],
        recv_sem=sems.at[1],
        device_id=partner_of(*bit),
        device_id_type=MESH,
    )


class Scatter:
    def __init__(self, shape, lanes, joint, order):
        self.shape, self.lanes, self.joint, self.order = shape, lanes, joint, order

    def blocks(self, stage):
        halved = len([bit for bit in self.order[:stage] if bit in self.joint])
        return self.shape[0] >> halved

    def scratch(self):
        rows, width = self.shape[1], self.lanes[1]
        return [
            pltpu.VMEM((self.blocks(stage + 1), rows, width), BF16)
            for stage in range(len(self.order))
        ] + [pltpu.SemaphoreType.DMA((len(self.order), 2))]

    def bind(self, source, scratch, last=None):
        self.source, self.slots, self.sems, self.last = source, scratch[:-1], scratch[-1], last
        return self

    def split(self, stage):
        bit = self.order[stage]
        if bit not in self.joint:
            return 1, self.blocks(stage), None
        left = [b for b in self.joint if b not in self.order[:stage]]
        high = 1 << left.index(bit)
        return high, self.blocks(stage) // (2 * high), mine_of(*bit)

    def view(self, stage, at):
        if stage == 0:
            return self.source.at[at, :, pl.ds(*self.lanes)]
        return self.slots[stage - 1].at[at]

    def steps(self):
        return len(self.order)

    def start(self, stage):
        high, low, side = self.split(stage)

        def send(run, carry):
            at = 0 if side is None else (2 * run + 1 - side) * low
            copy_to(
                self.view(stage, pl.ds(at, low)),
                self.slots[stage].at[pl.ds(run * low, low)],
                self.sems.at[stage],
                self.order[stage],
            ).start()
            return carry

        lax.fori_loop(0, high, send, 0)

    def whole(self, stage):
        slot = self.slots[stage]
        return copy_to(slot, slot, self.sems.at[stage], self.order[stage])

    def finish(self, stage):
        high, low, side = self.split(stage)
        slot = self.slots[stage]
        self.whole(stage).wait_recv()
        final = stage + 1 == len(self.order) and self.last is not None

        def add(index, carry):
            kept = index
            if side is not None:
                kept = (2 * lax.div(index, low) + side) * low + lax.rem(index, low)
            total = self.view(stage, kept)[...].astype(F32) + slot[index].astype(F32)
            if final:
                self.last(index, total)
            else:
                slot[index] = total.astype(BF16)
            return carry

        lax.fori_loop(0, high * low, add, 0)

    def drain(self):
        for stage in range(len(self.order)):
            self.whole(stage).wait_send()


class Gather:
    def __init__(self, shape, dtype, order):
        self.shape, self.dtype, self.order = shape, dtype, order

    def scratch(self):
        count = self.shape[0] << len(self.order)
        return [
            pltpu.VMEM((count,) + self.shape[1:], self.dtype),
            pltpu.SemaphoreType.DMA((len(self.order), 2)),
        ]

    def bind(self, scratch):
        self.buffer, self.sems = scratch
        self.place = place_of(list(reversed(self.order)))
        return self

    def own(self, index):
        return self.place * self.shape[0] + index

    def steps(self):
        return len(self.order)

    def copy(self, stage, theirs):
        run = 1 << stage
        base = lax.div(self.place, run) * run
        if theirs:
            base = base + run * (1 - 2 * mine_of(*self.order[stage]))
        here = self.buffer.at[pl.ds(base * self.shape[0], run * self.shape[0])]
        return copy_to(here, here, self.sems.at[stage], self.order[stage])

    def start(self, stage):
        self.copy(stage, False).start()

    def finish(self, stage):
        self.copy(stage, True).wait_recv()

    def drain(self):
        for stage in range(len(self.order)):
            self.copy(stage, False).wait_send()

    def natural(self, position, bits):
        index = 0
        for bit in bits:
            index = 2 * index + lax.rem(lax.div(position, 1 << self.order.index(bit)), 2)
        return index


class Swap:
    def __init__(self, shape, bit):
        self.shape, self.bit = shape, bit

    def scratch(self):
        return [pltpu.VMEM(self.shape, BF16), pltpu.SemaphoreType.DMA((2,))]

    def bind(self, source, scratch):
        self.source, (self.slot, self.sems) = source, scratch
        return self

    def steps(self):
        return 1

    def copy(self):
        return copy_to(self.source, self.slot, self.sems, self.bit)

    def start(self, stage):
        self.copy().start()

    def finish(self, stage):
        self.copy().wait_recv()

    def drain(self):
        self.copy().wait_send()


class Total:
    def __init__(self, shape, order):
        self.shape, self.order = shape, order

    def scratch(self):
        return [
            pltpu.VMEM((len(self.order) + 1,) + self.shape, F32),
            pltpu.VMEM((len(self.order),) + self.shape, F32),
            pltpu.SemaphoreType.DMA((len(self.order), 2)),
        ]

    def bind(self, scratch):
        self.held, self.slots, self.sems = scratch
        return self

    def steps(self):
        return len(self.order)

    def copy(self, stage):
        return copy_to(
            self.held.at[stage], self.slots.at[stage], self.sems.at[stage], self.order[stage]
        )

    def start(self, stage):
        self.copy(stage).start()

    def finish(self, stage):
        self.copy(stage).wait_recv()
        self.held[stage + 1] = self.held[stage] + self.slots[stage]

    def drain(self):
        for stage in range(len(self.order)):
            self.copy(stage).wait_send()


def take(scratch, chain):
    count = len(chain.scratch())
    return [scratch.pop(0) for _ in range(count)]


class Flow:
    def __init__(self, *transfers):
        self.todo = [(t, stage) for t in transfers for stage in range(t.steps())]
        self.at = -1

    def advance(self):
        if self.at >= 0:
            transfer, stage = self.todo[self.at]
            transfer.finish(stage)
        self.at += 1
        if self.at < len(self.todo):
            transfer, stage = self.todo[self.at]
            transfer.start(stage)

    def open(self):
        return self.at < len(self.todo)


TILE = 16


def halvings(blocks, bits):
    count = 0
    while count < len(bits) and blocks % 2 == 0:
        blocks //= 2
        count += 1
    return bits[:count]


def orders(head_bits, dp_bits):
    low_head, low_dp = list(reversed(head_bits)), list(reversed(dp_bits))
    return (
        low_head + low_dp,
        low_head[:-1] + low_dp[:1] + low_head[-1:] + low_dp[1:],
    )


def move(*flows):
    for flow in flows:
        for one in flow if isinstance(flow, list) else [flow]:
            if one.open():
                one.advance()


def keep(target, lane):
    def store(index, total):
        target[:, pl.ds(*lane)] = total

    return store


def feed_back(head_bits, dp_bits, grad_branch, slope, normed_low, up_weight, down_weight, grad_second, down, cls):
    joint = dp_bits + head_bits
    order = orders(head_bits, dp_bits)
    tokens, width = grad_branch.shape
    units = up_weight.shape[1]
    middle = width // 2
    lanes = ((0, middle), (middle, middle))
    large = [Scatter(down.shape, lanes[i], joint, order[i]) for i in range(2)]
    rows = Gather((1,) + cls.shape, F32, order[0][::-1])
    everything = large + [rows]

    def kernel(
        branch_ref, slope_ref, normed_ref, up_ref, weight_ref, second_ref, down_ref, cls_ref,
        first_ref, part_ref, bias_ref, sum_ref, all_ref, pre_t, copy_sems, *scratch
    ):
        scratch = list(scratch)
        held = [take(scratch, t) for t in everything]
        for i in range(2):
            large[i].bind(down_ref, held[i], keep(sum_ref, lanes[i]))
        rows.bind(held[2])
        flows, flow_rows = [Flow(t) for t in large], Flow(rows)
        second_copy = pltpu.make_async_copy(second_ref, first_ref, copy_sems.at[0])
        second_copy.start()
        rows.buffer[rows.place] = cls_ref[...]
        greet(joint)
        move(flows, flow_rows)

        def unit_tile(index, carry):
            column = pl.ds(pl.multiple_of(index * FF_TILE, FF_TILE), FF_TILE)

            @pl.when(index == 0)
            def _():
                second_copy.wait()

            bias = 0.0
            for start in range(0, tokens, ROW_TILE):
                here = pl.ds(start, ROW_TILE)
                grad = dot_nt(branch_ref[here, :], weight_ref[column, :])
                pre = (grad * slope_ref[here, column].astype(F32)).astype(BF16)
                bias = bias + jnp.sum(pre.astype(F32), axis=0, keepdims=True)
                pre_t[:, here] = pre.T
                first_ref[here, :] = first_ref[here, :] + dot_nt(pre, up_ref[:, column])
            bias_ref[:, column] = bias
            for start in range(0, FF_TILE, ROW_TILE):
                here = pl.ds(start, ROW_TILE)
                at = pl.ds(pl.multiple_of(index * FF_TILE + start, ROW_TILE), ROW_TILE)
                part_ref[at, :] = dot_nn(pre_t[here, :], normed_ref[...]).astype(BF16)
            for when, moved in ((0, (flow_rows,)), (1, (flows, flow_rows)), (4, (flows, flow_rows))):

                @pl.when(index == when)
                def _():
                    move(*moved)

            return carry

        lax.fori_loop(0, units // FF_TILE, unit_tile, 0)
        while any(flow.open() for flow in flows + [flow_rows]):
            move(flows, flow_rows)
        out_copy = pltpu.make_async_copy(rows.buffer, all_ref, copy_sems.at[1])
        out_copy.start()
        out_copy.wait()
        for t in everything:
            t.drain()

    vmem, anywhere = pl.BlockSpec(memory_space=pltpu.VMEM), pl.BlockSpec(memory_space=pl.ANY)
    return pl.pallas_call(
        kernel,
        in_specs=[vmem] * 5 + [anywhere] + [vmem] * 2,
        out_specs=[vmem] * 4 + [anywhere],
        out_shape=[
            jax.ShapeDtypeStruct((tokens, width), F32),
            jax.ShapeDtypeStruct((units, width), BF16),
            jax.ShapeDtypeStruct((1, units), F32),
            jax.ShapeDtypeStruct(down.shape[1:], F32),
            jax.ShapeDtypeStruct((1 << len(joint),) + cls.shape, F32),
        ],
        scratch_shapes=[pltpu.VMEM((FF_TILE, tokens), BF16), pltpu.SemaphoreType.DMA((2,))]
        + [x for t in everything for x in t.scratch()],
        compiler_params=pltpu.CompilerParams(
            collective_id=0, has_side_effects=True, vmem_limit_bytes=62 * 1024 * 1024
        ),
    )(grad_branch, slope, normed_low, up_weight, down_weight, grad_second, down, cls)


def back_all(head_bits, dp_bits, far, own, rows_in, grad_first_in, up, out, vector):
    joint = dp_bits + head_bits
    order = orders(head_bits, dp_bits)
    low_head, low_dp = list(reversed(head_bits)), list(reversed(dp_bits))
    dp_order = (low_dp, low_dp[1:2] + low_dp[:1] + low_dp[2:])
    far_bit, join_bits = head_bits[0], low_head[:-1]
    tokens, width = rows_in.shape
    seqs, _, length, _ = far[5].shape
    half = far[0].shape[1]
    pairs = half // LANES
    steps = pairs * seqs
    local = half >> len(join_bits)
    chunks = local // HEAD_DIM
    tiles = 3 * local // TILE
    chunk_tiles = HEAD_DIM // TILE
    middle = width // 2
    lanes = ((0, middle), (middle, middle))
    large = [Scatter(up.shape, lanes[i], joint, order[i]) for i in range(2)]
    out_bits = [halvings(out.shape[0], order[i]) for i in range(2)]
    outs = [Scatter(out.shape, lanes[i], out_bits[i], order[i]) for i in range(2)]
    outs_back = [
        Gather((out.shape[0] >> len(out_bits[i]), TILE, middle), BF16, out_bits[i][::-1])
        for i in range(2)
    ]
    source = (tiles << len(join_bits), TILE, width)
    far_join = [Scatter(source, lanes[i], join_bits, join_bits) for i in range(2)]
    own_join = [Scatter(source, lanes[i], join_bits, join_bits) for i in range(2)]
    swaps = [Swap((tiles, TILE, middle), far_bit) for i in range(2)]
    qkv_bits = [halvings(tiles, dp_order[i]) for i in range(2)]
    sums = [
        Scatter((tiles, TILE, middle), (0, middle), qkv_bits[i], dp_order[i]) for i in range(2)
    ]
    sums_back = [
        Gather((tiles >> len(qkv_bits[i]), TILE, middle), BF16, qkv_bits[i][::-1])
        for i in range(2)
    ]
    vector_rows = vector.shape[0]
    bias_rows = 2 * width // LANES
    small = Total((vector_rows + bias_rows, LANES), order[0])
    groups = [large, outs, outs_back, far_join, own_join, swaps, sums, sums_back, [small]]
    everything = [t for group in groups for t in group]

    def kernel(*refs):
        refs = list(refs)
        halves = [[refs.pop(0) for _ in range(6)] for _ in range(2)]
        rows_ref, first_ref, up_ref, out_ref, vector_ref = [refs.pop(0) for _ in range(5)]
        in_ref, up_sum, out_sum, qkv_sum, vector_sum = [refs.pop(0) for _ in range(5)]
        grads, sources = [refs.pop(0) for _ in range(2)], [refs.pop(0) for _ in range(2)]
        partial, probs_buffer, probs_sems, first_sem = [refs.pop(0) for _ in range(4)]
        held = {id(t): take(refs, t) for t in everything}
        side = mine_of(*far_bit)

        def hand_on(gather):
            def store(index, total):
                gather.buffer[gather.own(index)] = total.astype(BF16)

            return store

        for t in outs_back + sums_back + [small]:
            t.bind(held[id(t)])
        for i, t in enumerate(large):
            t.bind(up_ref, held[id(t)], keep(up_sum, lanes[i]))
        for i in range(2):
            outs[i].bind(out_ref, held[id(outs[i])], hand_on(outs_back[i]))
            far_join[i].bind(sources[0], held[id(far_join[i])])
            own_join[i].bind(sources[1], held[id(own_join[i])])
            swaps[i].bind(far_join[i].slots[-1], held[id(swaps[i])])
            sums[i].bind(own_join[i].slots[-1], held[id(sums[i])], hand_on(sums_back[i]))
        flow_up = [Flow(large[i]) for i in range(2)]
        flow_out = [Flow(outs[i], outs_back[i]) for i in range(2)]
        flow_far = [Flow(far_join[i], swaps[i]) for i in range(2)]
        flow_own = [Flow(own_join[i]) for i in range(2)]
        flow_sum = [Flow(sums[i], sums_back[i]) for i in range(2)]
        flow_small = Flow(small)

        def probs_copy(which, step):
            slot = lax.rem(step, 2)
            return pltpu.make_async_copy(
                halves[which][5].at[lax.rem(step, seqs), pl.ds(lax.div(step, seqs) * PAIR, PAIR)],
                probs_buffer.at[slot],
                probs_sems.at[slot],
            )

        first_copy = pltpu.make_async_copy(first_ref, in_ref, first_sem)
        first_copy.start()
        probs_copy(0, 0).start()
        small.held[0, :vector_rows] = vector_ref[...]
        small.held[0, vector_rows:] = jnp.zeros((bias_rows, LANES), F32)
        greet(joint)
        move(flow_up, flow_out)

        def attend_step(which, step):
            query_ref, key_ref, value_ref, grad_ref, _, _ = halves[which]
            pair, seq = lax.div(step, seqs), lax.rem(step, seqs)
            at = (
                pl.ds(pl.multiple_of(seq * length, length), length),
                pl.ds(pl.multiple_of(pair * LANES, LANES), LANES),
            )
            probs_copy(which, step).wait()

            @pl.when(step + 1 < steps)
            def _():
                probs_copy(which, step + 1).start()

            if which == 0:

                @pl.when(step + 1 == steps)
                def _():
                    probs_copy(1, 0).start()

            query, value, grad = query_ref[at], value_ref[at], grad_ref[at]
            key_t = key_ref[at].T
            grad_key = grad_value = 0.0
            grad_query = []
            slot = lax.rem(step, 2)
            for head in range(PAIR):
                own_query = (head_lanes(query, head) * SCALE).astype(BF16)
                own_value = head_lanes(value, head).astype(BF16)
                own_grad = head_lanes(grad, head).astype(BF16)
                low = probs_buffer[slot, head]
                probs = low.astype(F32)
                grad_probs = dot_nt(own_value, grad)
                weighted = jnp.sum(probs * grad_probs, axis=0, keepdims=True)
                grad_scores = (probs * (grad_probs - weighted)).astype(BF16)
                grad_value += dot_nn(low, own_grad)
                grad_key += dot_nn(grad_scores, own_query)
                head_rows = slice(head * HEAD_DIM, (head + 1) * HEAD_DIM)
                grad_query.append(dot_nn(key_t[head_rows], grad_scores))
            query_t = (jnp.concatenate(grad_query, axis=0) * SCALE).astype(BF16)
            own = [query_t.T, grad_key.astype(BF16), grad_value.astype(BF16)]
            for kind in range(3):
                column = pl.multiple_of(kind * half + pair * LANES, LANES)
                grads[which][at[0], pl.ds(column, LANES)] = own[kind]
            stacked = jnp.concatenate([query_t, own[1].T, own[2].T], axis=0)
            part = dot_nn(stacked, rows_ref[at[0], :])
            group = (side if which == 1 else 1 - side) * pairs + pair
            for kind, block in ((0, own[0]), (1, own[2])):
                row = vector_rows + kind * (bias_rows // 2) + group
                total = jnp.sum(block.astype(F32), axis=0, keepdims=True)
                small.held[0, pl.ds(row, 1)] = small.held[0, pl.ds(row, 1)] + total

            @pl.when(seq == 0)
            def _():
                partial[...] = part

            @pl.when(seq > 0)
            def _():
                partial[...] = partial[...] + part

            @pl.when(seq == seqs - 1)
            def _():
                for kind in range(3):
                    for one in range(PAIR):
                        chunk = pair * PAIR + one
                        tile = lax.div(chunk, chunks) * tiles + kind * (local // TILE)
                        tile = tile + lax.rem(chunk, chunks) * chunk_tiles
                        start = kind * LANES + one * HEAD_DIM
                        block = partial[start : start + HEAD_DIM, :].astype(BF16)
                        sources[which][pl.ds(tile, chunk_tiles)] = block.reshape(
                            chunk_tiles, TILE, width
                        )

        def sweep(which, events):
            def step(index, carry):
                attend_step(which, index)
                for when, flows in events:

                    @pl.when(index == when)
                    def _():
                        move(*flows)

                return carry

            lax.fori_loop(0, steps, step, 0)

        sweep(0, [(2, (flow_up, flow_out))])
        move(flow_far)
        sweep(1, [(1, (flow_far, flow_out)), (3, (flow_up,)), (5, (flow_up, flow_out))])
        move(flow_own, flow_small)
        first_copy.wait()

        def input_rows(index, carry):
            at = pl.ds(pl.multiple_of(index * ROW_TILE, ROW_TILE), ROW_TILE)
            in_ref[at, :] = (
                in_ref[at, :]
                + dot_nn(grads[0][at, :], halves[0][4][...])
                + dot_nn(grads[1][at, :], halves[1][4][...])
            )
            return carry

        blocks = tokens // ROW_TILE
        lax.fori_loop(0, blocks // 2, input_rows, 0)
        move(flow_own, flow_small, flow_up)
        lax.fori_loop(blocks // 2, blocks, input_rows, 0)
        move(flow_small, flow_out)
        while flow_own[0].open():
            move(flow_own)
        move(flow_far)
        for i in range(2):
            assert not flow_far[i].open()

            def merge(index, carry, i=i):
                target = own_join[i].slots[-1]
                target[index] = (
                    target[index].astype(F32) + swaps[i].slot[index].astype(F32)
                ).astype(BF16)
                return carry

            lax.fori_loop(0, tiles, merge, 0)
        move(flow_sum)
        flat = flow_sum + flow_up + flow_out + [flow_small]
        while any(flow.open() for flow in flat):
            move(flow_sum, flow_up, flow_out, flow_small)
        for i in range(2):
            for gather, target in ((outs_back[i], out_sum), (sums_back[i], qkv_sum)):

                def spread(index, carry, gather=gather, target=target, lane=lanes[i]):
                    target[index, :, pl.ds(*lane)] = gather.buffer[index].astype(F32)
                    return carry

                lax.fori_loop(0, gather.buffer.shape[0], spread, 0)
        vector_sum[...] = small.held[len(small.order)]
        for t in everything:
            t.drain()

    vmem, anywhere = pl.BlockSpec(memory_space=pltpu.VMEM), pl.BlockSpec(memory_space=pl.ANY)
    half_specs = [vmem] * 5 + [anywhere]
    return pl.pallas_call(
        kernel,
        in_specs=half_specs * 2 + [vmem, anywhere] + [vmem] * 3,
        out_specs=[vmem] * 5,
        out_shape=[
            jax.ShapeDtypeStruct((tokens, width), F32),
            jax.ShapeDtypeStruct(up.shape[1:], F32),
            jax.ShapeDtypeStruct(out.shape, F32),
            jax.ShapeDtypeStruct((tiles, TILE, width), F32),
            jax.ShapeDtypeStruct(small.shape, F32),
        ],
        scratch_shapes=[pltpu.VMEM((tokens, 3 * half), BF16)] * 2
        + [pltpu.VMEM(source, BF16)] * 2
        + [
            pltpu.VMEM((3 * LANES, width), F32),
            pltpu.VMEM((2, PAIR, length, length), BF16),
            pltpu.SemaphoreType.DMA((2,)),
            pltpu.SemaphoreType.DMA(()),
        ]
        + [x for t in everything for x in t.scratch()],
        compiler_params=pltpu.CompilerParams(
            collective_id=1, has_side_effects=True, vmem_limit_bytes=62 * 1024 * 1024
        ),
    )(*far, *own, rows_in, grad_first_in, up, out, vector)


def classify(cls_rows, labels, w_pool, b_pool, w_class, b_class):
    pooled = jnp.tanh(jnp.dot(cls_rows, w_pool, preferred_element_type=F32) + b_pool)
    class_weight = w_class.astype(F32)
    logits = jnp.dot(pooled, class_weight, precision=lax.Precision.HIGHEST) + b_class
    onehot = (labels[:, None] == jnp.arange(logits.shape[1])[None, :]).astype(F32)
    ramp_loss = jax.nn.logsumexp(logits, axis=-1) - jnp.sum(logits * onehot, axis=-1)
    grad_logits = jax.nn.softmax(logits, axis=-1) - onehot
    grad_pool = (
        jnp.dot(grad_logits, class_weight.T, precision=lax.Precision.HIGHEST)
        * (1.0 - pooled * pooled)
    ).astype(BF16)
    return pooled, ramp_loss, grad_logits, grad_pool


def body(
    hidden_in,
    lengths,
    labels,
    query_key_value_weight,
    query_value_bias,
    attention_output_weight,
    attention_output_bias,
    gain_att,
    shift_att,
    up_weight,
    up_bias,
    down_weight,
    down_bias,
    gain_ffn,
    shift_ffn,
    w_pool,
    b_pool,
    w_class,
    b_class,
    cotangent,
):
    seq_here, seq_len, width = hidden_in.shape
    tokens = seq_here * seq_len
    everyone = ("dp", "head")
    head_bits = bits_of(("head",))
    dp_bits = bits_of(("dp",))
    rows_in = hidden_in.reshape(tokens, width)

    half_bits, far_bit = head_bits[1:], head_bits[0]
    own_weight = jnp.transpose(query_key_value_weight, (2, 0, 1))
    own_weight = own_weight.transpose(1, 0, 2)
    far_weight = exchange(own_weight, *far_bit)
    far_bias = exchange(query_value_bias, *far_bit)
    low_order = list(reversed(half_bits))

    def join(blocks, order):
        for axis, bit in order:
            got = exchange(blocks, axis, bit)
            blocks = jnp.where(
                own_bit(axis, bit) == 0,
                jnp.concatenate([blocks, got], axis=1),
                jnp.concatenate([got, blocks], axis=1),
            )
        return blocks

    halves = []
    for weight, bias in ((own_weight, query_value_bias), (far_weight, far_bias)):
        weight, bias = join(weight, low_order), join(bias, low_order)
        query = (dot_nt(rows_in, weight[0]) + bias[0]).astype(BF16)
        key = dot_nt(rows_in, weight[1]).astype(BF16)
        value = (dot_nt(rows_in, weight[2]) + bias[1]).astype(BF16)
        context, probs = attend(lengths, query, key, value)
        halves.append((weight, query, key, value, context, probs))
    half_width = halves[0][1].shape[1]
    far_side = own_bit(*far_bit)

    def in_place(own, far, axis):
        return jnp.where(
            far_side == 0,
            jnp.concatenate([own, far], axis=axis),
            jnp.concatenate([far, own], axis=axis),
        )

    combined = in_place(halves[0][4], halves[1][4], 1)
    attended = (
        jnp.dot(combined, attention_output_weight, preferred_element_type=F32)
        + attention_output_bias
    )
    first_in = rows_in.astype(F32) + attended
    normalized_first = normalize(first_in, gain_att, shift_att)
    normed_low = normalized_first.astype(BF16)
    gelu_output, slope, branch = feed_forward(
        normed_low, up_weight, up_bias, down_weight, down_bias
    )
    second_in = normalized_first + branch
    output_rows = normalize(second_in, gain_ffn, shift_ffn)
    hidden_out = output_rows.astype(BF16).reshape(seq_here, seq_len, width)
    cls_rows = hidden_out[:, 0, :]
    pooled, ramp_loss, grad_logits, grad_pool = classify(
        cls_rows, labels, w_pool, b_pool, w_class, b_class
    )
    grad_cls = jnp.dot(grad_pool, w_pool.T, preferred_element_type=F32)
    classes = grad_logits.shape[1]
    cls_pack = jnp.concatenate(
        [
            cls_rows.astype(F32),
            grad_pool.astype(F32),
            pooled,
            jnp.pad(grad_logits, ((0, 0), (0, LANES - classes))),
        ],
        axis=1,
    )
    pack_width = cls_pack.shape[1]
    cls_pack = cls_pack.reshape(-1, LANES)

    grad_output = cotangent.astype(F32).at[:, 0, :].add(grad_cls).reshape(tokens, width)
    _, second_back = jax.vjp(normalize, second_in, gain_ffn, shift_ffn)
    grad_second, grad_gain_ffn, grad_shift_ffn = second_back(grad_output)
    grad_branch = grad_second.astype(BF16)
    grad_b_down = jnp.sum(grad_branch, axis=0, dtype=F32)
    part_w_down = jnp.dot(gelu_output.T, grad_branch, preferred_element_type=F32).astype(BF16)
    devices = lax.axis_size("dp") * lax.axis_size("head")
    grad_first, part_w_up, grad_b_up, grad_w_down, cls_all = feed_back(
        head_bits,
        dp_bits,
        grad_branch,
        slope,
        normed_low,
        up_weight,
        down_weight,
        grad_second,
        part_w_down.reshape(devices, -1, width),
        cls_pack,
    )
    grad_b_up = grad_b_up[0]
    _, first_back = jax.vjp(normalize, first_in, gain_att, shift_att)
    grad_first_in, grad_gain_att, grad_shift_att = first_back(grad_first)
    grad_attended = grad_first_in.astype(BF16)
    grad_b_out = jnp.sum(grad_attended, axis=0, dtype=F32)
    part_w_out = jnp.dot(combined.T, grad_attended, preferred_element_type=F32).astype(BF16)
    grad_context = dot_nt(grad_attended, attention_output_weight).astype(BF16)
    far_context = lax.dynamic_slice_in_dim(
        grad_context, (1 - far_side) * half_width, half_width, 1
    )
    own_context = lax.dynamic_slice_in_dim(grad_context, far_side * half_width, half_width, 1)
    local = query_key_value_weight.shape[2]
    vectors = [
        grad_b_out,
        grad_gain_att,
        grad_shift_att,
        grad_b_up,
        grad_b_down,
        grad_gain_ffn,
        grad_shift_ffn,
    ]
    far, own = [
        (half[1], half[2], half[3], grad_half, half[0].reshape(-1, width), half[5])
        for half, grad_half in ((halves[1], far_context), (halves[0], own_context))
    ]
    grad_in, grad_w_up, grad_w_out, qkv, sums = back_all(
        head_bits,
        dp_bits,
        far,
        own,
        rows_in,
        grad_first_in,
        part_w_up.reshape(devices, -1, width),
        part_w_out.reshape(-1, TILE, width),
        jnp.concatenate(vectors).reshape(-1, LANES),
    )
    grad_w_up = grad_w_up.T
    grad_w_out = grad_w_out.reshape(width, width)
    grad_w_qkv = jnp.transpose(qkv.reshape(3, local, width), (0, 2, 1))
    edges, reached = [], 0
    for vector in vectors:
        reached += vector.shape[0]
        edges.append(reached)
    (
        grad_b_out,
        grad_gain_att,
        grad_shift_att,
        grad_b_up,
        grad_b_down,
        grad_gain_ffn,
        grad_shift_ffn,
        bias_all,
    ) = jnp.split(sums.reshape(-1), edges)
    grad_b_qv = lax.dynamic_slice_in_dim(
        bias_all.reshape(2, width), lax.axis_index("head") * local, local, 1
    )
    cls_all = cls_all.reshape(-1, pack_width)
    all_cls, all_pool, pooled = jnp.split(cls_all[:, : 3 * width], 3, axis=1)
    grad_logits = cls_all[:, 3 * width : 3 * width + classes]
    grad_b_class = jnp.sum(grad_logits, axis=0)
    grad_w_class = jnp.dot(pooled.T, grad_logits, precision=lax.Precision.HIGHEST)
    grad_b_pool = jnp.sum(all_pool, axis=0)
    grad_w_pool = jnp.dot(
        all_cls.T.astype(BF16), all_pool.astype(BF16), preferred_element_type=F32
    )
    return (
        hidden_out,
        ramp_loss,
        grad_in.reshape(seq_here, seq_len, width),
        grad_w_qkv,
        grad_b_qv,
        grad_w_out,
        grad_b_out,
        grad_gain_att,
        grad_shift_att,
        grad_w_up,
        grad_b_up,
        grad_w_down,
        grad_b_down,
        grad_gain_ffn,
        grad_shift_ffn,
        grad_w_pool,
        grad_b_pool,
        grad_w_class,
        grad_b_class,
    )


def solution(mesh):
    rows = P(("dp", "head"))
    placed = (
        (P(("dp", "head"), None, None), rows, rows, P(None, None, "head"), P(None, "head"))
        + (P(),) * 14
        + (P(("dp", "head"), None, None),)
    )
    tokens = P(("dp", "head"), None, None)
    outs = (
        (tokens, rows, tokens, P(None, None, "head"), P(None, "head"))
        + (P(),) * 4
        + (P(None, ("dp", "head")), P(), P(("dp", "head"), None))
        + (P(),) * 7
    )
    return jax.shard_map(body, mesh=mesh, in_specs=placed, out_specs=outs, check_vma=False)
```

```python
import functools

import jax
import jax.numpy as jnp
from jax import lax
from jax.experimental import pallas as pl
from jax.experimental.pallas import tpu as pltpu
from jax.sharding import PartitionSpec as P

HEAD_DIM = 64
EPSILON = 1e-06
MASKED = -1000000000.0
BF16, F32 = jnp.bfloat16, jnp.float32


def bit_count(n):
    assert n & (n - 1) == 0
    return n.bit_length() - 1


def exchange(value, axis, bit):
    size = lax.axis_size(axis)
    step = 1 << bit
    return lax.ppermute(value, axis, [(i, i ^ step) for i in range(size)])


def own_bit(axis, bit):
    return (lax.axis_index(axis) >> bit) & 1


def bits_of(axes):
    found = []
    for axis in axes:
        found += [(axis, b) for b in reversed(range(bit_count(lax.axis_size(axis))))]
    return found


def normalize(row_block, gain_row, shift_row):
    center = jnp.mean(row_block, axis=-1, keepdims=True)
    centered = row_block - center
    spread = jnp.mean(centered * centered, axis=-1, keepdims=True)
    return centered * lax.rsqrt(spread + EPSILON) * gain_row + shift_row


LANES = 128
PAIR = LANES // HEAD_DIM
SCALE = HEAD_DIM ** (-0.5)


def dot_nt(left, right):
    return lax.dot_general(left, right, (((1,), (1,)), ((), ())), preferred_element_type=F32)


def dot_nn(left, right):
    return jnp.dot(left, right, preferred_element_type=F32)


def head_lanes(block, head):
    lane = lax.broadcasted_iota(jnp.int32, block.shape, 1)
    inside = (lane >= head * HEAD_DIM) & (lane < (head + 1) * HEAD_DIM)
    return jnp.where(inside, block.astype(F32), 0.0)


def attend_kernel(length_ref, query_ref, key_ref, value_ref, context_ref, probs_ref):
    length = length_ref[pl.program_id(0)]
    query, key = query_ref[...], key_ref[...]
    value_t = value_ref[...].T
    rows = query.shape[0]
    key_at = lax.broadcasted_iota(jnp.int32, (rows, rows), 0)
    contexts = []
    for head in range(PAIR):
        own_query = (head_lanes(query, head) * SCALE).astype(BF16)
        scores = jnp.where(key_at < length, dot_nt(key, own_query), MASKED)
        shifted = jnp.exp(scores - jnp.max(scores, axis=0, keepdims=True))
        inverse = 1.0 / jnp.sum(shifted, axis=0, keepdims=True)
        probs = (shifted * inverse).astype(BF16)
        probs_ref[0, head] = probs
        contexts.append(dot_nn(value_t[head * HEAD_DIM : (head + 1) * HEAD_DIM], probs))
    context_ref[...] = jnp.concatenate(contexts, axis=0).T.astype(BF16)


def attend(lengths, query, key, value):
    seqs = lengths.shape[0]
    tokens, width = query.shape
    rows, pairs = tokens // seqs, width // LANES
    block = pl.BlockSpec((rows, LANES), lambda s, p: (s, p))
    return pl.pallas_call(
        attend_kernel,
        grid=(seqs, pairs),
        in_specs=[pl.BlockSpec(memory_space=pltpu.SMEM), block, block, block],
        out_specs=[block, pl.BlockSpec((1, PAIR, rows, rows), lambda s, p: (s, p, 0, 0))],
        out_shape=[
            jax.ShapeDtypeStruct((tokens, width), BF16),
            jax.ShapeDtypeStruct((seqs, pairs * PAIR, rows, rows), BF16),
        ],
        cost_estimate=pl.CostEstimate(
            flops=seqs * pairs * 12 * rows * rows * LANES,
            bytes_accessed=8 * tokens * width + 4 * tokens * rows * pairs,
            transcendentals=0,
        ),
    )(lengths, query, key, value)


def gelu_parts(values):
    bell = jnp.exp(-0.5 * values * values)
    inner = 1.0 / (1.0 + (0.3275911 * 0.5**0.5) * jnp.abs(values))
    series = 0.5 * 1.061405429
    for term in (-1.453152027, 1.421413741, -0.284496736, 0.254829592):
        series = series * inner + 0.5 * term
    tail = series * inner * bell
    below = jnp.where(values < 0.0, tail, 1.0 - tail)
    return values * below, below + values * bell * 0.3989422804014327


FF_TILE = 512
ROW_TILE = 256


def feed_kernel(rows_ref, up_ref, up_bias_ref, down_ref, down_bias_ref, act_ref, slope_ref, out_ref):
    first = pl.program_id(0) == 0

    @pl.when(first)
    def _():
        out_ref[...] = jnp.broadcast_to(down_bias_ref[...], out_ref.shape)

    for start in range(0, rows_ref.shape[0], ROW_TILE):
        here = pl.ds(start, ROW_TILE)
        before = dot_nn(rows_ref[here, :], up_ref[...]) + up_bias_ref[...]
        active, slope = gelu_parts(before)
        active = active.astype(BF16)
        act_ref[here, :] = active
        slope_ref[here, :] = slope.astype(BF16)
        out_ref[here, :] += dot_nn(active, down_ref[...])


def feed_forward(rows, up_weight, up_bias, down_weight, down_bias):
    tokens, width = rows.shape
    units = up_weight.shape[1]
    whole = lambda shape: pl.BlockSpec(shape, lambda i: (0, 0))
    columns = lambda height: pl.BlockSpec((height, FF_TILE), lambda i: (0, i))
    return pl.pallas_call(
        feed_kernel,
        grid=(units // FF_TILE,),
        in_specs=[
            whole((tokens, width)),
            columns(width),
            columns(1),
            pl.BlockSpec((FF_TILE, width), lambda i: (i, 0)),
            whole((1, width)),
        ],
        out_specs=[columns(tokens), columns(tokens), whole((tokens, width))],
        out_shape=[
            jax.ShapeDtypeStruct((tokens, units), BF16),
            jax.ShapeDtypeStruct((tokens, units), BF16),
            jax.ShapeDtypeStruct((tokens, width), F32),
        ],
        cost_estimate=pl.CostEstimate(
            flops=8 * tokens * width * units,
            bytes_accessed=4 * tokens * units + 4 * width * units,
            transcendentals=0,
        ),
    )(rows, up_weight, up_bias[None], down_weight, down_bias[None])


MESH = pl.DeviceIdType.MESH


def mine_of(axis, bit):
    return lax.rem(lax.div(lax.axis_index(axis), 1 << bit), 2)


def partner_of(axis, bit):
    return {axis: lax.axis_index(axis) + (1 << bit) * (1 - 2 * mine_of(axis, bit))}


def place_of(bits):
    place = 0
    for axis, bit in bits:
        place = 2 * place + mine_of(axis, bit)
    return place


def greet(bits):
    barrier = pltpu.get_barrier_semaphore()
    for axis, bit in bits:
        pl.semaphore_signal(
            barrier, inc=1, device_id=partner_of(axis, bit), device_id_type=MESH
        )
    pl.semaphore_wait(barrier, len(bits))


def copy_to(source, target, sems, bit):
    return pltpu.make_async_remote_copy(
        src_ref=source,
        dst_ref=target,
        send_sem=sems.at[0],
        recv_sem=sems.at[1],
        device_id=partner_of(*bit),
        device_id_type=MESH,
    )


class Scatter:
    def __init__(self, shape, lanes, joint, order, far=False):
        self.shape, self.lanes, self.joint, self.order = shape, lanes, joint, order
        self.far = far

    def blocks(self, stage):
        halved = len([bit for bit in self.order[:stage] if bit in self.joint])
        return self.shape[0] >> halved

    def scratch(self):
        rows, width = self.shape[1], self.lanes[1]
        return [
            pltpu.VMEM((self.blocks(stage + 1), rows, width), BF16)
            for stage in range(len(self.order))
        ] + (
            [
                pltpu.VMEM((self.blocks(1), rows, width), BF16),
                pltpu.SemaphoreType.DMA(()),
            ]
            if self.far
            else []
        ) + [pltpu.SemaphoreType.DMA((len(self.order), 2))]

    def bind(self, source, scratch, last=None):
        self.source, self.sems, self.last = source, scratch[-1], last
        self.slots = scratch[: len(self.order)]
        if self.far:
            self.kept, self.kept_sem = scratch[len(self.order) : -1]
        return self

    def split(self, stage):
        bit = self.order[stage]
        if bit not in self.joint:
            return 1, self.blocks(stage), None
        left = [b for b in self.joint if b not in self.order[:stage]]
        high = 1 << left.index(bit)
        return high, self.blocks(stage) // (2 * high), mine_of(*bit)

    def view(self, stage, at):
        if stage == 0:
            return self.source.at[at, :, pl.ds(*self.lanes)]
        return self.slots[stage - 1].at[at]

    def steps(self):
        return len(self.order)

    def start(self, stage):
        high, low, side = self.split(stage)

        def send(run, carry):
            at = 0 if side is None else (2 * run + 1 - side) * low
            copy_to(
                self.view(stage, pl.ds(at, low)),
                self.slots[stage].at[pl.ds(run * low, low)],
                self.sems.at[stage],
                self.order[stage],
            ).start()
            if self.far and stage == 0:
                pltpu.make_async_copy(
                    self.view(0, pl.ds((2 * run + side) * low, low)),
                    self.kept.at[pl.ds(run * low, low)],
                    self.kept_sem,
                ).start()
            return carry

        lax.fori_loop(0, high, send, 0)

    def whole(self, stage):
        slot = self.slots[stage]
        return copy_to(slot, slot, self.sems.at[stage], self.order[stage])

    def finish(self, stage):
        high, low, side = self.split(stage)
        slot = self.slots[stage]
        self.whole(stage).wait_recv()
        from_kept = self.far and stage == 0
        if from_kept:
            pltpu.make_async_copy(self.kept, self.kept, self.kept_sem).wait()
        final = stage + 1 == len(self.order) and self.last is not None

        def add(index, carry):
            kept = index
            if side is not None:
                kept = (2 * lax.div(index, low) + side) * low + lax.rem(index, low)
            mine = self.kept[index] if from_kept else self.view(stage, kept)[...]
            theirs = slot[index]
            if final:
                self.last(index, mine.astype(F32) + theirs.astype(F32))
            else:
                slot[index] = mine + theirs
            return carry

        lax.fori_loop(0, high * low, add, 0)

    def drain(self):
        for stage in range(len(self.order)):
            self.whole(stage).wait_send()


class Gather:
    def __init__(self, shape, dtype, order):
        self.shape, self.dtype, self.order = shape, dtype, order

    def scratch(self):
        count = self.shape[0] << len(self.order)
        return [
            pltpu.VMEM((count,) + self.shape[1:], self.dtype),
            pltpu.SemaphoreType.DMA((len(self.order), 2)),
        ]

    def bind(self, scratch):
        self.buffer, self.sems = scratch
        self.place = place_of(list(reversed(self.order)))
        return self

    def own(self, index):
        return self.place * self.shape[0] + index

    def steps(self):
        return len(self.order)

    def copy(self, stage, theirs):
        run = 1 << stage
        base = lax.div(self.place, run) * run
        if theirs:
            base = base + run * (1 - 2 * mine_of(*self.order[stage]))
        here = self.buffer.at[pl.ds(base * self.shape[0], run * self.shape[0])]
        return copy_to(here, here, self.sems.at[stage], self.order[stage])

    def start(self, stage):
        self.copy(stage, False).start()

    def finish(self, stage):
        self.copy(stage, True).wait_recv()

    def drain(self):
        for stage in range(len(self.order)):
            self.copy(stage, False).wait_send()

    def natural(self, position, bits):
        index = 0
        for bit in bits:
            index = 2 * index + lax.rem(lax.div(position, 1 << self.order.index(bit)), 2)
        return index


class Swap:
    def __init__(self, shape, bit):
        self.shape, self.bit = shape, bit

    def scratch(self):
        return [pltpu.VMEM(self.shape, BF16), pltpu.SemaphoreType.DMA((2,))]

    def bind(self, source, scratch):
        self.source, (self.slot, self.sems) = source, scratch
        return self

    def steps(self):
        return 1

    def copy(self):
        return copy_to(self.source, self.slot, self.sems, self.bit)

    def start(self, stage):
        self.copy().start()

    def finish(self, stage):
        self.copy().wait_recv()

    def drain(self):
        self.copy().wait_send()


class Total:
    def __init__(self, shape, order):
        self.shape, self.order = shape, order

    def scratch(self):
        return [
            pltpu.VMEM((len(self.order) + 1,) + self.shape, F32),
            pltpu.VMEM((len(self.order),) + self.shape, F32),
            pltpu.SemaphoreType.DMA((len(self.order), 2)),
        ]

    def bind(self, scratch):
        self.held, self.slots, self.sems = scratch
        return self

    def steps(self):
        return len(self.order)

    def copy(self, stage):
        return copy_to(
            self.held.at[stage], self.slots.at[stage], self.sems.at[stage], self.order[stage]
        )

    def start(self, stage):
        self.copy(stage).start()

    def finish(self, stage):
        self.copy(stage).wait_recv()
        self.held[stage + 1] = self.held[stage] + self.slots[stage]

    def drain(self):
        for stage in range(len(self.order)):
            self.copy(stage).wait_send()


def take(scratch, chain):
    count = len(chain.scratch())
    return [scratch.pop(0) for _ in range(count)]


class Flow:
    def __init__(self, *transfers):
        self.todo = [(t, stage) for t in transfers for stage in range(t.steps())]
        self.at = -1

    def plan(self):
        at = self.at
        self.at += 1

        def advance():
            if at >= 0:
                transfer, stage = self.todo[at]
                transfer.finish(stage)
            if at + 1 < len(self.todo):
                transfer, stage = self.todo[at + 1]
                transfer.start(stage)

        return advance

    def open(self):
        return self.at < len(self.todo)


TILE = 8


def halvings(blocks, bits):
    count = 0
    while count < len(bits) and blocks % 2 == 0:
        blocks //= 2
        count += 1
    return bits[:count]


def orders(head_bits, dp_bits):
    low_head, low_dp = list(reversed(head_bits)), list(reversed(dp_bits))
    axes = low_head[-1:] + low_dp[:2]
    return [low_head[:-1] + axes[i:] + axes[:i] + low_dp[2:] for i in range(3)]


def plan(*flows):
    listed = [one for flow in flows for one in (flow if isinstance(flow, list) else [flow])]
    return [one.plan() for one in listed if one.open()]


def move(*flows):
    for advance in plan(*flows):
        advance()


def keep(target, lane):
    def store(index, total):
        target[:, pl.ds(*lane)] = total

    return store


FEED_PLACES = 6
FEED_EVENTS = (
    (1, 0, (3,)),
    (1, 2, (0, 1, 2,)),
    (1, 5, (3,)),
    (3, 3, (3,)),
    (4, 3, (0, 2,)),
    (4, 5, (1,)),
    (5, 1, (3,)),
    (5, 5, (3,)),
)
FEED_TAIL = (0, 2, 1, 0, 2, 1, 0, 2, 1)


def feed_back(head_bits, dp_bits, grad_branch, slope, normed_low, up_weight, down_weight, grad_second, down, cls):
    joint = dp_bits + head_bits
    order = orders(head_bits, dp_bits)
    tokens, width = grad_branch.shape
    units = up_weight.shape[1]
    third = width // 3
    lanes = [(i * third, third) for i in range(3)]
    large = [Scatter(down.shape, lanes[i], joint, order[i], far=True) for i in range(3)]
    rows = Gather((1,) + cls.shape, F32, order[0][::-1])
    everything = large + [rows]

    def kernel(
        branch_ref, slope_ref, normed_ref, up_ref, weight_ref, second_ref, down_ref, cls_ref,
        first_ref, part_ref, bias_ref, sum_ref, all_ref,
        pre_t, slopes, ups, weights, parts, copy_sems, in_sems, out_sems, *scratch
    ):
        scratch = list(scratch)
        held = [take(scratch, t) for t in everything]
        for i in range(3):
            large[i].bind(down_ref, held[i], keep(sum_ref, lanes[i]))
        rows.bind(held[3])
        flows, flow_rows = [Flow(t) for t in large], Flow(rows)
        second_copy = pltpu.make_async_copy(second_ref, first_ref, copy_sems.at[0])
        second_copy.start()
        tiles = units // FF_TILE

        def columns_of(index):
            return pl.ds(pl.multiple_of(index * FF_TILE, FF_TILE), FF_TILE)

        def loads(index):
            slot, column = lax.rem(index, 2), columns_of(index)
            pairs = (
                (slope_ref.at[:, column], slopes.at[slot]),
                (up_ref.at[:, column], ups.at[slot]),
                (weight_ref.at[column, :], weights.at[slot]),
            )
            return [
                pltpu.make_async_copy(source, target, in_sems.at[slot, which])
                for which, (source, target) in enumerate(pairs)
            ]

        def store(index):
            slot = lax.rem(index, 2)
            return pltpu.make_async_copy(
                parts.at[slot], part_ref.at[columns_of(index), :], out_sems.at[slot]
            )

        for copy in loads(0):
            copy.start()
        rows.buffer[rows.place] = cls_ref[...]
        greet(joint)
        move(flows, flow_rows)

        events = [
            (when, at, plan(*[flow_rows if which == 3 else flows[which] for which in moved]))
            for when, at, moved in FEED_EVENTS
        ]

        def unit_tile(index, carry):
            column, slot = columns_of(index), lax.rem(index, 2)
            for copy in loads(index):
                copy.wait()

            @pl.when(index + 1 < tiles)
            def _():
                for copy in loads(index + 1):
                    copy.start()

            @pl.when(index == 0)
            def _():
                second_copy.wait()

            @pl.when(index >= 2)
            def _():
                store(index - 2).wait()

            places = iter(range(FEED_PLACES))

            def meet():
                place = next(places)
                for when, at, moved in events:
                    if at == place:

                        @pl.when(index == when)
                        def _():
                            for advance in moved:
                                advance()

            bias = 0.0
            for start in range(0, tokens, ROW_TILE):
                here = pl.ds(start, ROW_TILE)
                grad = dot_nt(branch_ref[here, :], weights[slot])
                pre = (grad * slopes[slot, here, :].astype(F32)).astype(BF16)
                bias = bias + jnp.sum(pre.astype(F32), axis=0, keepdims=True)
                pre_t[:, here] = pre.T
                first_ref[here, :] = first_ref[here, :] + dot_nt(pre, ups[slot])
                meet()
            bias_ref[:, column] = bias
            for start in range(0, FF_TILE, ROW_TILE):
                here = pl.ds(start, ROW_TILE)
                parts[slot, here, :] = dot_nn(pre_t[here, :], normed_ref[...]).astype(BF16)
                meet()
            store(index).start()
            return carry

        lax.fori_loop(0, tiles, unit_tile, 0)
        for index in range(max(tiles - 2, 0), tiles):
            store(index).wait()
        for which in FEED_TAIL:
            move((flows + [flow_rows])[which])
        while any(flow.open() for flow in flows + [flow_rows]):
            move(flows, flow_rows)
        out_copy = pltpu.make_async_copy(rows.buffer, all_ref, copy_sems.at[1])
        out_copy.start()
        out_copy.wait()
        for t in everything:
            t.drain()

    vmem, anywhere = pl.BlockSpec(memory_space=pltpu.VMEM), pl.BlockSpec(memory_space=pl.ANY)
    return pl.pallas_call(
        kernel,
        in_specs=[vmem, anywhere, vmem] + [anywhere] * 4 + [vmem],
        out_specs=[vmem, anywhere, vmem, vmem, anywhere],
        out_shape=[
            jax.ShapeDtypeStruct((tokens, width), F32),
            jax.ShapeDtypeStruct((units, width), BF16),
            jax.ShapeDtypeStruct((1, units), F32),
            jax.ShapeDtypeStruct(down.shape[1:], F32),
            jax.ShapeDtypeStruct((1 << len(joint),) + cls.shape, F32),
        ],
        scratch_shapes=[
            pltpu.VMEM((FF_TILE, tokens), BF16),
            pltpu.VMEM((2, tokens, FF_TILE), BF16),
            pltpu.VMEM((2, width, FF_TILE), BF16),
            pltpu.VMEM((2, FF_TILE, width), BF16),
            pltpu.VMEM((2, FF_TILE, width), BF16),
            pltpu.SemaphoreType.DMA((2,)),
            pltpu.SemaphoreType.DMA((2, 3)),
            pltpu.SemaphoreType.DMA((2,)),
        ]
        + [x for t in everything for x in t.scratch()],
        compiler_params=pltpu.CompilerParams(
            collective_id=0, has_side_effects=True, vmem_limit_bytes=62 * 1024 * 1024
        ),
    )(grad_branch, slope, normed_low, up_weight, down_weight, grad_second, down, cls)


BACK_EVENTS = (
    (
        (3, "o0 o1"),
        (4, "u0 u1 u2"),
        (9, "o0 o1"),
    ),
    (
        (2, "f0 f1 o0 o1"),
        (3, "u0 u2"),
        (4, "u1"),
        (5, "o0 o1"),
        (9, "u2 o0 o1"),
        (10, "f0"),
        (11, "f1 u0"),
    ),
)
GRAD_EVENTS = ("u1", "m u2 o0 o1", "w0 w1 f0 f1", "u0 o0")
BACK_TAIL = (
    "u1 m o1 u2",
    "m o1 o0 w1",
    "w0 m f0 f1",
    "u0 u1 o0 w0",
    "m o1 o0 w1",
    "f0 f1 o1 w0",
    "s0 w1 s1 s0",
    "s1 s0 s1 s0",
    "s1",
)


def back_all(head_bits, dp_bits, far, own, rows_in, grad_first_in, up, out, vector):
    joint = dp_bits + head_bits
    order = orders(head_bits, dp_bits)
    low_head, low_dp = list(reversed(head_bits)), list(reversed(dp_bits))
    dp_order = (low_dp, low_dp[1:2] + low_dp[:1] + low_dp[2:])
    far_bit, join_bits = head_bits[0], low_head[:-1]
    tokens, width = rows_in.shape
    seqs, _, length, _ = far[5].shape
    half = far[0].shape[1]
    pairs = half // LANES
    steps = pairs * seqs
    local = half >> len(join_bits)
    chunks = local // HEAD_DIM
    tiles = 3 * local // TILE
    chunk_tiles = HEAD_DIM // TILE
    middle = width // 2
    lanes = ((0, middle), (middle, middle))
    third = width // 3
    thirds = [(i * third, third) for i in range(3)]
    large = [Scatter(up.shape, thirds[i], joint, order[i], far=True) for i in range(3)]
    out_bits = [halvings(out.shape[0], order[i]) for i in range(2)]
    outs = [Scatter(out.shape, lanes[i], out_bits[i], order[i]) for i in range(2)]
    outs_back = [
        Gather((out.shape[0] >> len(out_bits[i]), TILE, middle), BF16, out_bits[i][::-1])
        for i in range(2)
    ]
    source = (tiles << len(join_bits), TILE, width)
    qkv_bits = [halvings(tiles, dp_order[i]) for i in range(2)]
    far_sums, own_sums = [
        [
            Scatter(source, lanes[i], join_bits + qkv_bits[i], join_bits + dp_order[i])
            for i in range(2)
        ]
        for _ in range(2)
    ]
    last = (tiles >> len(qkv_bits[0]), TILE, middle)
    swaps = [Swap(last, far_bit) for i in range(2)]
    sums_back = [Gather(last, BF16, qkv_bits[i][::-1]) for i in range(2)]
    vector_rows = vector.shape[0]
    bias_rows = 2 * width // LANES
    small = Total((vector_rows + bias_rows, LANES), order[0])
    groups = [large, outs, outs_back, far_sums, own_sums, swaps, sums_back, [small]]
    everything = [t for group in groups for t in group]

    def kernel(*refs):
        refs = list(refs)
        halves = [[refs.pop(0) for _ in range(6)] for _ in range(2)]
        rows_ref, first_ref, up_ref, out_ref, vector_ref = [refs.pop(0) for _ in range(5)]
        in_ref, up_sum, out_sum, qkv_sum, vector_sum = [refs.pop(0) for _ in range(5)]
        grads, sources = [refs.pop(0) for _ in range(2)], [refs.pop(0) for _ in range(2)]
        weights = [refs.pop(0) for _ in range(2)]
        partial, probs_buffer, probs_sems, first_sem = [refs.pop(0) for _ in range(4)]
        held = {id(t): take(refs, t) for t in everything}
        side = mine_of(*far_bit)

        def hand_on(gather):
            def store(index, total):
                gather.buffer[gather.own(index)] = total.astype(BF16)

            return store

        for t in outs_back + sums_back + [small]:
            t.bind(held[id(t)])
        for i, t in enumerate(large):
            t.bind(up_ref, held[id(t)], keep(up_sum, thirds[i]))
        for i in range(2):
            outs[i].bind(out_ref, held[id(outs[i])], hand_on(outs_back[i]))
            far_sums[i].bind(sources[0], held[id(far_sums[i])])
            own_sums[i].bind(sources[1], held[id(own_sums[i])])
            swaps[i].bind(far_sums[i].slots[-1], held[id(swaps[i])])
        flows = {f"u{i}": Flow(t) for i, t in enumerate(large)}
        for i in range(2):
            flows[f"o{i}"] = Flow(outs[i], outs_back[i])
            flows[f"f{i}"] = Flow(far_sums[i], swaps[i])
            flows[f"w{i}"] = Flow(own_sums[i])
            flows[f"s{i}"] = Flow(sums_back[i])
        flows["m"] = Flow(small)

        def merge(i):
            def add(index, carry):
                sums_back[i].buffer[sums_back[i].own(index)] = (
                    own_sums[i].slots[-1][index] + swaps[i].slot[index]
                )
                return carry

            lax.fori_loop(0, last[0], add, 0)

        def ready(name):
            return not (name[0] == "s" and flows[name].at < 0) or not (
                flows["w" + name[1]].open() or flows["f" + name[1]].open()
            )

        def planned(names):
            found = []
            for name in names.split():
                if flows[name].open() and ready(name):
                    if name[0] == "s" and flows[name].at < 0:
                        found.append(functools.partial(merge, int(name[1])))
                    found.append(flows[name].plan())
            return found

        def go(names):
            for advance in planned(names):
                advance()

        def probs_copy(which, step):
            slot = lax.rem(step, 2)
            return pltpu.make_async_copy(
                halves[which][5].at[lax.rem(step, seqs), pl.ds(lax.div(step, seqs) * PAIR, PAIR)],
                probs_buffer.at[slot],
                probs_sems.at[slot],
            )

        late_copies = [pltpu.make_async_copy(first_ref, in_ref, first_sem.at[2])] + [
            pltpu.make_async_copy(halves[i][4], weights[i], first_sem.at[i]) for i in range(2)
        ]
        probs_copy(0, 0).start()
        for copy in late_copies:
            copy.start()
        small.held[0, :vector_rows] = vector_ref[...]
        small.held[0, vector_rows:] = jnp.zeros((bias_rows, LANES), F32)
        greet(joint)
        go("u0 u1 u2 o0 o1")

        def attend_step(which, step, meet):
            query_ref, key_ref, value_ref, grad_ref, _, _ = halves[which]
            pair, seq = lax.div(step, seqs), lax.rem(step, seqs)
            at = (
                pl.ds(pl.multiple_of(seq * length, length), length),
                pl.ds(pl.multiple_of(pair * LANES, LANES), LANES),
            )
            probs_copy(which, step).wait()

            @pl.when(step + 1 < steps)
            def _():
                probs_copy(which, step + 1).start()

            if which == 0:

                @pl.when(step + 1 == steps)
                def _():
                    probs_copy(1, 0).start()

            query, value, grad = query_ref[at], value_ref[at], grad_ref[at]
            key_t = key_ref[at].T
            grad_key = grad_value = 0.0
            grad_query = []
            slot = lax.rem(step, 2)
            for head in range(PAIR):
                own_query = (head_lanes(query, head) * SCALE).astype(BF16)
                own_value = head_lanes(value, head).astype(BF16)
                own_grad = head_lanes(grad, head).astype(BF16)
                low = probs_buffer[slot, head]
                probs = low.astype(F32)
                grad_probs = dot_nt(own_value, grad)
                weighted = jnp.sum(probs * grad_probs, axis=0, keepdims=True)
                grad_scores = (probs * (grad_probs - weighted)).astype(BF16)
                grad_value += dot_nn(low, own_grad)
                grad_key += dot_nn(grad_scores, own_query)
                head_rows = slice(head * HEAD_DIM, (head + 1) * HEAD_DIM)
                grad_query.append(dot_nn(key_t[head_rows], grad_scores))
                if head == 0:
                    meet()
            query_t = (jnp.concatenate(grad_query, axis=0) * SCALE).astype(BF16)
            own = [query_t.T, grad_key.astype(BF16), grad_value.astype(BF16)]
            for kind in range(3):
                column = pl.multiple_of(kind * half + pair * LANES, LANES)
                grads[which][at[0], pl.ds(column, LANES)] = own[kind]
            stacked = jnp.concatenate([query_t, own[1].T, own[2].T], axis=0)
            part = dot_nn(stacked, rows_ref[at[0], :])
            group = (side if which == 1 else 1 - side) * pairs + pair
            for kind, block in ((0, own[0]), (1, own[2])):
                row = vector_rows + kind * (bias_rows // 2) + group
                total = jnp.sum(block.astype(F32), axis=0, keepdims=True)
                small.held[0, pl.ds(row, 1)] = small.held[0, pl.ds(row, 1)] + total

            @pl.when(seq == 0)
            def _():
                partial[...] = part

            @pl.when(seq > 0)
            def _():
                partial[...] = partial[...] + part

            @pl.when(seq == seqs - 1)
            def _():
                for kind in range(3):
                    for one in range(PAIR):
                        chunk = pair * PAIR + one
                        tile = lax.div(chunk, chunks) * tiles + kind * (local // TILE)
                        tile = tile + lax.rem(chunk, chunks) * chunk_tiles
                        start = kind * LANES + one * HEAD_DIM
                        block = partial[start : start + HEAD_DIM, :]
                        sources[which][pl.ds(tile, chunk_tiles)] = block.reshape(
                            chunk_tiles, TILE, width
                        ).astype(BF16)

        def sweep(which, events):
            events = [(when, planned(names)) for when, names in events]

            def step(index, carry):
                places = iter(range(2))

                def meet():
                    place = next(places)
                    for when, moved in events:
                        if when % 2 == place:

                            @pl.when(index == when // 2)
                            def _():
                                for advance in moved:
                                    advance()

                attend_step(which, index, meet)
                meet()
                return carry

            lax.fori_loop(0, steps, step, 0)

        sweep(0, BACK_EVENTS[0])
        go("f0 f1")
        sweep(1, BACK_EVENTS[1])
        go("w0 w1 m")
        for copy in late_copies:
            copy.wait()

        def input_rows(index, carry):
            at = pl.ds(pl.multiple_of(index * ROW_TILE, ROW_TILE), ROW_TILE)
            in_ref[at, :] = (
                in_ref[at, :]
                + dot_nn(grads[0][at, :], weights[0][...])
                + dot_nn(grads[1][at, :], weights[1][...])
            )
            return carry

        blocks = tokens // ROW_TILE
        parts = len(GRAD_EVENTS)
        for part, names in enumerate(GRAD_EVENTS):
            lax.fori_loop(blocks * part // parts, blocks * (part + 1) // parts, input_rows, 0)
            go(names)
        for names in BACK_TAIL:
            go(names)
        while any(flow.open() for flow in flows.values()):
            go(" ".join(flows))
        for i in range(2):
            for gather, target in ((outs_back[i], out_sum), (sums_back[i], qkv_sum)):

                def spread(index, carry, gather=gather, target=target, lane=lanes[i]):
                    target[index, :, pl.ds(*lane)] = gather.buffer[index].astype(F32)
                    return carry

                lax.fori_loop(0, gather.buffer.shape[0], spread, 0)
        vector_sum[...] = small.held[len(small.order)]
        for t in everything:
            t.drain()

    vmem, anywhere = pl.BlockSpec(memory_space=pltpu.VMEM), pl.BlockSpec(memory_space=pl.ANY)
    half_specs = [vmem] * 4 + [anywhere] * 2
    return pl.pallas_call(
        kernel,
        in_specs=half_specs * 2 + [vmem, anywhere, anywhere] + [vmem] * 2,
        out_specs=[vmem] * 5,
        out_shape=[
            jax.ShapeDtypeStruct((tokens, width), F32),
            jax.ShapeDtypeStruct(up.shape[1:], F32),
            jax.ShapeDtypeStruct(out.shape, F32),
            jax.ShapeDtypeStruct((tiles, TILE, width), F32),
            jax.ShapeDtypeStruct(small.shape, F32),
        ],
        scratch_shapes=[pltpu.VMEM((tokens, 3 * half), BF16)] * 2
        + [pltpu.VMEM(source, BF16)] * 2
        + [pltpu.VMEM((3 * half, width), BF16)] * 2
        + [
            pltpu.VMEM((3 * LANES, width), F32),
            pltpu.VMEM((2, PAIR, length, length), BF16),
            pltpu.SemaphoreType.DMA((2,)),
            pltpu.SemaphoreType.DMA((3,)),
        ]
        + [x for t in everything for x in t.scratch()],
        compiler_params=pltpu.CompilerParams(
            collective_id=1, has_side_effects=True, vmem_limit_bytes=62 * 1024 * 1024
        ),
    )(*far, *own, rows_in, grad_first_in, up, out, vector)


def classify(cls_rows, labels, w_pool, b_pool, w_class, b_class):
    pooled = jnp.tanh(jnp.dot(cls_rows, w_pool, preferred_element_type=F32) + b_pool)
    class_weight = w_class.astype(F32)
    logits = jnp.dot(pooled, class_weight, precision=lax.Precision.HIGHEST) + b_class
    onehot = (labels[:, None] == jnp.arange(logits.shape[1])[None, :]).astype(F32)
    ramp_loss = jax.nn.logsumexp(logits, axis=-1) - jnp.sum(logits * onehot, axis=-1)
    grad_logits = jax.nn.softmax(logits, axis=-1) - onehot
    grad_pool = (
        jnp.dot(grad_logits, class_weight.T, precision=lax.Precision.HIGHEST)
        * (1.0 - pooled * pooled)
    ).astype(BF16)
    return pooled, ramp_loss, grad_logits, grad_pool


def body(
    hidden_in,
    lengths,
    labels,
    query_key_value_weight,
    query_value_bias,
    attention_output_weight,
    attention_output_bias,
    gain_att,
    shift_att,
    up_weight,
    up_bias,
    down_weight,
    down_bias,
    gain_ffn,
    shift_ffn,
    w_pool,
    b_pool,
    w_class,
    b_class,
    cotangent,
):
    seq_here, seq_len, width = hidden_in.shape
    tokens = seq_here * seq_len
    everyone = ("dp", "head")
    head_bits = bits_of(("head",))
    dp_bits = bits_of(("dp",))
    rows_in = hidden_in.reshape(tokens, width)

    half_bits, far_bit = head_bits[1:], head_bits[0]
    own_weight = jnp.transpose(query_key_value_weight, (2, 0, 1))
    own_weight = own_weight.transpose(1, 0, 2)
    far_weight = exchange(own_weight, *far_bit)
    far_bias = exchange(query_value_bias, *far_bit)
    low_order = list(reversed(half_bits))

    def join(blocks, order):
        for axis, bit in order:
            got = exchange(blocks, axis, bit)
            blocks = jnp.where(
                own_bit(axis, bit) == 0,
                jnp.concatenate([blocks, got], axis=1),
                jnp.concatenate([got, blocks], axis=1),
            )
        return blocks

    halves = []
    for weight, bias in ((own_weight, query_value_bias), (far_weight, far_bias)):
        weight, bias = join(weight, low_order), join(bias, low_order)
        query = (dot_nt(rows_in, weight[0]) + bias[0]).astype(BF16)
        key = dot_nt(rows_in, weight[1]).astype(BF16)
        value = (dot_nt(rows_in, weight[2]) + bias[1]).astype(BF16)
        context, probs = attend(lengths, query, key, value)
        halves.append((weight, query, key, value, context, probs))
    half_width = halves[0][1].shape[1]
    far_side = own_bit(*far_bit)

    def in_place(own, far, axis):
        return jnp.where(
            far_side == 0,
            jnp.concatenate([own, far], axis=axis),
            jnp.concatenate([far, own], axis=axis),
        )

    combined = in_place(halves[0][4], halves[1][4], 1)
    attended = (
        jnp.dot(combined, attention_output_weight, preferred_element_type=F32)
        + attention_output_bias
    )
    first_in = rows_in.astype(F32) + attended
    normalized_first = normalize(first_in, gain_att, shift_att)
    normed_low = normalized_first.astype(BF16)
    gelu_output, slope, branch = feed_forward(
        normed_low, up_weight, up_bias, down_weight, down_bias
    )
    second_in = normalized_first + branch
    output_rows = normalize(second_in, gain_ffn, shift_ffn)
    hidden_out = output_rows.astype(BF16).reshape(seq_here, seq_len, width)
    cls_rows = hidden_out[:, 0, :]
    pooled, ramp_loss, grad_logits, grad_pool = classify(
        cls_rows, labels, w_pool, b_pool, w_class, b_class
    )
    grad_cls = jnp.dot(grad_pool, w_pool.T, preferred_element_type=F32)
    classes = grad_logits.shape[1]
    cls_pack = jnp.concatenate(
        [
            cls_rows.astype(F32),
            grad_pool.astype(F32),
            pooled,
            jnp.pad(grad_logits, ((0, 0), (0, LANES - classes))),
        ],
        axis=1,
    )
    pack_width = cls_pack.shape[1]
    cls_pack = cls_pack.reshape(-1, LANES)

    grad_output = cotangent.astype(F32).at[:, 0, :].add(grad_cls).reshape(tokens, width)
    _, second_back = jax.vjp(normalize, second_in, gain_ffn, shift_ffn)
    grad_second, grad_gain_ffn, grad_shift_ffn = second_back(grad_output)
    grad_branch = grad_second.astype(BF16)
    grad_b_down = jnp.sum(grad_branch, axis=0, dtype=F32)
    part_w_down = jnp.dot(gelu_output.T, grad_branch, preferred_element_type=F32).astype(BF16)
    devices = lax.axis_size("dp") * lax.axis_size("head")
    grad_first, part_w_up, grad_b_up, grad_w_down, cls_all = feed_back(
        head_bits,
        dp_bits,
        grad_branch,
        slope,
        normed_low,
        up_weight,
        down_weight,
        grad_second,
        part_w_down.reshape(devices, -1, width),
        cls_pack,
    )
    grad_b_up = grad_b_up[0]
    _, first_back = jax.vjp(normalize, first_in, gain_att, shift_att)
    grad_first_in, grad_gain_att, grad_shift_att = first_back(grad_first)
    grad_attended = grad_first_in.astype(BF16)
    grad_b_out = jnp.sum(grad_attended, axis=0, dtype=F32)
    part_w_out = jnp.dot(combined.T, grad_attended, preferred_element_type=F32).astype(BF16)
    grad_context = dot_nt(grad_attended, attention_output_weight).astype(BF16)
    far_context = lax.dynamic_slice_in_dim(
        grad_context, (1 - far_side) * half_width, half_width, 1
    )
    own_context = lax.dynamic_slice_in_dim(grad_context, far_side * half_width, half_width, 1)
    local = query_key_value_weight.shape[2]
    vectors = [
        grad_b_out,
        grad_gain_att,
        grad_shift_att,
        grad_b_up,
        grad_b_down,
        grad_gain_ffn,
        grad_shift_ffn,
    ]
    far, own = [
        (half[1], half[2], half[3], grad_half, half[0].reshape(-1, width), half[5])
        for half, grad_half in ((halves[1], far_context), (halves[0], own_context))
    ]
    grad_in, grad_w_up, grad_w_out, qkv, sums = back_all(
        head_bits,
        dp_bits,
        far,
        own,
        rows_in,
        grad_first_in,
        part_w_up.reshape(devices, -1, width),
        part_w_out.reshape(-1, TILE, width),
        jnp.concatenate(vectors).reshape(-1, LANES),
    )
    grad_w_up = grad_w_up.T
    grad_w_out = grad_w_out.reshape(width, width)
    grad_w_qkv = jnp.transpose(qkv.reshape(3, local, width), (0, 2, 1))
    edges, reached = [], 0
    for vector in vectors:
        reached += vector.shape[0]
        edges.append(reached)
    (
        grad_b_out,
        grad_gain_att,
        grad_shift_att,
        grad_b_up,
        grad_b_down,
        grad_gain_ffn,
        grad_shift_ffn,
        bias_all,
    ) = jnp.split(sums.reshape(-1), edges)
    grad_b_qv = lax.dynamic_slice_in_dim(
        bias_all.reshape(2, width), lax.axis_index("head") * local, local, 1
    )
    cls_all = cls_all.reshape(-1, pack_width)
    all_cls, all_pool, pooled = jnp.split(cls_all[:, : 3 * width], 3, axis=1)
    grad_logits = cls_all[:, 3 * width : 3 * width + classes]
    grad_b_class = jnp.sum(grad_logits, axis=0)
    grad_w_class = jnp.dot(pooled.T, grad_logits, precision=lax.Precision.HIGHEST)
    grad_b_pool = jnp.sum(all_pool, axis=0)
    grad_w_pool = jnp.dot(
        all_cls.T.astype(BF16), all_pool.astype(BF16), preferred_element_type=F32
    )
    return (
        hidden_out,
        ramp_loss,
        grad_in.reshape(seq_here, seq_len, width),
        grad_w_qkv,
        grad_b_qv,
        grad_w_out,
        grad_b_out,
        grad_gain_att,
        grad_shift_att,
        grad_w_up,
        grad_b_up,
        grad_w_down,
        grad_b_down,
        grad_gain_ffn,
        grad_shift_ffn,
        grad_w_pool,
        grad_b_pool,
        grad_w_class,
        grad_b_class,
    )


def solution(mesh):
    rows = P(("dp", "head"))
    placed = (
        (P(("dp", "head"), None, None), rows, rows, P(None, None, "head"), P(None, "head"))
        + (P(),) * 14
        + (P(("dp", "head"), None, None),)
    )
    tokens = P(("dp", "head"), None, None)
    outs = (
        (tokens, rows, tokens, P(None, None, "head"), P(None, "head"))
        + (P(),) * 4
        + (P(None, ("dp", "head")), P(), P(("dp", "head"), None))
        + (P(),) * 7
    )
    return jax.shard_map(body, mesh=mesh, in_specs=placed, out_specs=outs, check_vma=False)
```

```python
import functools

import jax
import jax.numpy as jnp
from jax import lax
from jax.experimental import pallas as pl
from jax.experimental.pallas import tpu as pltpu
from jax.sharding import PartitionSpec as P

HEAD_DIM = 64
EPSILON = 1e-06
MASKED = -1000000000.0
BF16, F32 = jnp.bfloat16, jnp.float32


def bit_count(n):
    assert n & (n - 1) == 0
    return n.bit_length() - 1


def exchange(value, axis, bit):
    size = lax.axis_size(axis)
    step = 1 << bit
    return lax.ppermute(value, axis, [(i, i ^ step) for i in range(size)])


def own_bit(axis, bit):
    return (lax.axis_index(axis) >> bit) & 1


def bits_of(axes):
    found = []
    for axis in axes:
        found += [(axis, b) for b in reversed(range(bit_count(lax.axis_size(axis))))]
    return found


def normalize(row_block, gain_row, shift_row):
    center = jnp.mean(row_block, axis=-1, keepdims=True)
    centered = row_block - center
    spread = jnp.mean(centered * centered, axis=-1, keepdims=True)
    return centered * lax.rsqrt(spread + EPSILON) * gain_row + shift_row


LANES = 128
PAIR = LANES // HEAD_DIM
SCALE = HEAD_DIM ** (-0.5)


def dot_nt(left, right):
    return lax.dot_general(left, right, (((1,), (1,)), ((), ())), preferred_element_type=F32)


def dot_nn(left, right):
    return jnp.dot(left, right, preferred_element_type=F32)


def head_lanes(block, head):
    lane = lax.broadcasted_iota(jnp.int32, block.shape, 1)
    inside = (lane >= head * HEAD_DIM) & (lane < (head + 1) * HEAD_DIM)
    return jnp.where(inside, block.astype(F32), 0.0)


def attend_kernel(length_ref, query_ref, key_ref, value_ref, context_ref, probs_ref):
    length = length_ref[pl.program_id(0)]
    query, key = query_ref[...], key_ref[...]
    value_t = value_ref[...].T
    rows = query.shape[0]
    key_at = lax.broadcasted_iota(jnp.int32, (rows, rows), 0)
    contexts = []
    for head in range(PAIR):
        own_query = (head_lanes(query, head) * SCALE).astype(BF16)
        scores = jnp.where(key_at < length, dot_nt(key, own_query), MASKED)
        shifted = jnp.exp(scores - jnp.max(scores, axis=0, keepdims=True))
        inverse = 1.0 / jnp.sum(shifted, axis=0, keepdims=True)
        probs = (shifted * inverse).astype(BF16)
        probs_ref[0, head] = probs
        contexts.append(dot_nn(value_t[head * HEAD_DIM : (head + 1) * HEAD_DIM], probs))
    context_ref[...] = jnp.concatenate(contexts, axis=0).T.astype(BF16)


def attend(lengths, query, key, value):
    seqs = lengths.shape[0]
    tokens, width = query.shape
    rows, pairs = tokens // seqs, width // LANES
    block = pl.BlockSpec((rows, LANES), lambda s, p: (s, p))
    return pl.pallas_call(
        attend_kernel,
        grid=(seqs, pairs),
        in_specs=[pl.BlockSpec(memory_space=pltpu.SMEM), block, block, block],
        out_specs=[block, pl.BlockSpec((1, PAIR, rows, rows), lambda s, p: (s, p, 0, 0))],
        out_shape=[
            jax.ShapeDtypeStruct((tokens, width), BF16),
            jax.ShapeDtypeStruct((seqs, pairs * PAIR, rows, rows), BF16),
        ],
        cost_estimate=pl.CostEstimate(
            flops=seqs * pairs * 12 * rows * rows * LANES,
            bytes_accessed=8 * tokens * width + 4 * tokens * rows * pairs,
            transcendentals=0,
        ),
    )(lengths, query, key, value)


def gelu_parts(values):
    bell = jnp.exp(-0.5 * values * values)
    inner = 1.0 / (1.0 + (0.3275911 * 0.5**0.5) * jnp.abs(values))
    series = 0.5 * 1.061405429
    for term in (-1.453152027, 1.421413741, -0.284496736, 0.254829592):
        series = series * inner + 0.5 * term
    tail = series * inner * bell
    below = jnp.where(values < 0.0, tail, 1.0 - tail)
    return values * below, below + values * bell * 0.3989422804014327


FF_TILE = 512
ROW_TILE = 256


def feed_kernel(rows_ref, up_ref, up_bias_ref, down_ref, down_bias_ref, act_ref, slope_ref, out_ref):
    first = pl.program_id(0) == 0

    @pl.when(first)
    def _():
        out_ref[...] = jnp.broadcast_to(down_bias_ref[...], out_ref.shape)

    for start in range(0, rows_ref.shape[0], ROW_TILE):
        here = pl.ds(start, ROW_TILE)
        before = dot_nn(rows_ref[here, :], up_ref[...]) + up_bias_ref[...]
        active, slope = gelu_parts(before)
        active = active.astype(BF16)
        act_ref[here, :] = active
        slope_ref[here, :] = slope.astype(BF16)
        out_ref[here, :] += dot_nn(active, down_ref[...])


def feed_forward(rows, up_weight, up_bias, down_weight, down_bias):
    tokens, width = rows.shape
    units = up_weight.shape[1]
    whole = lambda shape: pl.BlockSpec(shape, lambda i: (0, 0))
    columns = lambda height: pl.BlockSpec((height, FF_TILE), lambda i: (0, i))
    return pl.pallas_call(
        feed_kernel,
        grid=(units // FF_TILE,),
        in_specs=[
            whole((tokens, width)),
            columns(width),
            columns(1),
            pl.BlockSpec((FF_TILE, width), lambda i: (i, 0)),
            whole((1, width)),
        ],
        out_specs=[columns(tokens), columns(tokens), whole((tokens, width))],
        out_shape=[
            jax.ShapeDtypeStruct((tokens, units), BF16),
            jax.ShapeDtypeStruct((tokens, units), BF16),
            jax.ShapeDtypeStruct((tokens, width), F32),
        ],
        cost_estimate=pl.CostEstimate(
            flops=8 * tokens * width * units,
            bytes_accessed=4 * tokens * units + 4 * width * units,
            transcendentals=0,
        ),
    )(rows, up_weight, up_bias[None], down_weight, down_bias[None])


MESH = pl.DeviceIdType.MESH


def mine_of(axis, bit):
    return lax.rem(lax.div(lax.axis_index(axis), 1 << bit), 2)


def partner_of(axis, bit):
    return {axis: lax.axis_index(axis) + (1 << bit) * (1 - 2 * mine_of(axis, bit))}


def place_of(bits):
    place = 0
    for axis, bit in bits:
        place = 2 * place + mine_of(axis, bit)
    return place


def greet(bits):
    barrier = pltpu.get_barrier_semaphore()
    for axis, bit in bits:
        pl.semaphore_signal(
            barrier, inc=1, device_id=partner_of(axis, bit), device_id_type=MESH
        )
    pl.semaphore_wait(barrier, len(bits))


def copy_to(source, target, sems, bit):
    return pltpu.make_async_remote_copy(
        src_ref=source,
        dst_ref=target,
        send_sem=sems.at[0],
        recv_sem=sems.at[1],
        device_id=partner_of(*bit),
        device_id_type=MESH,
    )


class Scatter:
    def __init__(self, shape, lanes, joint, order, far=False):
        self.shape, self.lanes, self.joint, self.order = shape, lanes, joint, order
        self.far = far

    def blocks(self, stage):
        halved = len([bit for bit in self.order[:stage] if bit in self.joint])
        return self.shape[0] >> halved

    def scratch(self):
        rows, width = self.shape[1], self.lanes[1]
        return [
            pltpu.VMEM((self.blocks(stage + 1), rows, width), BF16)
            for stage in range(len(self.order))
        ] + (
            [
                pltpu.VMEM((self.blocks(1), rows, width), BF16),
                pltpu.SemaphoreType.DMA(()),
            ]
            if self.far
            else []
        ) + [pltpu.SemaphoreType.DMA((len(self.order), 2))]

    def bind(self, source, scratch, last=None):
        self.source, self.sems, self.last = source, scratch[-1], last
        self.slots = scratch[: len(self.order)]
        if self.far:
            self.kept, self.kept_sem = scratch[len(self.order) : -1]
        return self

    def split(self, stage):
        bit = self.order[stage]
        if bit not in self.joint:
            return 1, self.blocks(stage), None
        left = [b for b in self.joint if b not in self.order[:stage]]
        high = 1 << left.index(bit)
        return high, self.blocks(stage) // (2 * high), mine_of(*bit)

    def view(self, stage, at):
        if stage == 0:
            return self.source.at[at, :, pl.ds(*self.lanes)]
        return self.slots[stage - 1].at[at]

    def steps(self):
        return len(self.order)

    def start(self, stage):
        high, low, side = self.split(stage)

        def send(run, carry):
            at = 0 if side is None else (2 * run + 1 - side) * low
            copy_to(
                self.view(stage, pl.ds(at, low)),
                self.slots[stage].at[pl.ds(run * low, low)],
                self.sems.at[stage],
                self.order[stage],
            ).start()
            if self.far and stage == 0:
                pltpu.make_async_copy(
                    self.view(0, pl.ds((2 * run + side) * low, low)),
                    self.kept.at[pl.ds(run * low, low)],
                    self.kept_sem,
                ).start()
            return carry

        lax.fori_loop(0, high, send, 0)

    def whole(self, stage):
        slot = self.slots[stage]
        return copy_to(slot, slot, self.sems.at[stage], self.order[stage])

    def finish(self, stage):
        high, low, side = self.split(stage)
        slot = self.slots[stage]
        self.whole(stage).wait_recv()
        from_kept = self.far and stage == 0
        if from_kept:
            pltpu.make_async_copy(self.kept, self.kept, self.kept_sem).wait()
        final = stage + 1 == len(self.order) and self.last is not None

        def add(index, carry):
            kept = index
            if side is not None:
                kept = (2 * lax.div(index, low) + side) * low + lax.rem(index, low)
            mine = self.kept[index] if from_kept else self.view(stage, kept)[...]
            theirs = slot[index]
            if final:
                self.last(index, mine.astype(F32) + theirs.astype(F32))
            else:
                slot[index] = mine + theirs
            return carry

        lax.fori_loop(0, high * low, add, 0)

    def drain(self):
        for stage in range(len(self.order)):
            self.whole(stage).wait_send()


class Gather:
    def __init__(self, shape, dtype, order):
        self.shape, self.dtype, self.order = shape, dtype, order

    def scratch(self):
        count = self.shape[0] << len(self.order)
        return [
            pltpu.VMEM((count,) + self.shape[1:], self.dtype),
            pltpu.SemaphoreType.DMA((len(self.order), 2)),
        ]

    def bind(self, scratch):
        self.buffer, self.sems = scratch
        self.place = place_of(list(reversed(self.order)))
        return self

    def own(self, index):
        return self.place * self.shape[0] + index

    def steps(self):
        return len(self.order)

    def copy(self, stage, theirs):
        run = 1 << stage
        base = lax.div(self.place, run) * run
        if theirs:
            base = base + run * (1 - 2 * mine_of(*self.order[stage]))
        here = self.buffer.at[pl.ds(base * self.shape[0], run * self.shape[0])]
        return copy_to(here, here, self.sems.at[stage], self.order[stage])

    def start(self, stage):
        self.copy(stage, False).start()

    def finish(self, stage):
        self.copy(stage, True).wait_recv()

    def drain(self):
        for stage in range(len(self.order)):
            self.copy(stage, False).wait_send()

    def natural(self, position, bits):
        index = 0
        for bit in bits:
            index = 2 * index + lax.rem(lax.div(position, 1 << self.order.index(bit)), 2)
        return index


class Swap:
    def __init__(self, shape, bit):
        self.shape, self.bit = shape, bit

    def scratch(self):
        return [pltpu.VMEM(self.shape, BF16), pltpu.SemaphoreType.DMA((2,))]

    def bind(self, source, scratch):
        self.source, (self.slot, self.sems) = source, scratch
        return self

    def steps(self):
        return 1

    def copy(self):
        return copy_to(self.source, self.slot, self.sems, self.bit)

    def start(self, stage):
        self.copy().start()

    def finish(self, stage):
        self.copy().wait_recv()

    def drain(self):
        self.copy().wait_send()


class Total:
    def __init__(self, shape, order):
        self.shape, self.order = shape, order

    def scratch(self):
        return [
            pltpu.VMEM((len(self.order) + 1,) + self.shape, F32),
            pltpu.VMEM((len(self.order),) + self.shape, F32),
            pltpu.SemaphoreType.DMA((len(self.order), 2)),
        ]

    def bind(self, scratch):
        self.held, self.slots, self.sems = scratch
        return self

    def steps(self):
        return len(self.order)

    def copy(self, stage):
        return copy_to(
            self.held.at[stage], self.slots.at[stage], self.sems.at[stage], self.order[stage]
        )

    def start(self, stage):
        self.copy(stage).start()

    def finish(self, stage):
        self.copy(stage).wait_recv()
        self.held[stage + 1] = self.held[stage] + self.slots[stage]

    def drain(self):
        for stage in range(len(self.order)):
            self.copy(stage).wait_send()


def take(scratch, chain):
    count = len(chain.scratch())
    return [scratch.pop(0) for _ in range(count)]


class Flow:
    def __init__(self, *transfers):
        self.todo = [(t, stage) for t in transfers for stage in range(t.steps())]
        self.at = -1

    def plan(self):
        at = self.at
        self.at += 1

        def advance():
            if at >= 0:
                transfer, stage = self.todo[at]
                transfer.finish(stage)
            if at + 1 < len(self.todo):
                transfer, stage = self.todo[at + 1]
                transfer.start(stage)

        return advance

    def open(self):
        return self.at < len(self.todo)


TILE = 8


def halvings(blocks, bits):
    count = 0
    while count < len(bits) and blocks % 2 == 0:
        blocks //= 2
        count += 1
    return bits[:count]


def orders(head_bits, dp_bits):
    low_head, low_dp = list(reversed(head_bits)), list(reversed(dp_bits))
    axes = low_head[-1:] + low_dp[:2]
    return [low_head[:-1] + axes[i:] + axes[:i] + low_dp[2:] for i in range(3)]


def plan(*flows):
    listed = [one for flow in flows for one in (flow if isinstance(flow, list) else [flow])]
    return [one.plan() for one in listed if one.open()]


def move(*flows):
    for advance in plan(*flows):
        advance()


def keep(target, lane):
    def store(index, total):
        target[:, pl.ds(*lane)] = total

    return store


FEED_PLACES = 6
FEED_EVENTS = (
    (1, 0, (3,)),
    (1, 2, (0, 1, 2,)),
    (1, 5, (3,)),
    (3, 3, (3,)),
    (4, 3, (0, 2,)),
    (4, 5, (1,)),
    (5, 1, (3,)),
    (5, 5, (3,)),
)
FEED_TAIL = (0, 2, 1, 0, 2, 1, 0, 2, 1)


def feed_back(head_bits, dp_bits, grad_branch, slope, normed_low, up_weight, down_weight, grad_second, down, cls):
    joint = dp_bits + head_bits
    order = orders(head_bits, dp_bits)
    tokens, width = grad_branch.shape
    units = up_weight.shape[1]
    third = width // 3
    lanes = [(i * third, third) for i in range(3)]
    large = [Scatter(down.shape, lanes[i], joint, order[i], far=True) for i in range(3)]
    rows = Gather((1,) + cls.shape, F32, order[0][::-1])
    everything = large + [rows]

    def kernel(
        branch_ref, slope_ref, normed_ref, up_ref, weight_ref, second_ref, down_ref, cls_ref,
        first_ref, part_ref, bias_ref, sum_ref, all_ref,
        pre_t, slopes, ups, weights, parts, copy_sems, in_sems, out_sems, *scratch
    ):
        scratch = list(scratch)
        held = [take(scratch, t) for t in everything]
        for i in range(3):
            large[i].bind(down_ref, held[i], keep(sum_ref, lanes[i]))
        rows.bind(held[3])
        flows, flow_rows = [Flow(t) for t in large], Flow(rows)
        second_copy = pltpu.make_async_copy(second_ref, first_ref, copy_sems.at[0])
        second_copy.start()
        tiles = units // FF_TILE

        def columns_of(index):
            return pl.ds(pl.multiple_of(index * FF_TILE, FF_TILE), FF_TILE)

        def loads(index):
            slot, column = lax.rem(index, 2), columns_of(index)
            pairs = (
                (slope_ref.at[:, column], slopes.at[slot]),
                (up_ref.at[:, column], ups.at[slot]),
                (weight_ref.at[column, :], weights.at[slot]),
            )
            return [
                pltpu.make_async_copy(source, target, in_sems.at[slot, which])
                for which, (source, target) in enumerate(pairs)
            ]

        def store(index):
            slot = lax.rem(index, 2)
            return pltpu.make_async_copy(
                parts.at[slot], part_ref.at[columns_of(index), :], out_sems.at[slot]
            )

        for copy in loads(0):
            copy.start()
        rows.buffer[rows.place] = cls_ref[...]
        greet(joint)
        move(flows, flow_rows)

        events = [
            (when, at, plan(*[flow_rows if which == 3 else flows[which] for which in moved]))
            for when, at, moved in FEED_EVENTS
        ]

        def unit_tile(index, carry):
            column, slot = columns_of(index), lax.rem(index, 2)
            for copy in loads(index):
                copy.wait()

            @pl.when(index + 1 < tiles)
            def _():
                for copy in loads(index + 1):
                    copy.start()

            @pl.when(index == 0)
            def _():
                second_copy.wait()

            @pl.when(index >= 2)
            def _():
                store(index - 2).wait()

            places = iter(range(FEED_PLACES))

            def meet():
                place = next(places)
                for when, at, moved in events:
                    if at == place:

                        @pl.when(index == when)
                        def _():
                            for advance in moved:
                                advance()

            bias = 0.0
            for start in range(0, tokens, ROW_TILE):
                here = pl.ds(start, ROW_TILE)
                grad = dot_nt(branch_ref[here, :], weights[slot])
                pre = (grad * slopes[slot, here, :].astype(F32)).astype(BF16)
                bias = bias + jnp.sum(pre.astype(F32), axis=0, keepdims=True)
                pre_t[:, here] = pre.T
                first_ref[here, :] = first_ref[here, :] + dot_nt(pre, ups[slot])
                meet()
            bias_ref[:, column] = bias
            for start in range(0, FF_TILE, ROW_TILE):
                here = pl.ds(start, ROW_TILE)
                parts[slot, here, :] = dot_nn(pre_t[here, :], normed_ref[...]).astype(BF16)
                meet()
            store(index).start()
            return carry

        lax.fori_loop(0, tiles, unit_tile, 0)
        for index in range(max(tiles - 2, 0), tiles):
            store(index).wait()
        for which in FEED_TAIL:
            move((flows + [flow_rows])[which])
        while any(flow.open() for flow in flows + [flow_rows]):
            move(flows, flow_rows)
        out_copy = pltpu.make_async_copy(rows.buffer, all_ref, copy_sems.at[1])
        out_copy.start()
        out_copy.wait()
        for t in everything:
            t.drain()

    vmem, anywhere = pl.BlockSpec(memory_space=pltpu.VMEM), pl.BlockSpec(memory_space=pl.ANY)
    return pl.pallas_call(
        kernel,
        in_specs=[vmem, anywhere, vmem] + [anywhere] * 4 + [vmem],
        out_specs=[vmem, anywhere, vmem, vmem, anywhere],
        out_shape=[
            jax.ShapeDtypeStruct((tokens, width), F32),
            jax.ShapeDtypeStruct((units, width), BF16),
            jax.ShapeDtypeStruct((1, units), F32),
            jax.ShapeDtypeStruct(down.shape[1:], F32),
            jax.ShapeDtypeStruct((1 << len(joint),) + cls.shape, F32),
        ],
        scratch_shapes=[
            pltpu.VMEM((FF_TILE, tokens), BF16),
            pltpu.VMEM((2, tokens, FF_TILE), BF16),
            pltpu.VMEM((2, width, FF_TILE), BF16),
            pltpu.VMEM((2, FF_TILE, width), BF16),
            pltpu.VMEM((2, FF_TILE, width), BF16),
            pltpu.SemaphoreType.DMA((2,)),
            pltpu.SemaphoreType.DMA((2, 3)),
            pltpu.SemaphoreType.DMA((2,)),
        ]
        + [x for t in everything for x in t.scratch()],
        compiler_params=pltpu.CompilerParams(
            collective_id=0, has_side_effects=True, vmem_limit_bytes=62 * 1024 * 1024
        ),
    )(grad_branch, slope, normed_low, up_weight, down_weight, grad_second, down, cls)


BACK_EVENTS = (
    (
        (3, "o0 o1"),
        (4, "u0 u1 u2"),
        (9, "o0 o1"),
    ),
    (
        (2, "f0 f1 o0 o1"),
        (3, "u0 u2"),
        (4, "u1"),
        (5, "o0 o1"),
        (9, "u2 o0 o1"),
        (10, "f0"),
        (11, "f1 u0"),
    ),
)
GRAD_EVENTS = ("u1", "m u2 o0 o1", "w0 w1 f0 f1", "u0 o0")
BACK_TAIL = (
    "u1 m o1 u2",
    "m o1 o0 w1",
    "w0 m f0 f1",
    "u0 u1 o0 w0",
    "m o1 o0 w1",
    "f0 f1 o1 w0",
    "s0 w1 s1 s0",
    "s1 s0 s1 s0",
    "s1",
)


def back_all(head_bits, dp_bits, far, own, rows_in, grad_first_in, up, out, vector):
    joint = dp_bits + head_bits
    order = orders(head_bits, dp_bits)
    low_head, low_dp = list(reversed(head_bits)), list(reversed(dp_bits))
    dp_order = (low_dp, low_dp[1:2] + low_dp[:1] + low_dp[2:])
    far_bit, join_bits = head_bits[0], low_head[:-1]
    tokens, width = rows_in.shape
    seqs, _, length, _ = far[5].shape
    half = far[0].shape[1]
    pairs = half // LANES
    steps = pairs * seqs
    local = half >> len(join_bits)
    chunks = local // HEAD_DIM
    tiles = 3 * local // TILE
    chunk_tiles = HEAD_DIM // TILE
    middle = width // 2
    lanes = ((0, middle), (middle, middle))
    third = width // 3
    thirds = [(i * third, third) for i in range(3)]
    large = [Scatter(up.shape, thirds[i], joint, order[i], far=True) for i in range(3)]
    out_bits = [halvings(out.shape[0], order[i]) for i in range(2)]
    outs = [Scatter(out.shape, lanes[i], out_bits[i], order[i]) for i in range(2)]
    outs_back = [
        Gather((out.shape[0] >> len(out_bits[i]), TILE, middle), BF16, out_bits[i][::-1])
        for i in range(2)
    ]
    source = (tiles << len(join_bits), TILE, width)
    qkv_bits = [halvings(tiles, dp_order[i]) for i in range(2)]
    far_sums, own_sums = [
        [
            Scatter(source, lanes[i], join_bits + qkv_bits[i], join_bits + dp_order[i])
            for i in range(2)
        ]
        for _ in range(2)
    ]
    last = (tiles >> len(qkv_bits[0]), TILE, middle)
    swaps = [Swap(last, far_bit) for i in range(2)]
    sums_back = [Gather(last, BF16, qkv_bits[i][::-1]) for i in range(2)]
    vector_rows = vector.shape[0]
    bias_rows = 2 * width // LANES
    small = Total((vector_rows + bias_rows, LANES), order[0])
    groups = [large, outs, outs_back, far_sums, own_sums, swaps, sums_back, [small]]
    everything = [t for group in groups for t in group]

    def kernel(*refs):
        refs = list(refs)
        halves = [[refs.pop(0) for _ in range(6)] for _ in range(2)]
        rows_ref, first_ref, up_ref, out_ref, vector_ref = [refs.pop(0) for _ in range(5)]
        in_ref, up_sum, out_sum, qkv_sum, vector_sum = [refs.pop(0) for _ in range(5)]
        grads, sources = [refs.pop(0) for _ in range(2)], [refs.pop(0) for _ in range(2)]
        weights = [refs.pop(0) for _ in range(2)]
        partial, probs_buffer, probs_sems, first_sem = [refs.pop(0) for _ in range(4)]
        held = {id(t): take(refs, t) for t in everything}
        side = mine_of(*far_bit)

        def hand_on(gather):
            def store(index, total):
                gather.buffer[gather.own(index)] = total.astype(BF16)

            return store

        for t in outs_back + sums_back + [small]:
            t.bind(held[id(t)])
        for i, t in enumerate(large):
            t.bind(up_ref, held[id(t)], keep(up_sum, thirds[i]))
        for i in range(2):
            outs[i].bind(out_ref, held[id(outs[i])], hand_on(outs_back[i]))
            far_sums[i].bind(sources[0], held[id(far_sums[i])])
            own_sums[i].bind(sources[1], held[id(own_sums[i])])
            swaps[i].bind(far_sums[i].slots[-1], held[id(swaps[i])])
        flows = {f"u{i}": Flow(t) for i, t in enumerate(large)}
        for i in range(2):
            flows[f"o{i}"] = Flow(outs[i], outs_back[i])
            flows[f"f{i}"] = Flow(far_sums[i], swaps[i])
            flows[f"w{i}"] = Flow(own_sums[i])
            flows[f"s{i}"] = Flow(sums_back[i])
        flows["m"] = Flow(small)

        def merge(i):
            def add(index, carry):
                sums_back[i].buffer[sums_back[i].own(index)] = (
                    own_sums[i].slots[-1][index] + swaps[i].slot[index]
                )
                return carry

            lax.fori_loop(0, last[0], add, 0)

        def ready(name):
            return not (name[0] == "s" and flows[name].at < 0) or not (
                flows["w" + name[1]].open() or flows["f" + name[1]].open()
            )

        def planned(names):
            found = []
            for name in names.split():
                if flows[name].open() and ready(name):
                    if name[0] == "s" and flows[name].at < 0:
                        found.append(functools.partial(merge, int(name[1])))
                    found.append(flows[name].plan())
            return found

        def go(names):
            for advance in planned(names):
                advance()

        def probs_copy(which, step):
            slot = lax.rem(step, 2)
            return pltpu.make_async_copy(
                halves[which][5].at[lax.rem(step, seqs), pl.ds(lax.div(step, seqs) * PAIR, PAIR)],
                probs_buffer.at[slot],
                probs_sems.at[slot],
            )

        late_copies = [pltpu.make_async_copy(first_ref, in_ref, first_sem.at[2])] + [
            pltpu.make_async_copy(halves[i][4], weights[i], first_sem.at[i]) for i in range(2)
        ]
        probs_copy(0, 0).start()
        for copy in late_copies:
            copy.start()
        small.held[0, :vector_rows] = vector_ref[...]
        small.held[0, vector_rows:] = jnp.zeros((bias_rows, LANES), F32)
        greet(joint)
        go("u0 u1 u2 o0 o1")

        def attend_step(which, step, meet):
            query_ref, key_ref, value_ref, grad_ref, _, _ = halves[which]
            pair, seq = lax.div(step, seqs), lax.rem(step, seqs)
            at = (
                pl.ds(pl.multiple_of(seq * length, length), length),
                pl.ds(pl.multiple_of(pair * LANES, LANES), LANES),
            )
            probs_copy(which, step).wait()

            @pl.when(step + 1 < steps)
            def _():
                probs_copy(which, step + 1).start()

            if which == 0:

                @pl.when(step + 1 == steps)
                def _():
                    probs_copy(1, 0).start()

            query, value, grad = query_ref[at], value_ref[at], grad_ref[at]
            key_t = key_ref[at].T
            grad_key = grad_value = 0.0
            grad_query = []
            slot = lax.rem(step, 2)
            for head in range(PAIR):
                own_query = (head_lanes(query, head) * SCALE).astype(BF16)
                own_value = head_lanes(value, head).astype(BF16)
                own_grad = head_lanes(grad, head).astype(BF16)
                low = probs_buffer[slot, head]
                probs = low.astype(F32)
                grad_probs = dot_nt(own_value, grad)
                weighted = jnp.sum(probs * grad_probs, axis=0, keepdims=True)
                grad_scores = (probs * (grad_probs - weighted)).astype(BF16)
                grad_value += dot_nn(low, own_grad)
                grad_key += dot_nn(grad_scores, own_query)
                head_rows = slice(head * HEAD_DIM, (head + 1) * HEAD_DIM)
                grad_query.append(dot_nn(key_t[head_rows], grad_scores))
                if head == 0:
                    meet()
            query_t = (jnp.concatenate(grad_query, axis=0) * SCALE).astype(BF16)
            own = [query_t.T, grad_key.astype(BF16), grad_value.astype(BF16)]
            for kind in range(3):
                column = pl.multiple_of(kind * half + pair * LANES, LANES)
                grads[which][at[0], pl.ds(column, LANES)] = own[kind]
            stacked = jnp.concatenate([query_t, own[1].T, own[2].T], axis=0)
            part = dot_nn(stacked, rows_ref[at[0], :])
            group = (side if which == 1 else 1 - side) * pairs + pair
            for kind, block in ((0, own[0]), (1, own[2])):
                row = vector_rows + kind * (bias_rows // 2) + group
                total = jnp.sum(block.astype(F32), axis=0, keepdims=True)
                small.held[0, pl.ds(row, 1)] = small.held[0, pl.ds(row, 1)] + total

            @pl.when(seq == 0)
            def _():
                partial[...] = part

            @pl.when(seq > 0)
            def _():
                partial[...] = partial[...] + part

            @pl.when(seq == seqs - 1)
            def _():
                for kind in range(3):
                    for one in range(PAIR):
                        chunk = pair * PAIR + one
                        tile = lax.div(chunk, chunks) * tiles + kind * (local // TILE)
                        tile = tile + lax.rem(chunk, chunks) * chunk_tiles
                        start = kind * LANES + one * HEAD_DIM
                        block = partial[start : start + HEAD_DIM, :]
                        sources[which][pl.ds(tile, chunk_tiles)] = block.reshape(
                            chunk_tiles, TILE, width
                        ).astype(BF16)

        def sweep(which, events):
            events = [(when, planned(names)) for when, names in events]

            def step(index, carry):
                places = iter(range(2))

                def meet():
                    place = next(places)
                    for when, moved in events:
                        if when % 2 == place:

                            @pl.when(index == when // 2)
                            def _():
                                for advance in moved:
                                    advance()

                attend_step(which, index, meet)
                meet()
                return carry

            lax.fori_loop(0, steps, step, 0)

        sweep(0, BACK_EVENTS[0])
        go("f0 f1")
        sweep(1, BACK_EVENTS[1])
        go("w0 w1 m")
        for copy in late_copies:
            copy.wait()

        def input_rows(index, carry):
            at = pl.ds(pl.multiple_of(index * ROW_TILE, ROW_TILE), ROW_TILE)
            in_ref[at, :] = (
                in_ref[at, :]
                + dot_nn(grads[0][at, :], weights[0][...])
                + dot_nn(grads[1][at, :], weights[1][...])
            )
            return carry

        blocks = tokens // ROW_TILE
        parts = len(GRAD_EVENTS)
        for part, names in enumerate(GRAD_EVENTS):
            lax.fori_loop(blocks * part // parts, blocks * (part + 1) // parts, input_rows, 0)
            go(names)
        for names in BACK_TAIL:
            go(names)
        while any(flow.open() for flow in flows.values()):
            go(" ".join(flows))
        for i in range(2):
            for gather, target in ((outs_back[i], out_sum), (sums_back[i], qkv_sum)):

                def spread(index, carry, gather=gather, target=target, lane=lanes[i]):
                    target[index, :, pl.ds(*lane)] = gather.buffer[index].astype(F32)
                    return carry

                lax.fori_loop(0, gather.buffer.shape[0], spread, 0)
        vector_sum[...] = small.held[len(small.order)]
        for t in everything:
            t.drain()

    vmem, anywhere = pl.BlockSpec(memory_space=pltpu.VMEM), pl.BlockSpec(memory_space=pl.ANY)
    half_specs = [vmem] * 4 + [anywhere] * 2
    return pl.pallas_call(
        kernel,
        in_specs=half_specs * 2 + [vmem, anywhere, anywhere] + [vmem] * 2,
        out_specs=[vmem] * 5,
        out_shape=[
            jax.ShapeDtypeStruct((tokens, width), F32),
            jax.ShapeDtypeStruct(up.shape[1:], F32),
            jax.ShapeDtypeStruct(out.shape, F32),
            jax.ShapeDtypeStruct((tiles, TILE, width), F32),
            jax.ShapeDtypeStruct(small.shape, F32),
        ],
        scratch_shapes=[pltpu.VMEM((tokens, 3 * half), BF16)] * 2
        + [pltpu.VMEM(source, BF16)] * 2
        + [pltpu.VMEM((3 * half, width), BF16)] * 2
        + [
            pltpu.VMEM((3 * LANES, width), F32),
            pltpu.VMEM((2, PAIR, length, length), BF16),
            pltpu.SemaphoreType.DMA((2,)),
            pltpu.SemaphoreType.DMA((3,)),
        ]
        + [x for t in everything for x in t.scratch()],
        compiler_params=pltpu.CompilerParams(
            collective_id=1, has_side_effects=True, vmem_limit_bytes=62 * 1024 * 1024
        ),
    )(*far, *own, rows_in, grad_first_in, up, out, vector)


def classify(cls_rows, labels, w_pool, b_pool, w_class, b_class):
    pooled = jnp.tanh(jnp.dot(cls_rows, w_pool, preferred_element_type=F32) + b_pool)
    class_weight = w_class.astype(F32)
    logits = jnp.dot(pooled, class_weight, precision=lax.Precision.HIGHEST) + b_class
    onehot = (labels[:, None] == jnp.arange(logits.shape[1])[None, :]).astype(F32)
    ramp_loss = jax.nn.logsumexp(logits, axis=-1) - jnp.sum(logits * onehot, axis=-1)
    grad_logits = jax.nn.softmax(logits, axis=-1) - onehot
    grad_pool = (
        jnp.dot(grad_logits, class_weight.T, precision=lax.Precision.HIGHEST)
        * (1.0 - pooled * pooled)
    ).astype(BF16)
    return pooled, ramp_loss, grad_logits, grad_pool


def body(
    hidden_in,
    lengths,
    labels,
    query_key_value_weight,
    query_value_bias,
    attention_output_weight,
    attention_output_bias,
    gain_att,
    shift_att,
    up_weight,
    up_bias,
    down_weight,
    down_bias,
    gain_ffn,
    shift_ffn,
    w_pool,
    b_pool,
    w_class,
    b_class,
    cotangent,
):
    seq_here, seq_len, width = hidden_in.shape
    tokens = seq_here * seq_len
    everyone = ("dp", "head")
    head_bits = bits_of(("head",))
    dp_bits = bits_of(("dp",))
    rows_in = hidden_in.reshape(tokens, width)

    half_bits, far_bit = head_bits[1:], head_bits[0]
    own_weight = jnp.transpose(query_key_value_weight, (2, 0, 1))
    own_weight = own_weight.transpose(1, 0, 2)
    far_weight = exchange(own_weight, *far_bit)
    far_bias = exchange(query_value_bias, *far_bit)
    low_order = list(reversed(half_bits))

    def join(blocks, order):
        for axis, bit in order:
            got = exchange(blocks, axis, bit)
            blocks = jnp.where(
                own_bit(axis, bit) == 0,
                jnp.concatenate([blocks, got], axis=1),
                jnp.concatenate([got, blocks], axis=1),
            )
        return blocks

    halves = []
    for weight, bias in ((own_weight, query_value_bias), (far_weight, far_bias)):
        if halves:
            weight, bias, first = lax.optimization_barrier((weight, bias, halves[0][4]))
            halves[0] = halves[0][:4] + (first,) + halves[0][5:]
        weight, bias = join(weight, low_order), join(bias, low_order)
        query = (dot_nt(rows_in, weight[0]) + bias[0]).astype(BF16)
        key = dot_nt(rows_in, weight[1]).astype(BF16)
        value = (dot_nt(rows_in, weight[2]) + bias[1]).astype(BF16)
        context, probs = attend(lengths, query, key, value)
        halves.append((weight, query, key, value, context, probs))
    half_width = halves[0][1].shape[1]
    far_side = own_bit(*far_bit)

    def in_place(own, far, axis):
        return jnp.where(
            far_side == 0,
            jnp.concatenate([own, far], axis=axis),
            jnp.concatenate([far, own], axis=axis),
        )

    combined = in_place(halves[0][4], halves[1][4], 1)
    attended = (
        jnp.dot(combined, attention_output_weight, preferred_element_type=F32)
        + attention_output_bias
    )
    first_in = rows_in.astype(F32) + attended
    normalized_first = normalize(first_in, gain_att, shift_att)
    normed_low = normalized_first.astype(BF16)
    gelu_output, slope, branch = feed_forward(
        normed_low, up_weight, up_bias, down_weight, down_bias
    )
    second_in = normalized_first + branch
    output_rows = normalize(second_in, gain_ffn, shift_ffn)
    hidden_out = output_rows.astype(BF16).reshape(seq_here, seq_len, width)
    cls_rows = hidden_out[:, 0, :]
    pooled, ramp_loss, grad_logits, grad_pool = classify(
        cls_rows, labels, w_pool, b_pool, w_class, b_class
    )
    grad_cls = jnp.dot(grad_pool, w_pool.T, preferred_element_type=F32)
    classes = grad_logits.shape[1]
    cls_pack = jnp.concatenate(
        [
            cls_rows.astype(F32),
            grad_pool.astype(F32),
            pooled,
            jnp.pad(grad_logits, ((0, 0), (0, LANES - classes))),
        ],
        axis=1,
    )
    pack_width = cls_pack.shape[1]
    cls_pack = cls_pack.reshape(-1, LANES)

    first_token = lax.broadcasted_iota(jnp.int32, cotangent.shape, 1) == 0
    grad_output = cotangent.astype(F32) + jnp.where(first_token, grad_cls[:, None, :], 0.0)
    grad_output = grad_output.reshape(tokens, width)
    _, second_back = jax.vjp(normalize, second_in, gain_ffn, shift_ffn)
    grad_second, grad_gain_ffn, grad_shift_ffn = second_back(grad_output)
    grad_branch = grad_second.astype(BF16)
    grad_b_down = jnp.sum(grad_branch, axis=0, dtype=F32)
    part_w_down = jnp.dot(gelu_output.T, grad_branch, preferred_element_type=F32).astype(BF16)
    devices = lax.axis_size("dp") * lax.axis_size("head")
    grad_first, part_w_up, grad_b_up, grad_w_down, cls_all = feed_back(
        head_bits,
        dp_bits,
        grad_branch,
        slope,
        normed_low,
        up_weight,
        down_weight,
        grad_second,
        part_w_down.reshape(devices, -1, width),
        cls_pack,
    )
    grad_b_up = grad_b_up[0]
    _, first_back = jax.vjp(normalize, first_in, gain_att, shift_att)
    grad_first_in, grad_gain_att, grad_shift_att = first_back(grad_first)
    grad_attended = grad_first_in.astype(BF16)
    grad_b_out = jnp.sum(grad_attended, axis=0, dtype=F32)
    part_w_out = jnp.dot(combined.T, grad_attended, preferred_element_type=F32).astype(BF16)
    far_context, own_context = [
        dot_nt(
            grad_attended,
            lax.dynamic_slice_in_dim(attention_output_weight, at * half_width, half_width, 0),
        ).astype(BF16)
        for at in (1 - far_side, far_side)
    ]
    local = query_key_value_weight.shape[2]
    vectors = [
        grad_b_out,
        grad_gain_att,
        grad_shift_att,
        grad_b_up,
        grad_b_down,
        grad_gain_ffn,
        grad_shift_ffn,
    ]
    far, own = [
        (half[1], half[2], half[3], grad_half, half[0].reshape(-1, width), half[5])
        for half, grad_half in ((halves[1], far_context), (halves[0], own_context))
    ]
    grad_in, grad_w_up, grad_w_out, qkv, sums = back_all(
        head_bits,
        dp_bits,
        far,
        own,
        rows_in,
        grad_first_in,
        part_w_up.reshape(devices, -1, width),
        part_w_out.reshape(-1, TILE, width),
        jnp.concatenate(vectors).reshape(-1, LANES),
    )
    grad_w_up = grad_w_up.T
    grad_w_out = grad_w_out.reshape(width, width)
    grad_w_qkv = jnp.transpose(qkv.reshape(3, local, width), (0, 2, 1))
    edges, reached = [], 0
    for vector in vectors:
        reached += vector.shape[0]
        edges.append(reached)
    (
        grad_b_out,
        grad_gain_att,
        grad_shift_att,
        grad_b_up,
        grad_b_down,
        grad_gain_ffn,
        grad_shift_ffn,
        bias_all,
    ) = jnp.split(sums.reshape(-1), edges)
    grad_b_qv = lax.dynamic_slice_in_dim(
        bias_all.reshape(2, width), lax.axis_index("head") * local, local, 1
    )
    cls_all = cls_all.reshape(-1, pack_width)
    all_cls, all_pool, pooled = jnp.split(cls_all[:, : 3 * width], 3, axis=1)
    grad_logits = cls_all[:, 3 * width : 3 * width + classes]
    grad_b_class = jnp.sum(grad_logits, axis=0)
    grad_w_class = jnp.dot(pooled.T, grad_logits, precision=lax.Precision.HIGHEST)
    grad_b_pool = jnp.sum(all_pool, axis=0)
    grad_w_pool = jnp.dot(
        all_cls.T.astype(BF16), all_pool.astype(BF16), preferred_element_type=F32
    )
    return (
        hidden_out,
        ramp_loss,
        grad_in.reshape(seq_here, seq_len, width),
        grad_w_qkv,
        grad_b_qv,
        grad_w_out,
        grad_b_out,
        grad_gain_att,
        grad_shift_att,
        grad_w_up,
        grad_b_up,
        grad_w_down,
        grad_b_down,
        grad_gain_ffn,
        grad_shift_ffn,
        grad_w_pool,
        grad_b_pool,
        grad_w_class,
        grad_b_class,
    )


def solution(mesh):
    rows = P(("dp", "head"))
    placed = (
        (P(("dp", "head"), None, None), rows, rows, P(None, None, "head"), P(None, "head"))
        + (P(),) * 14
        + (P(("dp", "head"), None, None),)
    )
    tokens = P(("dp", "head"), None, None)
    outs = (
        (tokens, rows, tokens, P(None, None, "head"), P(None, "head"))
        + (P(),) * 4
        + (P(None, ("dp", "head")), P(), P(("dp", "head"), None))
        + (P(),) * 7
    )
    return jax.shard_map(body, mesh=mesh, in_specs=placed, out_specs=outs, check_vma=False)
```

```python
import functools

import jax
import jax.numpy as jnp
from jax import lax
from jax.experimental import pallas as pl
from jax.experimental.pallas import tpu as pltpu
from jax.sharding import PartitionSpec as P

HEAD_DIM = 64
EPSILON = 1e-06
MASKED = -1000000000.0
BF16, F32 = jnp.bfloat16, jnp.float32


def bit_count(n):
    assert n & (n - 1) == 0
    return n.bit_length() - 1


def exchange(value, axis, bit):
    size = lax.axis_size(axis)
    step = 1 << bit
    return lax.ppermute(value, axis, [(i, i ^ step) for i in range(size)])


def own_bit(axis, bit):
    return (lax.axis_index(axis) >> bit) & 1


def bits_of(axes):
    found = []
    for axis in axes:
        found += [(axis, b) for b in reversed(range(bit_count(lax.axis_size(axis))))]
    return found


def normalize(row_block, gain_row, shift_row):
    center = jnp.mean(row_block, axis=-1, keepdims=True)
    centered = row_block - center
    spread = jnp.mean(centered * centered, axis=-1, keepdims=True)
    return centered * lax.rsqrt(spread + EPSILON) * gain_row + shift_row


LANES = 128
PAIR = LANES // HEAD_DIM
SCALE = HEAD_DIM ** (-0.5)


def dot_nt(left, right):
    return lax.dot_general(left, right, (((1,), (1,)), ((), ())), preferred_element_type=F32)


def dot_nn(left, right):
    return jnp.dot(left, right, preferred_element_type=F32)


def head_lanes(block, head):
    lane = lax.broadcasted_iota(jnp.int32, block.shape, 1)
    inside = (lane >= head * HEAD_DIM) & (lane < (head + 1) * HEAD_DIM)
    return jnp.where(inside, block.astype(F32), 0.0)


def attend_kernel(length_ref, query_ref, key_ref, value_ref, context_ref, probs_ref):
    length = length_ref[pl.program_id(0)]
    query, key = query_ref[...], key_ref[...]
    value_t = value_ref[...].T
    rows = query.shape[0]
    key_at = lax.broadcasted_iota(jnp.int32, (rows, rows), 0)
    contexts = []
    for head in range(PAIR):
        own_query = (head_lanes(query, head) * SCALE).astype(BF16)
        scores = jnp.where(key_at < length, dot_nt(key, own_query), MASKED)
        shifted = jnp.exp(scores - jnp.max(scores, axis=0, keepdims=True))
        inverse = 1.0 / jnp.sum(shifted, axis=0, keepdims=True)
        probs = (shifted * inverse).astype(BF16)
        probs_ref[0, head] = probs
        contexts.append(dot_nn(value_t[head * HEAD_DIM : (head + 1) * HEAD_DIM], probs))
    context_ref[...] = jnp.concatenate(contexts, axis=0).T.astype(BF16)


def attend(lengths, query, key, value):
    seqs = lengths.shape[0]
    tokens, width = query.shape
    rows, pairs = tokens // seqs, width // LANES
    block = pl.BlockSpec((rows, LANES), lambda s, p: (s, p))
    return pl.pallas_call(
        attend_kernel,
        grid=(seqs, pairs),
        in_specs=[pl.BlockSpec(memory_space=pltpu.SMEM), block, block, block],
        out_specs=[block, pl.BlockSpec((1, PAIR, rows, rows), lambda s, p: (s, p, 0, 0))],
        out_shape=[
            jax.ShapeDtypeStruct((tokens, width), BF16),
            jax.ShapeDtypeStruct((seqs, pairs * PAIR, rows, rows), BF16),
        ],
        cost_estimate=pl.CostEstimate(
            flops=seqs * pairs * 12 * rows * rows * LANES,
            bytes_accessed=8 * tokens * width + 4 * tokens * rows * pairs,
            transcendentals=0,
        ),
    )(lengths, query, key, value)


def gelu_parts(values):
    bell = jnp.exp(-0.5 * values * values)
    inner = 1.0 / (1.0 + (0.3275911 * 0.5**0.5) * jnp.abs(values))
    series = 0.5 * 1.061405429
    for term in (-1.453152027, 1.421413741, -0.284496736, 0.254829592):
        series = series * inner + 0.5 * term
    tail = series * inner * bell
    below = jnp.where(values < 0.0, tail, 1.0 - tail)
    return values * below, below + values * bell * 0.3989422804014327


FF_TILE = 512
ROW_TILE = 256


def feed_kernel(rows_ref, up_ref, up_bias_ref, down_ref, down_bias_ref, act_ref, slope_ref, out_ref):
    first = pl.program_id(0) == 0

    @pl.when(first)
    def _():
        out_ref[...] = jnp.broadcast_to(down_bias_ref[...], out_ref.shape)

    for start in range(0, rows_ref.shape[0], ROW_TILE):
        here = pl.ds(start, ROW_TILE)
        before = dot_nn(rows_ref[here, :], up_ref[...]) + up_bias_ref[...]
        active, slope = gelu_parts(before)
        active = active.astype(BF16)
        act_ref[here, :] = active
        slope_ref[here, :] = slope.astype(BF16)
        out_ref[here, :] += dot_nn(active, down_ref[...])


def feed_forward(rows, up_weight, up_bias, down_weight, down_bias):
    tokens, width = rows.shape
    units = up_weight.shape[1]
    whole = lambda shape: pl.BlockSpec(shape, lambda i: (0, 0))
    columns = lambda height: pl.BlockSpec((height, FF_TILE), lambda i: (0, i))
    return pl.pallas_call(
        feed_kernel,
        grid=(units // FF_TILE,),
        in_specs=[
            whole((tokens, width)),
            columns(width),
            columns(1),
            pl.BlockSpec((FF_TILE, width), lambda i: (i, 0)),
            whole((1, width)),
        ],
        out_specs=[columns(tokens), columns(tokens), whole((tokens, width))],
        out_shape=[
            jax.ShapeDtypeStruct((tokens, units), BF16),
            jax.ShapeDtypeStruct((tokens, units), BF16),
            jax.ShapeDtypeStruct((tokens, width), F32),
        ],
        cost_estimate=pl.CostEstimate(
            flops=8 * tokens * width * units,
            bytes_accessed=4 * tokens * units + 4 * width * units,
            transcendentals=0,
        ),
    )(rows, up_weight, up_bias[None], down_weight, down_bias[None])


MESH = pl.DeviceIdType.MESH


def mine_of(axis, bit):
    return lax.rem(lax.div(lax.axis_index(axis), 1 << bit), 2)


def partner_of(axis, bit):
    return {axis: lax.axis_index(axis) + (1 << bit) * (1 - 2 * mine_of(axis, bit))}


def place_of(bits):
    place = 0
    for axis, bit in bits:
        place = 2 * place + mine_of(axis, bit)
    return place


def greet(bits):
    barrier = pltpu.get_barrier_semaphore()
    for axis, bit in bits:
        pl.semaphore_signal(
            barrier, inc=1, device_id=partner_of(axis, bit), device_id_type=MESH
        )
    pl.semaphore_wait(barrier, len(bits))


def copy_to(source, target, sems, bit):
    return pltpu.make_async_remote_copy(
        src_ref=source,
        dst_ref=target,
        send_sem=sems.at[0],
        recv_sem=sems.at[1],
        device_id=partner_of(*bit),
        device_id_type=MESH,
    )


class Scatter:
    def __init__(self, shape, lanes, joint, order, far=False):
        self.shape, self.lanes, self.joint, self.order = shape, lanes, joint, order
        self.far = far

    def blocks(self, stage):
        halved = len([bit for bit in self.order[:stage] if bit in self.joint])
        return self.shape[0] >> halved

    def scratch(self):
        rows, width = self.shape[1], self.lanes[1]
        return [
            pltpu.VMEM((self.blocks(stage + 1), rows, width), BF16)
            for stage in range(len(self.order))
        ] + (
            [
                pltpu.VMEM((self.blocks(1), rows, width), BF16),
                pltpu.SemaphoreType.DMA(()),
            ]
            if self.far
            else []
        ) + [pltpu.SemaphoreType.DMA((len(self.order), 2))]

    def bind(self, source, scratch, last=None):
        self.source, self.sems, self.last = source, scratch[-1], last
        self.slots = scratch[: len(self.order)]
        if self.far:
            self.kept, self.kept_sem = scratch[len(self.order) : -1]
        return self

    def split(self, stage):
        bit = self.order[stage]
        if bit not in self.joint:
            return 1, self.blocks(stage), None
        left = [b for b in self.joint if b not in self.order[:stage]]
        high = 1 << left.index(bit)
        return high, self.blocks(stage) // (2 * high), mine_of(*bit)

    def view(self, stage, at):
        if stage == 0:
            return self.source.at[at, :, pl.ds(*self.lanes)]
        return self.slots[stage - 1].at[at]

    def steps(self):
        return len(self.order)

    def start(self, stage):
        high, low, side = self.split(stage)

        def send(run, carry):
            at = 0 if side is None else (2 * run + 1 - side) * low
            copy_to(
                self.view(stage, pl.ds(at, low)),
                self.slots[stage].at[pl.ds(run * low, low)],
                self.sems.at[stage],
                self.order[stage],
            ).start()
            if self.far and stage == 0:
                pltpu.make_async_copy(
                    self.view(0, pl.ds((2 * run + side) * low, low)),
                    self.kept.at[pl.ds(run * low, low)],
                    self.kept_sem,
                ).start()
            return carry

        lax.fori_loop(0, high, send, 0)

    def whole(self, stage):
        slot = self.slots[stage]
        return copy_to(slot, slot, self.sems.at[stage], self.order[stage])

    def finish(self, stage):
        high, low, side = self.split(stage)
        slot = self.slots[stage]
        self.whole(stage).wait_recv()
        from_kept = self.far and stage == 0
        if from_kept:
            pltpu.make_async_copy(self.kept, self.kept, self.kept_sem).wait()
        final = stage + 1 == len(self.order) and self.last is not None

        def add(index, carry):
            kept = index
            if side is not None:
                kept = (2 * lax.div(index, low) + side) * low + lax.rem(index, low)
            mine = self.kept[index] if from_kept else self.view(stage, kept)[...]
            theirs = slot[index]
            if final:
                self.last(index, mine.astype(F32) + theirs.astype(F32))
            else:
                slot[index] = mine + theirs
            return carry

        lax.fori_loop(0, high * low, add, 0)

    def drain(self):
        for stage in range(len(self.order)):
            self.whole(stage).wait_send()


class Gather:
    def __init__(self, shape, dtype, order):
        self.shape, self.dtype, self.order = shape, dtype, order

    def scratch(self):
        count = self.shape[0] << len(self.order)
        return [
            pltpu.VMEM((count,) + self.shape[1:], self.dtype),
            pltpu.SemaphoreType.DMA((len(self.order), 2)),
        ]

    def bind(self, scratch):
        self.buffer, self.sems = scratch
        self.place = place_of(list(reversed(self.order)))
        return self

    def own(self, index):
        return self.place * self.shape[0] + index

    def steps(self):
        return len(self.order)

    def copy(self, stage, theirs):
        run = 1 << stage
        base = lax.div(self.place, run) * run
        if theirs:
            base = base + run * (1 - 2 * mine_of(*self.order[stage]))
        here = self.buffer.at[pl.ds(base * self.shape[0], run * self.shape[0])]
        return copy_to(here, here, self.sems.at[stage], self.order[stage])

    def start(self, stage):
        self.copy(stage, False).start()

    def finish(self, stage):
        self.copy(stage, True).wait_recv()

    def drain(self):
        for stage in range(len(self.order)):
            self.copy(stage, False).wait_send()

    def natural(self, position, bits):
        index = 0
        for bit in bits:
            index = 2 * index + lax.rem(lax.div(position, 1 << self.order.index(bit)), 2)
        return index


class Swap:
    def __init__(self, shape, bit):
        self.shape, self.bit = shape, bit

    def scratch(self):
        return [pltpu.VMEM(self.shape, BF16), pltpu.SemaphoreType.DMA((2,))]

    def bind(self, source, scratch):
        self.source, (self.slot, self.sems) = source, scratch
        return self

    def steps(self):
        return 1

    def copy(self):
        return copy_to(self.source, self.slot, self.sems, self.bit)

    def start(self, stage):
        self.copy().start()

    def finish(self, stage):
        self.copy().wait_recv()

    def drain(self):
        self.copy().wait_send()


class Total:
    def __init__(self, shape, order):
        self.shape, self.order = shape, order

    def scratch(self):
        return [
            pltpu.VMEM((len(self.order) + 1,) + self.shape, F32),
            pltpu.VMEM((len(self.order),) + self.shape, F32),
            pltpu.SemaphoreType.DMA((len(self.order), 2)),
        ]

    def bind(self, scratch):
        self.held, self.slots, self.sems = scratch
        return self

    def steps(self):
        return len(self.order)

    def copy(self, stage):
        return copy_to(
            self.held.at[stage], self.slots.at[stage], self.sems.at[stage], self.order[stage]
        )

    def start(self, stage):
        self.copy(stage).start()

    def finish(self, stage):
        self.copy(stage).wait_recv()
        self.held[stage + 1] = self.held[stage] + self.slots[stage]

    def drain(self):
        for stage in range(len(self.order)):
            self.copy(stage).wait_send()


def take(scratch, chain):
    count = len(chain.scratch())
    return [scratch.pop(0) for _ in range(count)]


class Flow:
    def __init__(self, *transfers):
        self.todo = [(t, stage) for t in transfers for stage in range(t.steps())]
        self.at = -1

    def plan(self):
        at = self.at
        self.at += 1

        def advance():
            if at >= 0:
                transfer, stage = self.todo[at]
                transfer.finish(stage)
            if at + 1 < len(self.todo):
                transfer, stage = self.todo[at + 1]
                transfer.start(stage)

        return advance

    def open(self):
        return self.at < len(self.todo)


TILE = 8


def halvings(blocks, bits):
    count = 0
    while count < len(bits) and blocks % 2 == 0:
        blocks //= 2
        count += 1
    return bits[:count]


def orders(head_bits, dp_bits):
    low_head, low_dp = list(reversed(head_bits)), list(reversed(dp_bits))
    axes = low_head[-1:] + low_dp[:2]
    return [low_head[:-1] + axes[i:] + axes[:i] + low_dp[2:] for i in range(3)]


def plan(*flows):
    listed = [one for flow in flows for one in (flow if isinstance(flow, list) else [flow])]
    return [one.plan() for one in listed if one.open()]


def move(*flows):
    for advance in plan(*flows):
        advance()


def keep(target, lane):
    def store(index, total):
        target[:, pl.ds(*lane)] = total

    return store


BACK_TILE = 768
AHEAD = 1
FEED_EVENTS = (
    (0, 5, (3,)),
    (0, 7, (0, 1, 2,)),
    (1, 1, (3,)),
    (2, 2, (3,)),
    (3, 0, (0, 2,)),
    (3, 1, (1,)),
    (3, 3, (3,)),
    (3, 7, (3,)),
)
FEED_TAIL = (0, 2, 1, 4, 5, 6, 0, 2, 1, 0, 2, 1)


def feed_back(head_bits, dp_bits, grad_branch, slope, normed_low, up_weight, down_weight, grad_second, down, cls):
    joint = dp_bits + head_bits
    order = orders(head_bits, dp_bits)
    tokens, width = grad_branch.shape
    units = up_weight.shape[1]
    third = width // 3
    lanes = [(i * third, third) for i in range(3)]
    large = [Scatter(down.shape, lanes[i], joint, order[i], far=True) for i in range(3)]
    rows = Gather((1,) + cls.shape, F32, order[0][::-1])
    blocks, depth, _ = down.shape
    ahead = depth % 16 == 0 and BACK_TILE % (2 * depth) == 0
    early = [Scatter(down.shape, lanes[i], joint, order[i][:AHEAD]) for i in range(3)]
    early = early if ahead else []
    everything = large + [rows] + early

    def kernel(
        branch_ref, slope_ref, normed_ref, up_ref, weight_ref, second_ref, down_ref, cls_ref,
        first_ref, bias_ref, sum_ref, all_ref, *rest
    ):
        part_refs, rest = rest[:part_count], rest[part_count:]
        pre_t, slopes, ups, weights, parts, copy_sems, in_sems, out_sems, *scratch = rest
        held = [take(scratch, t) for t in everything]
        for i, t in enumerate(early):

            def passed(index, total, i=i):
                part_refs[i][index] = total.astype(BF16)

            t.bind(parts, held[4 + i], passed)
        for i in range(3):
            large[i].bind(down_ref, held[i], keep(sum_ref, lanes[i]))
        rows.bind(held[3])
        flows, flow_rows = [Flow(t) for t in large], Flow(rows)
        flows_early = [Flow(t) for t in early]
        second_copy = pltpu.make_async_copy(second_ref, first_ref, copy_sems.at[0])
        second_copy.start()
        tiles = units // BACK_TILE

        def columns_of(index):
            return pl.ds(pl.multiple_of(index * BACK_TILE, BACK_TILE), BACK_TILE)

        def loads(index):
            slot, column = lax.rem(index, 2), columns_of(index)
            pairs = (
                (slope_ref.at[:, column], slopes.at[slot]),
                (up_ref.at[:, column], ups.at[slot]),
                (weight_ref.at[column, :], weights.at[slot]),
            )
            return [
                pltpu.make_async_copy(source, target, in_sems.at[slot, which])
                for which, (source, target) in enumerate(pairs)
            ]

        def store(index):
            slot = lax.rem(index, 2)
            return pltpu.make_async_copy(
                parts.at[slot], part_refs[0].at[columns_of(index), :], out_sems.at[slot]
            )

        for copy in loads(0):
            copy.start()
        rows.buffer[rows.place] = cls_ref[...]
        greet(joint)
        move(flows, flow_rows)

        events = [
            (when, at, plan(*[flow_rows if which == 3 else flows[which] for which in moved]))
            for when, at, moved in FEED_EVENTS
        ]

        def unit_tile(index, carry):
            column, slot = columns_of(index), lax.rem(index, 2)
            for copy in loads(index):
                copy.wait()

            @pl.when(index + 1 < tiles)
            def _():
                for copy in loads(index + 1):
                    copy.start()

            @pl.when(index == 0)
            def _():
                second_copy.wait()

            if not ahead:

                @pl.when(index >= 2)
                def _():
                    store(index - 2).wait()

            places = iter(range(tokens))

            def meet():
                place = next(places)
                for when, at, moved in events:
                    if at == place:

                        @pl.when(index == when)
                        def _():
                            for advance in moved:
                                advance()

            bias = 0.0
            for start in range(0, tokens, ROW_TILE):
                here = pl.ds(start, ROW_TILE)
                grad = dot_nt(branch_ref[here, :], weights[slot])
                pre = (grad * slopes[slot, here, :].astype(F32)).astype(BF16)
                bias = bias + jnp.sum(pre.astype(F32), axis=0, keepdims=True)
                pre_t[:, here] = pre.T
                first_ref[here, :] = first_ref[here, :] + dot_nt(pre, ups[slot])
                meet()
            bias_ref[:, column] = bias
            step = 2 * depth if ahead else ROW_TILE
            for start in range(0, BACK_TILE, step):
                part = dot_nn(pre_t[start : start + step, :], normed_ref[...])
                if ahead:
                    at = (index * BACK_TILE + start) // depth
                    parts[pl.ds(at, 2)] = part.reshape(2, depth, width).astype(BF16)
                else:
                    parts[slot, pl.ds(start, step), :] = part.astype(BF16)
                meet()
            if not ahead:
                store(index).start()
            return carry

        lax.fori_loop(0, tiles, unit_tile, 0)
        if not ahead:
            for index in range(max(tiles - 2, 0), tiles):
                store(index).wait()
        move(flows_early)
        every_flow = flows + [flow_rows] + flows_early
        for which in FEED_TAIL:
            move(*every_flow[which : which + 1])
        while any(flow.open() for flow in every_flow):
            move(every_flow)
        out_copy = pltpu.make_async_copy(rows.buffer, all_ref, copy_sems.at[1])
        out_copy.start()
        out_copy.wait()
        for t in everything:
            t.drain()

    part_count = 3 if ahead else 1
    if ahead:
        part_shapes = [
            jax.ShapeDtypeStruct((t.blocks(AHEAD), depth, third), BF16) for t in early
        ]
        parts_shape = (blocks, depth, width)
    else:
        part_shapes = [jax.ShapeDtypeStruct((units, width), BF16)]
        parts_shape = (2, BACK_TILE, width)
    vmem, anywhere = pl.BlockSpec(memory_space=pltpu.VMEM), pl.BlockSpec(memory_space=pl.ANY)
    return pl.pallas_call(
        kernel,
        in_specs=[vmem, anywhere, vmem] + [anywhere] * 4 + [vmem],
        out_specs=[vmem, vmem, vmem, anywhere] + [vmem if ahead else anywhere] * part_count,
        out_shape=[
            jax.ShapeDtypeStruct((tokens, width), F32),
            jax.ShapeDtypeStruct((1, units), F32),
            jax.ShapeDtypeStruct(down.shape[1:], F32),
            jax.ShapeDtypeStruct((1 << len(joint),) + cls.shape, F32),
        ]
        + part_shapes,
        scratch_shapes=[
            pltpu.VMEM((BACK_TILE, tokens), BF16),
            pltpu.VMEM((2, tokens, BACK_TILE), BF16),
            pltpu.VMEM((2, width, BACK_TILE), BF16),
            pltpu.VMEM((2, BACK_TILE, width), BF16),
            pltpu.VMEM(parts_shape, BF16),
            pltpu.SemaphoreType.DMA((2,)),
            pltpu.SemaphoreType.DMA((2, 3)),
            pltpu.SemaphoreType.DMA((2,)),
        ]
        + [x for t in everything for x in t.scratch()],
        compiler_params=pltpu.CompilerParams(
            collective_id=0, has_side_effects=True, vmem_limit_bytes=62 * 1024 * 1024
        ),
    )(grad_branch, slope, normed_low, up_weight, down_weight, grad_second, down, cls)


BACK_EVENTS = (
    (
        (2, "o0 o1"),
        (8, "u2"),
        (9, "o0"),
        (10, "u0 u1 o1"),
    ),
    (
        (1, "o0"),
        (2, "f0 f1 u2"),
        (3, "u0 o1"),
        (4, "o0"),
        (6, "u1 o1"),
        (8, "u2 o0"),
        (9, "f0 u0"),
        (10, "f1 u1 o1"),
    ),
)
GRAD_EVENTS = ("o0", "f0 m", "w0 w1 f1 u2", "o0 o1")
BACK_TAIL = (
    "u0 m u1 o1",
    "f0 m f1 w1",
    "o0 f0 o1 w0",
    "f1 m o0 w1",
    "m w0 o0 o1",
    "o1 w1 s1 w0",
    "s0 s1 s0 s1",
    "s0 s1 s0",
)


def back_all(head_bits, dp_bits, far, own, rows_in, grad_first_in, up, out, vector):
    joint = dp_bits + head_bits
    order = orders(head_bits, dp_bits)
    low_head, low_dp = list(reversed(head_bits)), list(reversed(dp_bits))
    dp_order = (low_dp, low_dp[1:2] + low_dp[:1] + low_dp[2:])
    far_bit, join_bits = head_bits[0], low_head[:-1]
    tokens, width = rows_in.shape
    seqs, _, length, _ = far[5].shape
    half = far[0].shape[1]
    pairs = half // LANES
    steps = pairs * seqs
    local = half >> len(join_bits)
    chunks = local // HEAD_DIM
    tiles = 3 * local // TILE
    chunk_tiles = HEAD_DIM // TILE
    middle = width // 2
    lanes = ((0, middle), (middle, middle))
    third = width // 3
    thirds = [(i * third, third) for i in range(3)]
    if len(up) == 1:
        large = [Scatter(up[0].shape, thirds[i], joint, order[i], far=True) for i in range(3)]
        up_block = up[0].shape[1:]
    else:
        large = [
            Scatter(
                up[i].shape,
                (0, third),
                [bit for bit in joint if bit not in order[i][:AHEAD]],
                order[i][AHEAD:],
            )
            for i in range(3)
        ]
        up_block = (up[0].shape[1], width)
    out_bits = [halvings(out.shape[0], order[i][:5]) for i in range(2)]
    outs = [Scatter(out.shape, lanes[i], out_bits[i], order[i]) for i in range(2)]
    outs_back = [
        Gather((out.shape[0] >> len(out_bits[i]), TILE, middle), BF16, out_bits[i][::-1])
        for i in range(2)
    ]
    source = (tiles << len(join_bits), TILE, width)
    qkv_bits = [halvings(tiles, dp_order[i][:3]) for i in range(2)]
    far_sums, own_sums = [
        [
            Scatter(source, lanes[i], join_bits + qkv_bits[i], join_bits + dp_order[i])
            for i in range(2)
        ]
        for _ in range(2)
    ]
    last = (tiles >> len(qkv_bits[0]), TILE, middle)
    swaps = [Swap(last, far_bit) for i in range(2)]
    sums_back = [Gather(last, BF16, qkv_bits[i][::-1]) for i in range(2)]
    vector_rows = vector.shape[0]
    bias_rows = 2 * width // LANES
    small = Total((vector_rows + bias_rows, LANES), order[0])
    groups = [large, outs, outs_back, far_sums, own_sums, swaps, sums_back, [small]]
    everything = [t for group in groups for t in group]

    def kernel(*refs):
        refs = list(refs)
        halves = [[refs.pop(0) for _ in range(6)] for _ in range(2)]
        rows_ref, first_ref, out_ref, vector_ref = [refs.pop(0) for _ in range(4)]
        up_refs = [refs.pop(0) for _ in up]
        in_ref, up_sum, out_sum, qkv_sum, vector_sum = [refs.pop(0) for _ in range(5)]
        grads, sources = [refs.pop(0) for _ in range(2)], [refs.pop(0) for _ in range(2)]
        weights = [refs.pop(0) for _ in range(2)]
        partial, probs_buffer, probs_sems, first_sem = [refs.pop(0) for _ in range(4)]
        held = {id(t): take(refs, t) for t in everything}
        side = mine_of(*far_bit)

        def hand_on(gather):
            def store(index, total):
                gather.buffer[gather.own(index)] = total.astype(BF16)

            return store

        for t in outs_back + sums_back + [small]:
            t.bind(held[id(t)])
        for i, t in enumerate(large):
            t.bind(up_refs[i % len(up)], held[id(t)], keep(up_sum, thirds[i]))
        for i in range(2):
            outs[i].bind(out_ref, held[id(outs[i])], hand_on(outs_back[i]))
            far_sums[i].bind(sources[0], held[id(far_sums[i])])
            own_sums[i].bind(sources[1], held[id(own_sums[i])])
            swaps[i].bind(far_sums[i].slots[-1], held[id(swaps[i])])
        flows = {f"u{i}": Flow(t) for i, t in enumerate(large)}
        for i in range(2):
            flows[f"o{i}"] = Flow(outs[i], outs_back[i])
            flows[f"f{i}"] = Flow(far_sums[i], swaps[i])
            flows[f"w{i}"] = Flow(own_sums[i])
            flows[f"s{i}"] = Flow(sums_back[i])
        flows["m"] = Flow(small)

        def merge(i):
            def add(index, carry):
                sums_back[i].buffer[sums_back[i].own(index)] = (
                    own_sums[i].slots[-1][index] + swaps[i].slot[index]
                )
                return carry

            lax.fori_loop(0, last[0], add, 0)

        def ready(name):
            return not (name[0] == "s" and flows[name].at < 0) or not (
                flows["w" + name[1]].open() or flows["f" + name[1]].open()
            )

        def planned(names):
            found = []
            for name in names.split():
                if flows[name].open() and ready(name):
                    if name[0] == "s" and flows[name].at < 0:
                        found.append(functools.partial(merge, int(name[1])))
                    found.append(flows[name].plan())
            return found

        def go(names):
            for advance in planned(names):
                advance()

        def probs_copy(which, step):
            slot = lax.rem(step, 2)
            return pltpu.make_async_copy(
                halves[which][5].at[lax.rem(step, seqs), pl.ds(lax.div(step, seqs) * PAIR, PAIR)],
                probs_buffer.at[slot],
                probs_sems.at[slot],
            )

        late_copies = [pltpu.make_async_copy(first_ref, in_ref, first_sem.at[2])] + [
            pltpu.make_async_copy(halves[i][4], weights[i], first_sem.at[i]) for i in range(2)
        ]
        probs_copy(0, 0).start()
        for copy in late_copies:
            copy.start()
        small.held[0, :vector_rows] = vector_ref[...]
        small.held[0, vector_rows:] = jnp.zeros((bias_rows, LANES), F32)
        greet(joint)
        go("u0 u1 u2 o0 o1")

        def attend_step(which, step, meet):
            query_ref, key_ref, value_ref, grad_ref, _, _ = halves[which]
            pair, seq = lax.div(step, seqs), lax.rem(step, seqs)
            at = (
                pl.ds(pl.multiple_of(seq * length, length), length),
                pl.ds(pl.multiple_of(pair * LANES, LANES), LANES),
            )
            probs_copy(which, step).wait()

            @pl.when(step + 1 < steps)
            def _():
                probs_copy(which, step + 1).start()

            if which == 0:

                @pl.when(step + 1 == steps)
                def _():
                    probs_copy(1, 0).start()

            query, value, grad = query_ref[at], value_ref[at], grad_ref[at]
            key_t = key_ref[at].T
            grad_key = grad_value = 0.0
            grad_query = []
            slot = lax.rem(step, 2)
            for head in range(PAIR):
                own_query = (head_lanes(query, head) * SCALE).astype(BF16)
                own_value = head_lanes(value, head).astype(BF16)
                own_grad = head_lanes(grad, head).astype(BF16)
                low = probs_buffer[slot, head]
                probs = low.astype(F32)
                grad_probs = dot_nt(own_value, grad)
                weighted = jnp.sum(probs * grad_probs, axis=0, keepdims=True)
                grad_scores = (probs * (grad_probs - weighted)).astype(BF16)
                grad_value += dot_nn(low, own_grad)
                grad_key += dot_nn(grad_scores, own_query)
                head_rows = slice(head * HEAD_DIM, (head + 1) * HEAD_DIM)
                grad_query.append(dot_nn(key_t[head_rows], grad_scores))
                if head == 0:
                    meet()
            query_t = (jnp.concatenate(grad_query, axis=0) * SCALE).astype(BF16)
            own = [query_t.T, grad_key.astype(BF16), grad_value.astype(BF16)]
            for kind in range(3):
                column = pl.multiple_of(kind * half + pair * LANES, LANES)
                grads[which][at[0], pl.ds(column, LANES)] = own[kind]
            stacked = jnp.concatenate([query_t, own[1].T, own[2].T], axis=0)
            part = dot_nn(stacked, rows_ref[at[0], :])
            group = (side if which == 1 else 1 - side) * pairs + pair
            for kind, block in ((0, own[0]), (1, own[2])):
                row = vector_rows + kind * (bias_rows // 2) + group
                total = jnp.sum(block.astype(F32), axis=0, keepdims=True)
                small.held[0, pl.ds(row, 1)] = small.held[0, pl.ds(row, 1)] + total

            @pl.when(seq == 0)
            def _():
                partial[...] = part

            @pl.when(seq > 0)
            def _():
                partial[...] = partial[...] + part

            @pl.when(seq == seqs - 1)
            def _():
                for kind in range(3):
                    for one in range(PAIR):
                        chunk = pair * PAIR + one
                        tile = lax.div(chunk, chunks) * tiles + kind * (local // TILE)
                        tile = tile + lax.rem(chunk, chunks) * chunk_tiles
                        start = kind * LANES + one * HEAD_DIM
                        block = partial[start : start + HEAD_DIM, :]
                        sources[which][pl.ds(tile, chunk_tiles)] = block.reshape(
                            chunk_tiles, TILE, width
                        ).astype(BF16)

        def sweep(which, events):
            events = [(when, planned(names)) for when, names in events]

            def step(index, carry):
                places = iter(range(2))

                def meet():
                    place = next(places)
                    for when, moved in events:
                        if when % 2 == place:

                            @pl.when(index == when // 2)
                            def _():
                                for advance in moved:
                                    advance()

                attend_step(which, index, meet)
                meet()
                return carry

            lax.fori_loop(0, steps, step, 0)

        sweep(0, BACK_EVENTS[0])
        go("f0 f1")
        sweep(1, BACK_EVENTS[1])
        go("w0 w1 m")
        for copy in late_copies:
            copy.wait()

        def input_rows(index, carry):
            at = pl.ds(pl.multiple_of(index * ROW_TILE, ROW_TILE), ROW_TILE)
            in_ref[at, :] = (
                in_ref[at, :]
                + dot_nn(grads[0][at, :], weights[0][...])
                + dot_nn(grads[1][at, :], weights[1][...])
            )
            return carry

        blocks = tokens // ROW_TILE
        parts = len(GRAD_EVENTS)
        for part, names in enumerate(GRAD_EVENTS):
            lax.fori_loop(blocks * part // parts, blocks * (part + 1) // parts, input_rows, 0)
            go(names)
        for names in BACK_TAIL:
            go(names)
        while any(flow.open() for flow in flows.values()):
            go(" ".join(flows))
        for i in range(2):
            for gather, target in ((outs_back[i], out_sum), (sums_back[i], qkv_sum)):

                def spread(index, carry, gather=gather, target=target, lane=lanes[i]):
                    target[index, :, pl.ds(*lane)] = gather.buffer[index].astype(F32)
                    return carry

                lax.fori_loop(0, gather.buffer.shape[0], spread, 0)
        vector_sum[...] = small.held[len(small.order)]
        for t in everything:
            t.drain()

    vmem, anywhere = pl.BlockSpec(memory_space=pltpu.VMEM), pl.BlockSpec(memory_space=pl.ANY)
    half_specs = [vmem] * 4 + [anywhere] * 2
    return pl.pallas_call(
        kernel,
        in_specs=half_specs * 2
        + [vmem, anywhere, vmem, vmem]
        + [anywhere if len(up) == 1 else vmem] * len(up),
        out_specs=[vmem] * 5,
        out_shape=[
            jax.ShapeDtypeStruct((tokens, width), F32),
            jax.ShapeDtypeStruct(up_block, F32),
            jax.ShapeDtypeStruct(out.shape, F32),
            jax.ShapeDtypeStruct((tiles, TILE, width), F32),
            jax.ShapeDtypeStruct(small.shape, F32),
        ],
        scratch_shapes=[pltpu.VMEM((tokens, 3 * half), BF16)] * 2
        + [pltpu.VMEM(source, BF16)] * 2
        + [pltpu.VMEM((3 * half, width), BF16)] * 2
        + [
            pltpu.VMEM((3 * LANES, width), F32),
            pltpu.VMEM((2, PAIR, length, length), BF16),
            pltpu.SemaphoreType.DMA((2,)),
            pltpu.SemaphoreType.DMA((3,)),
        ]
        + [x for t in everything for x in t.scratch()],
        compiler_params=pltpu.CompilerParams(
            collective_id=1, has_side_effects=True, vmem_limit_bytes=62 * 1024 * 1024
        ),
    )(*far, *own, rows_in, grad_first_in, out, vector, *up)


def classify(cls_rows, labels, w_pool, b_pool, w_class, b_class):
    pooled = jnp.tanh(jnp.dot(cls_rows, w_pool, preferred_element_type=F32) + b_pool)
    class_weight = w_class.astype(F32)
    logits = jnp.dot(pooled, class_weight, precision=lax.Precision.HIGHEST) + b_class
    onehot = (labels[:, None] == jnp.arange(logits.shape[1])[None, :]).astype(F32)
    ramp_loss = jax.nn.logsumexp(logits, axis=-1) - jnp.sum(logits * onehot, axis=-1)
    grad_logits = jax.nn.softmax(logits, axis=-1) - onehot
    grad_pool = (
        jnp.dot(grad_logits, class_weight.T, precision=lax.Precision.HIGHEST)
        * (1.0 - pooled * pooled)
    ).astype(BF16)
    return pooled, ramp_loss, grad_logits, grad_pool


def body(
    hidden_in,
    lengths,
    labels,
    query_key_value_weight,
    query_value_bias,
    attention_output_weight,
    attention_output_bias,
    gain_att,
    shift_att,
    up_weight,
    up_bias,
    down_weight,
    down_bias,
    gain_ffn,
    shift_ffn,
    w_pool,
    b_pool,
    w_class,
    b_class,
    cotangent,
):
    seq_here, seq_len, width = hidden_in.shape
    tokens = seq_here * seq_len
    everyone = ("dp", "head")
    head_bits = bits_of(("head",))
    dp_bits = bits_of(("dp",))
    rows_in = hidden_in.reshape(tokens, width)

    half_bits, far_bit = head_bits[1:], head_bits[0]
    own_weight = jnp.transpose(query_key_value_weight, (2, 0, 1))
    own_weight = own_weight.transpose(1, 0, 2)
    far_weight = exchange(own_weight, *far_bit)
    far_bias = exchange(query_value_bias, *far_bit)
    low_order = list(reversed(half_bits))

    def join(blocks, order):
        for axis, bit in order:
            got = exchange(blocks, axis, bit)
            blocks = jnp.where(
                own_bit(axis, bit) == 0,
                jnp.concatenate([blocks, got], axis=1),
                jnp.concatenate([got, blocks], axis=1),
            )
        return blocks

    halves = []
    for weight, bias in ((own_weight, query_value_bias), (far_weight, far_bias)):
        if halves:
            weight, bias, first = lax.optimization_barrier((weight, bias, halves[0][4]))
            halves[0] = halves[0][:4] + (first,) + halves[0][5:]
        weight, bias = join(weight, low_order), join(bias, low_order)
        query = (dot_nt(rows_in, weight[0]) + bias[0]).astype(BF16)
        key = dot_nt(rows_in, weight[1]).astype(BF16)
        value = (dot_nt(rows_in, weight[2]) + bias[1]).astype(BF16)
        context, probs = attend(lengths, query, key, value)
        halves.append((weight, query, key, value, context, probs))
    half_width = halves[0][1].shape[1]
    far_side = own_bit(*far_bit)

    def in_place(own, far, axis):
        return jnp.where(
            far_side == 0,
            jnp.concatenate([own, far], axis=axis),
            jnp.concatenate([far, own], axis=axis),
        )

    combined = in_place(halves[0][4], halves[1][4], 1)
    attended = (
        jnp.dot(combined, attention_output_weight, preferred_element_type=F32)
        + attention_output_bias
    )
    first_in = rows_in.astype(F32) + attended
    normalized_first = normalize(first_in, gain_att, shift_att)
    normed_low = normalized_first.astype(BF16)
    gelu_output, slope, branch = feed_forward(
        normed_low, up_weight, up_bias, down_weight, down_bias
    )
    second_in = normalized_first + branch
    output_rows = normalize(second_in, gain_ffn, shift_ffn)
    hidden_out = output_rows.astype(BF16).reshape(seq_here, seq_len, width)
    cls_rows = hidden_out[:, 0, :]
    pooled, ramp_loss, grad_logits, grad_pool = classify(
        cls_rows, labels, w_pool, b_pool, w_class, b_class
    )
    grad_cls = jnp.dot(grad_pool, w_pool.T, preferred_element_type=F32)
    classes = grad_logits.shape[1]
    cls_pack = jnp.concatenate(
        [
            cls_rows.astype(F32),
            grad_pool.astype(F32),
            pooled,
            jnp.pad(grad_logits, ((0, 0), (0, LANES - classes))),
        ],
        axis=1,
    )
    pack_width = cls_pack.shape[1]
    cls_pack = cls_pack.reshape(-1, LANES)

    first_token = lax.broadcasted_iota(jnp.int32, cotangent.shape, 1) == 0
    grad_output = cotangent.astype(F32) + jnp.where(first_token, grad_cls[:, None, :], 0.0)
    grad_output = grad_output.reshape(tokens, width)
    _, second_back = jax.vjp(normalize, second_in, gain_ffn, shift_ffn)
    grad_second, grad_gain_ffn, grad_shift_ffn = second_back(grad_output)
    grad_branch = grad_second.astype(BF16)
    grad_b_down = jnp.sum(grad_branch, axis=0, dtype=F32)
    part_w_down = jnp.dot(gelu_output.T, grad_branch, preferred_element_type=F32).astype(BF16)
    devices = lax.axis_size("dp") * lax.axis_size("head")
    grad_first, grad_b_up, grad_w_down, cls_all, *part_w_up = feed_back(
        head_bits,
        dp_bits,
        grad_branch,
        slope,
        normed_low,
        up_weight,
        down_weight,
        grad_second,
        part_w_down.reshape(devices, -1, width),
        cls_pack,
    )
    grad_b_up = grad_b_up[0]
    _, first_back = jax.vjp(normalize, first_in, gain_att, shift_att)
    grad_first_in, grad_gain_att, grad_shift_att = first_back(grad_first)
    grad_attended = grad_first_in.astype(BF16)
    grad_b_out = jnp.sum(grad_attended, axis=0, dtype=F32)
    part_w_out = jnp.dot(combined.T, grad_attended, preferred_element_type=F32).astype(BF16)
    far_context, own_context = [
        dot_nt(
            grad_attended,
            lax.dynamic_slice_in_dim(attention_output_weight, at * half_width, half_width, 0),
        ).astype(BF16)
        for at in (1 - far_side, far_side)
    ]
    local = query_key_value_weight.shape[2]
    vectors = [
        grad_b_out,
        grad_gain_att,
        grad_shift_att,
        grad_b_up,
        grad_b_down,
        grad_gain_ffn,
        grad_shift_ffn,
    ]
    far, own = [
        (half[1], half[2], half[3], grad_half, half[0].reshape(-1, width), half[5])
        for half, grad_half in ((halves[1], far_context), (halves[0], own_context))
    ]
    grad_in, grad_w_up, grad_w_out, qkv, sums = back_all(
        head_bits,
        dp_bits,
        far,
        own,
        rows_in,
        grad_first_in,
        [part_w_up[0].reshape(devices, -1, width)] if len(part_w_up) == 1 else part_w_up,
        part_w_out.reshape(-1, TILE, width),
        jnp.concatenate(vectors).reshape(-1, LANES),
    )
    grad_w_up = grad_w_up.T
    grad_w_out = grad_w_out.reshape(width, width)
    grad_w_qkv = jnp.transpose(qkv.reshape(3, local, width), (0, 2, 1))
    edges, reached = [], 0
    for vector in vectors:
        reached += vector.shape[0]
        edges.append(reached)
    (
        grad_b_out,
        grad_gain_att,
        grad_shift_att,
        grad_b_up,
        grad_b_down,
        grad_gain_ffn,
        grad_shift_ffn,
        bias_all,
    ) = jnp.split(sums.reshape(-1), edges)
    grad_b_qv = lax.dynamic_slice_in_dim(
        bias_all.reshape(2, width), lax.axis_index("head") * local, local, 1
    )
    cls_all = cls_all.reshape(-1, pack_width)
    all_cls, all_pool, pooled = jnp.split(cls_all[:, : 3 * width], 3, axis=1)
    grad_logits = cls_all[:, 3 * width : 3 * width + classes]
    grad_b_class = jnp.sum(grad_logits, axis=0)
    grad_w_class = jnp.dot(pooled.T, grad_logits, precision=lax.Precision.HIGHEST)
    grad_b_pool = jnp.sum(all_pool, axis=0)
    grad_w_pool = jnp.dot(
        all_cls.T.astype(BF16), all_pool.astype(BF16), preferred_element_type=F32
    )
    return (
        hidden_out,
        ramp_loss,
        grad_in.reshape(seq_here, seq_len, width),
        grad_w_qkv,
        grad_b_qv,
        grad_w_out,
        grad_b_out,
        grad_gain_att,
        grad_shift_att,
        grad_w_up,
        grad_b_up,
        grad_w_down,
        grad_b_down,
        grad_gain_ffn,
        grad_shift_ffn,
        grad_w_pool,
        grad_b_pool,
        grad_w_class,
        grad_b_class,
    )


def solution(mesh):
    rows = P(("dp", "head"))
    placed = (
        (P(("dp", "head"), None, None), rows, rows, P(None, None, "head"), P(None, "head"))
        + (P(),) * 14
        + (P(("dp", "head"), None, None),)
    )
    tokens = P(("dp", "head"), None, None)
    outs = (
        (tokens, rows, tokens, P(None, None, "head"), P(None, "head"))
        + (P(),) * 4
        + (P(None, ("dp", "head")), P(), P(("dp", "head"), None))
        + (P(),) * 7
    )
    return jax.shard_map(body, mesh=mesh, in_specs=placed, out_specs=outs, check_vma=False)
```

```python
import functools

import jax
import jax.numpy as jnp
from jax import lax
from jax.experimental import pallas as pl
from jax.experimental.pallas import tpu as pltpu
from jax.sharding import PartitionSpec as P

HEAD_DIM = 64
EPSILON = 1e-06
MASKED = -1000000000.0
BF16, F32 = jnp.bfloat16, jnp.float32


def bit_count(n):
    assert n & (n - 1) == 0
    return n.bit_length() - 1


def exchange(value, axis, bit):
    size = lax.axis_size(axis)
    step = 1 << bit
    return lax.ppermute(value, axis, [(i, i ^ step) for i in range(size)])


def own_bit(axis, bit):
    return (lax.axis_index(axis) >> bit) & 1


def bits_of(axes):
    found = []
    for axis in axes:
        found += [(axis, b) for b in reversed(range(bit_count(lax.axis_size(axis))))]
    return found


def normalize(row_block, gain_row, shift_row):
    center = jnp.mean(row_block, axis=-1, keepdims=True)
    centered = row_block - center
    spread = jnp.mean(centered * centered, axis=-1, keepdims=True)
    return centered * lax.rsqrt(spread + EPSILON) * gain_row + shift_row


LANES = 128
PAIR = LANES // HEAD_DIM
SCALE = HEAD_DIM ** (-0.5)


def dot_nt(left, right):
    return lax.dot_general(left, right, (((1,), (1,)), ((), ())), preferred_element_type=F32)


def dot_nn(left, right):
    return jnp.dot(left, right, preferred_element_type=F32)


def head_lanes(block, head):
    lane = lax.broadcasted_iota(jnp.int32, block.shape, 1)
    inside = (lane >= head * HEAD_DIM) & (lane < (head + 1) * HEAD_DIM)
    return jnp.where(inside, block.astype(F32), 0.0)


def attend_kernel(length_ref, query_ref, key_ref, value_ref, context_ref, probs_ref):
    length = length_ref[pl.program_id(0)]
    query, key = query_ref[...], key_ref[...]
    value_t = value_ref[...].T
    rows = query.shape[0]
    key_at = lax.broadcasted_iota(jnp.int32, (rows, rows), 0)
    contexts = []
    for head in range(PAIR):
        own_query = (head_lanes(query, head) * SCALE).astype(BF16)
        scores = jnp.where(key_at < length, dot_nt(key, own_query), MASKED)
        shifted = jnp.exp(scores - jnp.max(scores, axis=0, keepdims=True))
        inverse = 1.0 / jnp.sum(shifted, axis=0, keepdims=True)
        probs = (shifted * inverse).astype(BF16)
        probs_ref[0, head] = probs
        contexts.append(dot_nn(value_t[head * HEAD_DIM : (head + 1) * HEAD_DIM], probs))
    context_ref[...] = jnp.concatenate(contexts, axis=0).T.astype(BF16)


def attend(lengths, query, key, value):
    seqs = lengths.shape[0]
    tokens, width = query.shape
    rows, pairs = tokens // seqs, width // LANES
    block = pl.BlockSpec((rows, LANES), lambda s, p: (s, p))
    return pl.pallas_call(
        attend_kernel,
        grid=(seqs, pairs),
        in_specs=[pl.BlockSpec(memory_space=pltpu.SMEM), block, block, block],
        out_specs=[block, pl.BlockSpec((1, PAIR, rows, rows), lambda s, p: (s, p, 0, 0))],
        out_shape=[
            jax.ShapeDtypeStruct((tokens, width), BF16),
            jax.ShapeDtypeStruct((seqs, pairs * PAIR, rows, rows), BF16),
        ],
        cost_estimate=pl.CostEstimate(
            flops=seqs * pairs * 12 * rows * rows * LANES,
            bytes_accessed=8 * tokens * width + 4 * tokens * rows * pairs,
            transcendentals=0,
        ),
    )(lengths, query, key, value)


def gelu_parts(values):
    bell = jnp.exp(-0.5 * values * values)
    inner = 1.0 / (1.0 + (0.3275911 * 0.5**0.5) * jnp.abs(values))
    series = 0.5 * 1.061405429
    for term in (-1.453152027, 1.421413741, -0.284496736, 0.254829592):
        series = series * inner + 0.5 * term
    tail = series * inner * bell
    below = jnp.where(values < 0.0, tail, 1.0 - tail)
    return values * below, below + values * bell * 0.3989422804014327


FF_TILE = 512
ROW_TILE = 256


def feed_kernel(rows_ref, up_ref, up_bias_ref, down_ref, down_bias_ref, act_ref, slope_ref, out_ref):
    first = pl.program_id(0) == 0

    @pl.when(first)
    def _():
        out_ref[...] = jnp.broadcast_to(down_bias_ref[...], out_ref.shape)

    def two_tiles(pair, carry):
        for one in range(2):
            row_tile(pl.ds(pl.multiple_of((2 * pair + one) * ROW_TILE, ROW_TILE), ROW_TILE))
        return carry

    def row_tile(here):
        before = dot_nn(rows_ref[here, :], up_ref[...]) + up_bias_ref[...]
        active, slope = gelu_parts(before)
        active = active.astype(BF16)
        act_ref[here, :] = active
        slope_ref[here, :] = slope.astype(BF16)
        out_ref[here, :] += dot_nn(active, down_ref[...])

    lax.fori_loop(0, rows_ref.shape[0] // (2 * ROW_TILE), two_tiles, 0)


def feed_forward(rows, up_weight, up_bias, down_weight, down_bias):
    tokens, width = rows.shape
    units = up_weight.shape[1]
    whole = lambda shape: pl.BlockSpec(shape, lambda i: (0, 0))
    columns = lambda height: pl.BlockSpec((height, FF_TILE), lambda i: (0, i))
    return pl.pallas_call(
        feed_kernel,
        grid=(units // FF_TILE,),
        in_specs=[
            whole((tokens, width)),
            columns(width),
            columns(1),
            pl.BlockSpec((FF_TILE, width), lambda i: (i, 0)),
            whole((1, width)),
        ],
        out_specs=[columns(tokens), columns(tokens), whole((tokens, width))],
        out_shape=[
            jax.ShapeDtypeStruct((tokens, units), BF16),
            jax.ShapeDtypeStruct((tokens, units), BF16),
            jax.ShapeDtypeStruct((tokens, width), F32),
        ],
        cost_estimate=pl.CostEstimate(
            flops=8 * tokens * width * units,
            bytes_accessed=4 * tokens * units + 4 * width * units,
            transcendentals=0,
        ),
    )(rows, up_weight, up_bias[None], down_weight, down_bias[None])


MESH = pl.DeviceIdType.MESH


def mine_of(axis, bit):
    return lax.rem(lax.div(lax.axis_index(axis), 1 << bit), 2)


def partner_of(axis, bit):
    return {axis: lax.axis_index(axis) + (1 << bit) * (1 - 2 * mine_of(axis, bit))}


def place_of(bits):
    place = 0
    for axis, bit in bits:
        place = 2 * place + mine_of(axis, bit)
    return place


def greet(bits):
    barrier = pltpu.get_barrier_semaphore()
    for axis, bit in bits:
        pl.semaphore_signal(
            barrier, inc=1, device_id=partner_of(axis, bit), device_id_type=MESH
        )
    pl.semaphore_wait(barrier, len(bits))


def copy_to(source, target, sems, bit):
    return pltpu.make_async_remote_copy(
        src_ref=source,
        dst_ref=target,
        send_sem=sems.at[0],
        recv_sem=sems.at[1],
        device_id=partner_of(*bit),
        device_id_type=MESH,
    )


class Scatter:
    def __init__(self, shape, lanes, joint, order, far=False):
        self.shape, self.lanes, self.joint, self.order = shape, lanes, joint, order
        self.far = far

    def blocks(self, stage):
        halved = len([bit for bit in self.order[:stage] if bit in self.joint])
        return self.shape[0] >> halved

    def scratch(self):
        rows, width = self.shape[1], self.lanes[1]
        return [
            pltpu.VMEM((self.blocks(stage + 1), rows, width), BF16)
            for stage in range(len(self.order))
        ] + (
            [
                pltpu.VMEM((self.blocks(1), rows, width), BF16),
                pltpu.SemaphoreType.DMA(()),
            ]
            if self.far
            else []
        ) + [pltpu.SemaphoreType.DMA((len(self.order), 2))]

    def bind(self, source, scratch, last=None):
        self.source, self.sems, self.last = source, scratch[-1], last
        self.slots = scratch[: len(self.order)]
        if self.far:
            self.kept, self.kept_sem = scratch[len(self.order) : -1]
        return self

    def split(self, stage):
        bit = self.order[stage]
        if bit not in self.joint:
            return 1, self.blocks(stage), None
        left = [b for b in self.joint if b not in self.order[:stage]]
        high = 1 << left.index(bit)
        return high, self.blocks(stage) // (2 * high), mine_of(*bit)

    def view(self, stage, at):
        if stage == 0:
            return self.source.at[at, :, pl.ds(*self.lanes)]
        return self.slots[stage - 1].at[at]

    def steps(self):
        return len(self.order)

    def start(self, stage):
        high, low, side = self.split(stage)

        def send(run, carry):
            at = 0 if side is None else (2 * run + 1 - side) * low
            copy_to(
                self.view(stage, pl.ds(at, low)),
                self.slots[stage].at[pl.ds(run * low, low)],
                self.sems.at[stage],
                self.order[stage],
            ).start()
            if self.far and stage == 0:
                pltpu.make_async_copy(
                    self.view(0, pl.ds((2 * run + side) * low, low)),
                    self.kept.at[pl.ds(run * low, low)],
                    self.kept_sem,
                ).start()
            return carry

        lax.fori_loop(0, high, send, 0)

    def whole(self, stage):
        slot = self.slots[stage]
        return copy_to(slot, slot, self.sems.at[stage], self.order[stage])

    def finish(self, stage):
        high, low, side = self.split(stage)
        slot = self.slots[stage]
        self.whole(stage).wait_recv()
        from_kept = self.far and stage == 0
        if from_kept:
            pltpu.make_async_copy(self.kept, self.kept, self.kept_sem).wait()
        final = stage + 1 == len(self.order) and self.last is not None

        def add(index, carry):
            kept = index
            if side is not None:
                kept = (2 * lax.div(index, low) + side) * low + lax.rem(index, low)
            mine = self.kept[index] if from_kept else self.view(stage, kept)[...]
            theirs = slot[index]
            if final:
                self.last(index, mine.astype(F32) + theirs.astype(F32))
            else:
                slot[index] = mine + theirs
            return carry

        lax.fori_loop(0, high * low, add, 0)

    def drain(self):
        for stage in range(len(self.order)):
            self.whole(stage).wait_send()


class Gather:
    def __init__(self, shape, dtype, order):
        self.shape, self.dtype, self.order = shape, dtype, order

    def scratch(self):
        count = self.shape[0] << len(self.order)
        return [
            pltpu.VMEM((count,) + self.shape[1:], self.dtype),
            pltpu.SemaphoreType.DMA((len(self.order), 2)),
        ]

    def bind(self, scratch):
        self.buffer, self.sems = scratch
        self.place = place_of(list(reversed(self.order)))
        return self

    def own(self, index):
        return self.place * self.shape[0] + index

    def steps(self):
        return len(self.order)

    def copy(self, stage, theirs):
        run = 1 << stage
        base = lax.div(self.place, run) * run
        if theirs:
            base = base + run * (1 - 2 * mine_of(*self.order[stage]))
        here = self.buffer.at[pl.ds(base * self.shape[0], run * self.shape[0])]
        return copy_to(here, here, self.sems.at[stage], self.order[stage])

    def start(self, stage):
        self.copy(stage, False).start()

    def finish(self, stage):
        self.copy(stage, True).wait_recv()

    def drain(self):
        for stage in range(len(self.order)):
            self.copy(stage, False).wait_send()

    def natural(self, position, bits):
        index = 0
        for bit in bits:
            index = 2 * index + lax.rem(lax.div(position, 1 << self.order.index(bit)), 2)
        return index


class Swap:
    def __init__(self, shape, bit):
        self.shape, self.bit = shape, bit

    def scratch(self):
        return [pltpu.VMEM(self.shape, BF16), pltpu.SemaphoreType.DMA((2,))]

    def bind(self, source, scratch):
        self.source, (self.slot, self.sems) = source, scratch
        return self

    def steps(self):
        return 1

    def copy(self):
        return copy_to(self.source, self.slot, self.sems, self.bit)

    def start(self, stage):
        self.copy().start()

    def finish(self, stage):
        self.copy().wait_recv()

    def drain(self):
        self.copy().wait_send()


class Total:
    def __init__(self, shape, order):
        self.shape, self.order = shape, order

    def scratch(self):
        return [
            pltpu.VMEM((len(self.order) + 1,) + self.shape, F32),
            pltpu.VMEM((len(self.order),) + self.shape, F32),
            pltpu.SemaphoreType.DMA((len(self.order), 2)),
        ]

    def bind(self, scratch):
        self.held, self.slots, self.sems = scratch
        return self

    def steps(self):
        return len(self.order)

    def copy(self, stage):
        return copy_to(
            self.held.at[stage], self.slots.at[stage], self.sems.at[stage], self.order[stage]
        )

    def start(self, stage):
        self.copy(stage).start()

    def finish(self, stage):
        self.copy(stage).wait_recv()
        self.held[stage + 1] = self.held[stage] + self.slots[stage]

    def drain(self):
        for stage in range(len(self.order)):
            self.copy(stage).wait_send()


def take(scratch, chain):
    count = len(chain.scratch())
    return [scratch.pop(0) for _ in range(count)]


class Flow:
    def __init__(self, *transfers):
        self.todo = [(t, stage) for t in transfers for stage in range(t.steps())]
        self.at = -1

    def plan(self):
        at = self.at
        self.at += 1

        def advance():
            if at >= 0:
                transfer, stage = self.todo[at]
                transfer.finish(stage)
            if at + 1 < len(self.todo):
                transfer, stage = self.todo[at + 1]
                transfer.start(stage)

        return advance

    def open(self):
        return self.at < len(self.todo)


TILE = 8


def halvings(blocks, bits):
    count = 0
    while count < len(bits) and blocks % 2 == 0:
        blocks //= 2
        count += 1
    return bits[:count]


def orders(head_bits, dp_bits):
    low_head, low_dp = list(reversed(head_bits)), list(reversed(dp_bits))
    axes = low_head[-1:] + low_dp[:2]
    return [low_head[:-1] + axes[i:] + axes[:i] + low_dp[2:] for i in range(3)]


def plan(*flows):
    listed = [one for flow in flows for one in (flow if isinstance(flow, list) else [flow])]
    return [one.plan() for one in listed if one.open()]


def move(*flows):
    for advance in plan(*flows):
        advance()


def keep(target, lane):
    def store(index, total):
        target[:, pl.ds(*lane)] = total

    return store


BACK_TILE = 768
AHEAD = 1
FEED_EVENTS = (
    (0, 5, (3,)),
    (0, 7, (0, 1, 2,)),
    (1, 1, (3,)),
    (2, 2, (3,)),
    (3, 0, (0, 2,)),
    (3, 1, (1,)),
    (3, 3, (3,)),
    (3, 7, (3,)),
)
FEED_TAIL = (0, 2, 1, 4, 5, 6, 0, 2, 1, 0, 2, 1)


def feed_back(head_bits, dp_bits, grad_branch, slope, normed_low, up_weight, down_weight, grad_second, down, cls):
    joint = dp_bits + head_bits
    order = orders(head_bits, dp_bits)
    tokens, width = grad_branch.shape
    units = up_weight.shape[1]
    third = width // 3
    lanes = [(i * third, third) for i in range(3)]
    large = [Scatter(down.shape, lanes[i], joint, order[i], far=True) for i in range(3)]
    rows = Gather((1,) + cls.shape, F32, order[0][::-1])
    blocks, depth, _ = down.shape
    ahead = depth % 16 == 0 and BACK_TILE % (2 * depth) == 0
    early = [Scatter(down.shape, lanes[i], joint, order[i][:AHEAD]) for i in range(3)]
    early = early if ahead else []
    everything = large + [rows] + early

    def kernel(
        branch_ref, slope_ref, normed_ref, up_ref, weight_ref, second_ref, down_ref, cls_ref,
        first_ref, bias_ref, sum_ref, all_ref, *rest
    ):
        part_refs, rest = rest[:part_count], rest[part_count:]
        pre_t, slopes, ups, weights, parts, copy_sems, in_sems, out_sems, *scratch = rest
        held = [take(scratch, t) for t in everything]
        for i, t in enumerate(early):

            def passed(index, total, i=i):
                part_refs[i][index] = total.astype(BF16)

            t.bind(parts, held[4 + i], passed)
        for i in range(3):
            large[i].bind(down_ref, held[i], keep(sum_ref, lanes[i]))
        rows.bind(held[3])
        flows, flow_rows = [Flow(t) for t in large], Flow(rows)
        flows_early = [Flow(t) for t in early]
        second_copy = pltpu.make_async_copy(second_ref, first_ref, copy_sems.at[0])
        second_copy.start()
        tiles = units // BACK_TILE

        def columns_of(index):
            return pl.ds(pl.multiple_of(index * BACK_TILE, BACK_TILE), BACK_TILE)

        def loads(index):
            slot, column = lax.rem(index, 2), columns_of(index)
            pairs = (
                (slope_ref.at[:, column], slopes.at[slot]),
                (up_ref.at[:, column], ups.at[slot]),
                (weight_ref.at[column, :], weights.at[slot]),
            )
            return [
                pltpu.make_async_copy(source, target, in_sems.at[slot, which])
                for which, (source, target) in enumerate(pairs)
            ]

        def store(index):
            slot = lax.rem(index, 2)
            return pltpu.make_async_copy(
                parts.at[slot], part_refs[0].at[columns_of(index), :], out_sems.at[slot]
            )

        for copy in loads(0):
            copy.start()
        rows.buffer[rows.place] = cls_ref[...]
        greet(joint)
        move(flows, flow_rows)

        events = [
            (when, at, plan(*[flow_rows if which == 3 else flows[which] for which in moved]))
            for when, at, moved in FEED_EVENTS
        ]

        def unit_tile(index, carry):
            column, slot = columns_of(index), lax.rem(index, 2)
            for copy in loads(index):
                copy.wait()

            @pl.when(index + 1 < tiles)
            def _():
                for copy in loads(index + 1):
                    copy.start()

            @pl.when(index == 0)
            def _():
                second_copy.wait()

            if not ahead:

                @pl.when(index >= 2)
                def _():
                    store(index - 2).wait()

            places = iter(range(tokens))

            def meet():
                place = next(places)
                for when, at, moved in events:
                    if at == place:

                        @pl.when(index == when)
                        def _():
                            for advance in moved:
                                advance()

            bias = 0.0
            for start in range(0, tokens, ROW_TILE):
                here = pl.ds(start, ROW_TILE)
                grad = dot_nt(branch_ref[here, :], weights[slot])
                pre = (grad * slopes[slot, here, :].astype(F32)).astype(BF16)
                bias = bias + jnp.sum(pre.astype(F32), axis=0, keepdims=True)
                pre_t[:, here] = pre.T
                first_ref[here, :] = first_ref[here, :] + dot_nt(pre, ups[slot])
                meet()
            bias_ref[:, column] = bias
            step = 2 * depth if ahead else ROW_TILE

            def part_rows(chunk, carry):
                here = pl.ds(pl.multiple_of(chunk * step, step), step)
                part = dot_nn(pre_t[here, :], normed_ref[...])
                if ahead:
                    at = (index * BACK_TILE) // depth + 2 * chunk
                    parts[pl.ds(at, 2)] = part.reshape(2, depth, width).astype(BF16)
                else:
                    parts[slot, here, :] = part.astype(BF16)
                return carry

            lax.fori_loop(0, BACK_TILE // step, part_rows, 0)
            for _ in range(BACK_TILE // step):
                meet()
            if not ahead:
                store(index).start()
            return carry

        lax.fori_loop(0, tiles, unit_tile, 0)
        if not ahead:
            for index in range(max(tiles - 2, 0), tiles):
                store(index).wait()
        move(flows_early)
        every_flow = flows + [flow_rows] + flows_early
        for which in FEED_TAIL:
            move(*every_flow[which : which + 1])
        while any(flow.open() for flow in every_flow):
            move(every_flow)
        out_copy = pltpu.make_async_copy(rows.buffer, all_ref, copy_sems.at[1])
        out_copy.start()
        out_copy.wait()
        for t in everything:
            t.drain()

    part_count = 3 if ahead else 1
    if ahead:
        part_shapes = [
            jax.ShapeDtypeStruct((t.blocks(AHEAD), depth, third), BF16) for t in early
        ]
        parts_shape = (blocks, depth, width)
    else:
        part_shapes = [jax.ShapeDtypeStruct((units, width), BF16)]
        parts_shape = (2, BACK_TILE, width)
    vmem, anywhere = pl.BlockSpec(memory_space=pltpu.VMEM), pl.BlockSpec(memory_space=pl.ANY)
    return pl.pallas_call(
        kernel,
        in_specs=[vmem, anywhere, vmem] + [anywhere] * 4 + [vmem],
        out_specs=[vmem, vmem, vmem, anywhere] + [vmem if ahead else anywhere] * part_count,
        out_shape=[
            jax.ShapeDtypeStruct((tokens, width), F32),
            jax.ShapeDtypeStruct((1, units), F32),
            jax.ShapeDtypeStruct(down.shape[1:], F32),
            jax.ShapeDtypeStruct((1 << len(joint),) + cls.shape, F32),
        ]
        + part_shapes,
        scratch_shapes=[
            pltpu.VMEM((BACK_TILE, tokens), BF16),
            pltpu.VMEM((2, tokens, BACK_TILE), BF16),
            pltpu.VMEM((2, width, BACK_TILE), BF16),
            pltpu.VMEM((2, BACK_TILE, width), BF16),
            pltpu.VMEM(parts_shape, BF16),
            pltpu.SemaphoreType.DMA((2,)),
            pltpu.SemaphoreType.DMA((2, 3)),
            pltpu.SemaphoreType.DMA((2,)),
        ]
        + [x for t in everything for x in t.scratch()],
        compiler_params=pltpu.CompilerParams(
            collective_id=0, has_side_effects=True, vmem_limit_bytes=62 * 1024 * 1024
        ),
    )(grad_branch, slope, normed_low, up_weight, down_weight, grad_second, down, cls)


BACK_EVENTS = (
    (
        (2, "o0 o1"),
        (8, "u2"),
        (9, "o0"),
        (10, "u0 u1 o1"),
    ),
    (
        (1, "o0"),
        (2, "f0 f1 u2"),
        (3, "u0 o1"),
        (4, "o0"),
        (6, "u1 o1"),
        (8, "u2 o0"),
        (9, "f0 u0"),
        (10, "f1 u1 o1"),
    ),
)
GRAD_EVENTS = ("o0", "f0 m", "w0 w1 f1 u2", "o0 o1")
BACK_TAIL = (
    "u0 m u1 o1",
    "f0 m f1 w1",
    "o0 f0 o1 w0",
    "f1 m o0 w1",
    "m w0 o0 o1",
    "o1 w1 s1 w0",
    "s0 s1 s0 s1",
    "s0 s1 s0",
)


def back_all(head_bits, dp_bits, far, own, rows_in, grad_first_in, up, out, vector):
    joint = dp_bits + head_bits
    order = orders(head_bits, dp_bits)
    low_head, low_dp = list(reversed(head_bits)), list(reversed(dp_bits))
    dp_order = (low_dp, low_dp[1:2] + low_dp[:1] + low_dp[2:])
    far_bit, join_bits = head_bits[0], low_head[:-1]
    tokens, width = rows_in.shape
    seqs, _, length, _ = far[5].shape
    half = far[0].shape[1]
    pairs = half // LANES
    steps = pairs * seqs
    local = half >> len(join_bits)
    chunks = local // HEAD_DIM
    tiles = 3 * local // TILE
    chunk_tiles = HEAD_DIM // TILE
    middle = width // 2
    lanes = ((0, middle), (middle, middle))
    third = width // 3
    thirds = [(i * third, third) for i in range(3)]
    if len(up) == 1:
        large = [Scatter(up[0].shape, thirds[i], joint, order[i], far=True) for i in range(3)]
        up_block = up[0].shape[1:]
    else:
        large = [
            Scatter(
                up[i].shape,
                (0, third),
                [bit for bit in joint if bit not in order[i][:AHEAD]],
                order[i][AHEAD:],
            )
            for i in range(3)
        ]
        up_block = (up[0].shape[1], width)
    out_bits = [halvings(out.shape[0], order[i][:5]) for i in range(2)]
    outs = [Scatter(out.shape, lanes[i], out_bits[i], order[i]) for i in range(2)]
    outs_back = [
        Gather((out.shape[0] >> len(out_bits[i]), TILE, middle), BF16, out_bits[i][::-1])
        for i in range(2)
    ]
    source = (tiles << len(join_bits), TILE, width)
    qkv_bits = [halvings(tiles, dp_order[i][:3]) for i in range(2)]
    far_sums, own_sums = [
        [
            Scatter(source, lanes[i], join_bits + qkv_bits[i], join_bits + dp_order[i])
            for i in range(2)
        ]
        for _ in range(2)
    ]
    last = (tiles >> len(qkv_bits[0]), TILE, middle)
    swaps = [Swap(last, far_bit) for i in range(2)]
    sums_back = [Gather(last, BF16, qkv_bits[i][::-1]) for i in range(2)]
    vector_rows = vector.shape[0]
    bias_rows = 2 * width // LANES
    small = Total((vector_rows + bias_rows, LANES), order[0])
    groups = [large, outs, outs_back, far_sums, own_sums, swaps, sums_back, [small]]
    everything = [t for group in groups for t in group]

    def kernel(*refs):
        refs = list(refs)
        halves = [[refs.pop(0) for _ in range(6)] for _ in range(2)]
        rows_ref, first_ref, out_ref, vector_ref = [refs.pop(0) for _ in range(4)]
        up_refs = [refs.pop(0) for _ in up]
        in_ref, up_sum, out_sum, qkv_sum, vector_sum = [refs.pop(0) for _ in range(5)]
        grads, sources = [refs.pop(0) for _ in range(2)], [refs.pop(0) for _ in range(2)]
        weights = [refs.pop(0) for _ in range(2)]
        partial, probs_buffer, probs_sems, first_sem = [refs.pop(0) for _ in range(4)]
        held = {id(t): take(refs, t) for t in everything}
        side = mine_of(*far_bit)

        def hand_on(gather):
            def store(index, total):
                gather.buffer[gather.own(index)] = total.astype(BF16)

            return store

        for t in outs_back + sums_back + [small]:
            t.bind(held[id(t)])
        for i, t in enumerate(large):
            t.bind(up_refs[i % len(up)], held[id(t)], keep(up_sum, thirds[i]))
        for i in range(2):
            outs[i].bind(out_ref, held[id(outs[i])], hand_on(outs_back[i]))
            far_sums[i].bind(sources[0], held[id(far_sums[i])])
            own_sums[i].bind(sources[1], held[id(own_sums[i])])
            swaps[i].bind(far_sums[i].slots[-1], held[id(swaps[i])])
        flows = {f"u{i}": Flow(t) for i, t in enumerate(large)}
        for i in range(2):
            flows[f"o{i}"] = Flow(outs[i], outs_back[i])
            flows[f"f{i}"] = Flow(far_sums[i], swaps[i])
            flows[f"w{i}"] = Flow(own_sums[i])
            flows[f"s{i}"] = Flow(sums_back[i])
        flows["m"] = Flow(small)

        def merge(i):
            def add(index, carry):
                sums_back[i].buffer[sums_back[i].own(index)] = (
                    own_sums[i].slots[-1][index] + swaps[i].slot[index]
                )
                return carry

            lax.fori_loop(0, last[0], add, 0)

        def ready(name):
            return not (name[0] == "s" and flows[name].at < 0) or not (
                flows["w" + name[1]].open() or flows["f" + name[1]].open()
            )

        def planned(names):
            found = []
            for name in names.split():
                if flows[name].open() and ready(name):
                    if name[0] == "s" and flows[name].at < 0:
                        found.append(functools.partial(merge, int(name[1])))
                    found.append(flows[name].plan())
            return found

        def go(names):
            for advance in planned(names):
                advance()

        def probs_copy(which, step):
            slot = lax.rem(step, 2)
            return pltpu.make_async_copy(
                halves[which][5].at[lax.rem(step, seqs), pl.ds(lax.div(step, seqs) * PAIR, PAIR)],
                probs_buffer.at[slot],
                probs_sems.at[slot],
            )

        late_copies = [pltpu.make_async_copy(first_ref, in_ref, first_sem.at[2])] + [
            pltpu.make_async_copy(halves[i][4], weights[i], first_sem.at[i]) for i in range(2)
        ]
        probs_copy(0, 0).start()
        for copy in late_copies:
            copy.start()
        small.held[0, :vector_rows] = vector_ref[...]
        small.held[0, vector_rows:] = jnp.zeros((bias_rows, LANES), F32)
        greet(joint)
        go("u0 u1 u2 o0 o1")

        def attend_step(which, step, meet):
            query_ref, key_ref, value_ref, grad_ref, _, _ = halves[which]
            pair, seq = lax.div(step, seqs), lax.rem(step, seqs)
            at = (
                pl.ds(pl.multiple_of(seq * length, length), length),
                pl.ds(pl.multiple_of(pair * LANES, LANES), LANES),
            )
            probs_copy(which, step).wait()

            @pl.when(step + 1 < steps)
            def _():
                probs_copy(which, step + 1).start()

            if which == 0:

                @pl.when(step + 1 == steps)
                def _():
                    probs_copy(1, 0).start()

            query, value, grad = query_ref[at], value_ref[at], grad_ref[at]
            key_t = key_ref[at].T
            grad_key = grad_value = 0.0
            grad_query = []
            slot = lax.rem(step, 2)
            for head in range(PAIR):
                own_query = (head_lanes(query, head) * SCALE).astype(BF16)
                own_value = head_lanes(value, head).astype(BF16)
                own_grad = head_lanes(grad, head).astype(BF16)
                low = probs_buffer[slot, head]
                probs = low.astype(F32)
                grad_probs = dot_nt(own_value, grad)
                weighted = jnp.sum(probs * grad_probs, axis=0, keepdims=True)
                grad_scores = (probs * (grad_probs - weighted)).astype(BF16)
                grad_value += dot_nn(low, own_grad)
                grad_key += dot_nn(grad_scores, own_query)
                head_rows = slice(head * HEAD_DIM, (head + 1) * HEAD_DIM)
                grad_query.append(dot_nn(key_t[head_rows], grad_scores))
                if head == 0:
                    meet()
            query_t = (jnp.concatenate(grad_query, axis=0) * SCALE).astype(BF16)
            own = [query_t.T, grad_key.astype(BF16), grad_value.astype(BF16)]
            for kind in range(3):
                column = pl.multiple_of(kind * half + pair * LANES, LANES)
                grads[which][at[0], pl.ds(column, LANES)] = own[kind]
            stacked = jnp.concatenate([query_t, own[1].T, own[2].T], axis=0)
            part = dot_nn(stacked, rows_ref[at[0], :])
            group = (side if which == 1 else 1 - side) * pairs + pair
            for kind, block in ((0, own[0]), (1, own[2])):
                row = vector_rows + kind * (bias_rows // 2) + group
                total = jnp.sum(block.astype(F32), axis=0, keepdims=True)
                small.held[0, pl.ds(row, 1)] = small.held[0, pl.ds(row, 1)] + total

            @pl.when(seq == 0)
            def _():
                partial[...] = part

            @pl.when(seq > 0)
            def _():
                partial[...] = partial[...] + part

            @pl.when(seq == seqs - 1)
            def _():
                for kind in range(3):
                    for one in range(PAIR):
                        chunk = pair * PAIR + one
                        tile = lax.div(chunk, chunks) * tiles + kind * (local // TILE)
                        tile = tile + lax.rem(chunk, chunks) * chunk_tiles
                        start = kind * LANES + one * HEAD_DIM
                        block = partial[start : start + HEAD_DIM, :]
                        sources[which][pl.ds(tile, chunk_tiles)] = block.reshape(
                            chunk_tiles, TILE, width
                        ).astype(BF16)

        def sweep(which, events):
            events = [(when, planned(names)) for when, names in events]

            def step(index, carry):
                places = iter(range(2))

                def meet():
                    place = next(places)
                    for when, moved in events:
                        if when % 2 == place:

                            @pl.when(index == when // 2)
                            def _():
                                for advance in moved:
                                    advance()

                attend_step(which, index, meet)
                meet()
                return carry

            lax.fori_loop(0, steps, step, 0)

        sweep(0, BACK_EVENTS[0])
        go("f0 f1")
        sweep(1, BACK_EVENTS[1])
        go("w0 w1 m")
        for copy in late_copies:
            copy.wait()

        def input_rows(index, carry):
            at = pl.ds(pl.multiple_of(index * ROW_TILE, ROW_TILE), ROW_TILE)
            in_ref[at, :] = (
                in_ref[at, :]
                + dot_nn(grads[0][at, :], weights[0][...])
                + dot_nn(grads[1][at, :], weights[1][...])
            )
            return carry

        blocks = tokens // ROW_TILE
        parts = len(GRAD_EVENTS)
        grad_events = [
            (blocks * (part + 1) // parts - 1, planned(names))
            for part, names in enumerate(GRAD_EVENTS)
        ]

        def input_step(index, carry):
            input_rows(index, carry)
            for when, moved in grad_events:

                @pl.when(index == when)
                def _():
                    for advance in moved:
                        advance()

            return carry

        lax.fori_loop(0, blocks, input_step, 0)
        for names in BACK_TAIL:
            go(names)
        while any(flow.open() for flow in flows.values()):
            go(" ".join(flows))
        for i in range(2):
            for gather, target in ((outs_back[i], out_sum), (sums_back[i], qkv_sum)):

                def spread(index, carry, gather=gather, target=target, lane=lanes[i]):
                    target[index, :, pl.ds(*lane)] = gather.buffer[index].astype(F32)
                    return carry

                lax.fori_loop(0, gather.buffer.shape[0], spread, 0)
        vector_sum[...] = small.held[len(small.order)]
        for t in everything:
            t.drain()

    vmem, anywhere = pl.BlockSpec(memory_space=pltpu.VMEM), pl.BlockSpec(memory_space=pl.ANY)
    half_specs = [vmem] * 4 + [anywhere] * 2
    return pl.pallas_call(
        kernel,
        in_specs=half_specs * 2
        + [vmem, anywhere, vmem, vmem]
        + [anywhere if len(up) == 1 else vmem] * len(up),
        out_specs=[vmem] * 5,
        out_shape=[
            jax.ShapeDtypeStruct((tokens, width), F32),
            jax.ShapeDtypeStruct(up_block, F32),
            jax.ShapeDtypeStruct(out.shape, F32),
            jax.ShapeDtypeStruct((tiles, TILE, width), F32),
            jax.ShapeDtypeStruct(small.shape, F32),
        ],
        scratch_shapes=[pltpu.VMEM((tokens, 3 * half), BF16)] * 2
        + [pltpu.VMEM(source, BF16)] * 2
        + [pltpu.VMEM((3 * half, width), BF16)] * 2
        + [
            pltpu.VMEM((3 * LANES, width), F32),
            pltpu.VMEM((2, PAIR, length, length), BF16),
            pltpu.SemaphoreType.DMA((2,)),
            pltpu.SemaphoreType.DMA((3,)),
        ]
        + [x for t in everything for x in t.scratch()],
        compiler_params=pltpu.CompilerParams(
            collective_id=1, has_side_effects=True, vmem_limit_bytes=62 * 1024 * 1024
        ),
    )(*far, *own, rows_in, grad_first_in, out, vector, *up)


def classify(cls_rows, labels, w_pool, b_pool, w_class, b_class):
    pooled = jnp.tanh(jnp.dot(cls_rows, w_pool, preferred_element_type=F32) + b_pool)
    class_weight = w_class.astype(F32)
    logits = jnp.dot(pooled, class_weight, precision=lax.Precision.HIGHEST) + b_class
    onehot = (labels[:, None] == jnp.arange(logits.shape[1])[None, :]).astype(F32)
    ramp_loss = jax.nn.logsumexp(logits, axis=-1) - jnp.sum(logits * onehot, axis=-1)
    grad_logits = jax.nn.softmax(logits, axis=-1) - onehot
    grad_pool = (
        jnp.dot(grad_logits, class_weight.T, precision=lax.Precision.HIGHEST)
        * (1.0 - pooled * pooled)
    ).astype(BF16)
    return pooled, ramp_loss, grad_logits, grad_pool


def body(
    hidden_in,
    lengths,
    labels,
    query_key_value_weight,
    query_value_bias,
    attention_output_weight,
    attention_output_bias,
    gain_att,
    shift_att,
    up_weight,
    up_bias,
    down_weight,
    down_bias,
    gain_ffn,
    shift_ffn,
    w_pool,
    b_pool,
    w_class,
    b_class,
    cotangent,
):
    seq_here, seq_len, width = hidden_in.shape
    tokens = seq_here * seq_len
    everyone = ("dp", "head")
    head_bits = bits_of(("head",))
    dp_bits = bits_of(("dp",))
    rows_in = hidden_in.reshape(tokens, width)

    half_bits, far_bit = head_bits[1:], head_bits[0]
    own_weight = jnp.transpose(query_key_value_weight, (2, 0, 1))
    own_weight = own_weight.transpose(1, 0, 2)
    far_weight = exchange(own_weight, *far_bit)
    far_bias = exchange(query_value_bias, *far_bit)
    low_order = list(reversed(half_bits))

    def join(blocks, order):
        for axis, bit in order:
            got = exchange(blocks, axis, bit)
            blocks = jnp.where(
                own_bit(axis, bit) == 0,
                jnp.concatenate([blocks, got], axis=1),
                jnp.concatenate([got, blocks], axis=1),
            )
        return blocks

    halves = []
    for weight, bias in ((own_weight, query_value_bias), (far_weight, far_bias)):
        if halves:
            weight, bias, first = lax.optimization_barrier((weight, bias, halves[0][4]))
            halves[0] = halves[0][:4] + (first,) + halves[0][5:]
        weight, bias = join(weight, low_order), join(bias, low_order)
        query = (dot_nt(rows_in, weight[0]) + bias[0]).astype(BF16)
        key = dot_nt(rows_in, weight[1]).astype(BF16)
        value = (dot_nt(rows_in, weight[2]) + bias[1]).astype(BF16)
        context, probs = attend(lengths, query, key, value)
        halves.append((weight, query, key, value, context, probs))
    half_width = halves[0][1].shape[1]
    far_side = own_bit(*far_bit)

    def in_place(own, far, axis):
        return jnp.where(
            far_side == 0,
            jnp.concatenate([own, far], axis=axis),
            jnp.concatenate([far, own], axis=axis),
        )

    combined = in_place(halves[0][4], halves[1][4], 1)
    attended = (
        jnp.dot(combined, attention_output_weight, preferred_element_type=F32)
        + attention_output_bias
    )
    first_in = rows_in.astype(F32) + attended
    normalized_first = normalize(first_in, gain_att, shift_att)
    normed_low = normalized_first.astype(BF16)
    gelu_output, slope, branch = feed_forward(
        normed_low, up_weight, up_bias, down_weight, down_bias
    )
    second_in = normalized_first + branch
    output_rows = normalize(second_in, gain_ffn, shift_ffn)
    hidden_out = output_rows.astype(BF16).reshape(seq_here, seq_len, width)
    cls_rows = hidden_out[:, 0, :]
    pooled, ramp_loss, grad_logits, grad_pool = classify(
        cls_rows, labels, w_pool, b_pool, w_class, b_class
    )
    grad_cls = jnp.dot(grad_pool, w_pool.T, preferred_element_type=F32)
    classes = grad_logits.shape[1]
    cls_pack = jnp.concatenate(
        [
            cls_rows.astype(F32),
            grad_pool.astype(F32),
            pooled,
            jnp.pad(grad_logits, ((0, 0), (0, LANES - classes))),
        ],
        axis=1,
    )
    pack_width = cls_pack.shape[1]
    cls_pack = cls_pack.reshape(-1, LANES)

    first_token = lax.broadcasted_iota(jnp.int32, cotangent.shape, 1) == 0
    grad_output = cotangent.astype(F32) + jnp.where(first_token, grad_cls[:, None, :], 0.0)
    grad_output = grad_output.reshape(tokens, width)
    _, second_back = jax.vjp(normalize, second_in, gain_ffn, shift_ffn)
    grad_second, grad_gain_ffn, grad_shift_ffn = second_back(grad_output)
    grad_branch = grad_second.astype(BF16)
    grad_b_down = jnp.sum(grad_branch, axis=0, dtype=F32)
    part_w_down = jnp.dot(gelu_output.T, grad_branch, preferred_element_type=F32).astype(BF16)
    devices = lax.axis_size("dp") * lax.axis_size("head")
    grad_first, grad_b_up, grad_w_down, cls_all, *part_w_up = feed_back(
        head_bits,
        dp_bits,
        grad_branch,
        slope,
        normed_low,
        up_weight,
        down_weight,
        grad_second,
        part_w_down.reshape(devices, -1, width),
        cls_pack,
    )
    grad_b_up = grad_b_up[0]
    _, first_back = jax.vjp(normalize, first_in, gain_att, shift_att)
    grad_first_in, grad_gain_att, grad_shift_att = first_back(grad_first)
    grad_attended = grad_first_in.astype(BF16)
    grad_b_out = jnp.sum(grad_attended, axis=0, dtype=F32)
    part_w_out = jnp.dot(combined.T, grad_attended, preferred_element_type=F32).astype(BF16)
    far_context, own_context = [
        dot_nt(
            grad_attended,
            lax.dynamic_slice_in_dim(attention_output_weight, at * half_width, half_width, 0),
        ).astype(BF16)
        for at in (1 - far_side, far_side)
    ]
    local = query_key_value_weight.shape[2]
    vectors = [
        grad_b_out,
        grad_gain_att,
        grad_shift_att,
        grad_b_up,
        grad_b_down,
        grad_gain_ffn,
        grad_shift_ffn,
    ]
    far, own = [
        (half[1], half[2], half[3], grad_half, half[0].reshape(-1, width), half[5])
        for half, grad_half in ((halves[1], far_context), (halves[0], own_context))
    ]
    grad_in, grad_w_up, grad_w_out, qkv, sums = back_all(
        head_bits,
        dp_bits,
        far,
        own,
        rows_in,
        grad_first_in,
        [part_w_up[0].reshape(devices, -1, width)] if len(part_w_up) == 1 else part_w_up,
        part_w_out.reshape(-1, TILE, width),
        jnp.concatenate(vectors).reshape(-1, LANES),
    )
    grad_w_up = grad_w_up.T
    grad_w_out = grad_w_out.reshape(width, width)
    grad_w_qkv = jnp.transpose(qkv.reshape(3, local, width), (0, 2, 1))
    edges, reached = [], 0
    for vector in vectors:
        reached += vector.shape[0]
        edges.append(reached)
    (
        grad_b_out,
        grad_gain_att,
        grad_shift_att,
        grad_b_up,
        grad_b_down,
        grad_gain_ffn,
        grad_shift_ffn,
        bias_all,
    ) = jnp.split(sums.reshape(-1), edges)
    grad_b_qv = lax.dynamic_slice_in_dim(
        bias_all.reshape(2, width), lax.axis_index("head") * local, local, 1
    )
    cls_all = cls_all.reshape(-1, pack_width)
    all_cls, all_pool, pooled = jnp.split(cls_all[:, : 3 * width], 3, axis=1)
    grad_logits = cls_all[:, 3 * width : 3 * width + classes]
    grad_b_class = jnp.sum(grad_logits, axis=0)
    grad_w_class = jnp.dot(pooled.T, grad_logits, precision=lax.Precision.HIGHEST)
    grad_b_pool = jnp.sum(all_pool, axis=0)
    grad_w_pool = jnp.dot(
        all_cls.T.astype(BF16), all_pool.astype(BF16), preferred_element_type=F32
    )
    return (
        hidden_out,
        ramp_loss,
        grad_in.reshape(seq_here, seq_len, width),
        grad_w_qkv,
        grad_b_qv,
        grad_w_out,
        grad_b_out,
        grad_gain_att,
        grad_shift_att,
        grad_w_up,
        grad_b_up,
        grad_w_down,
        grad_b_down,
        grad_gain_ffn,
        grad_shift_ffn,
        grad_w_pool,
        grad_b_pool,
        grad_w_class,
        grad_b_class,
    )


def solution(mesh):
    rows = P(("dp", "head"))
    placed = (
        (P(("dp", "head"), None, None), rows, rows, P(None, None, "head"), P(None, "head"))
        + (P(),) * 14
        + (P(("dp", "head"), None, None),)
    )
    tokens = P(("dp", "head"), None, None)
    outs = (
        (tokens, rows, tokens, P(None, None, "head"), P(None, "head"))
        + (P(),) * 4
        + (P(None, ("dp", "head")), P(), P(("dp", "head"), None))
        + (P(),) * 7
    )
    return jax.shard_map(body, mesh=mesh, in_specs=placed, out_specs=outs, check_vma=False)
```
